32 devices in a mesh: gx: 4 (over z), gy: 8 (over y, x, core).
Axes of the slice: x: 2, y: 2, z: 4, core: 2. Of those that a mesh axis runs over, the one named last changes fastest.
Arguments:
- policy_logp: float32 [16, 512, 4096], P('gy', 'gx'), may hold values from -2 to 0
- anchor_logp: float32 [16, 512, 4096], P('gy', 'gx'), may hold values from -2 to 0
- lengths: int32 [16, 512], P('gy', 'gx'), may hold values from 512 to 4096
- rewards: int32 [16, 512], P('gy', 'gx'), may hold values from 0 to 8
- slot_prompt: int32 [16, 512], P('gy', 'gx'), may hold values from 0 to 511, as said below
Outputs:
- token_grad: float32 [16, 512, 4096], P(None, ('gx', 'gy'))
- sample_loss: float32 [16, 512], P(None, ('gx', 'gy'))
- advantage: float32 [16, 512], P(None, ('gx', 'gy'))
The draws below stay inside these ranges and needn't reach their ends.
Inputs may be any that keep to these rules, and one draw needn't show every extreme that they name: `slot_prompt`: for every member k and every aligned block of 128 slots, the slots of the block hold each prompt of the same block exactly once.
All inputs are finite; a program needn't handle non-finite values.
Results may differ from the reference program's by a relative error of at most 0.00002.
Values sent between devices are 32-bit elements; how exact they have to be, the bound alone decides.
A program may use at most 64 MiB of HBM per device.

```python
import jax
import jax.numpy as jnp

K = 16
LMAX = 4096
PROMPTS = 512
BLOCK = 128
SAMPLES = 8192
N_GX = 4


def draw_slot_prompt(key, part):
    subkeys = jax.random.split(jax.random.fold_in(key, 7), K * N_GX)
    shuffled = jax.vmap(lambda subkey: jax.random.permutation(subkey, BLOCK))(subkeys)
    shuffled = shuffled.astype(jnp.int32).reshape(K, N_GX, BLOCK)
    offsets = (jnp.arange(N_GX, dtype=jnp.int32) * BLOCK)[None, :, None]
    return (shuffled + offsets).reshape(K, PROMPTS).astype(jnp.int32)


def with_ends(values, stream_key, least, high):
    spot = [jax.random.randint(jax.random.fold_in(stream_key, axis), (), 0, length) for axis, length in enumerate(values.shape)]
    widest = values.shape.index(max(values.shape))
    neighbour = spot[:widest] + [(spot[widest] + 1) % values.shape[widest]] + spot[widest + 1:]
    return values.at[tuple(spot)].set(least).at[tuple(neighbour)].set(high)


def level_of(stream_key, shape, cuts, low, top_value):
    level, own = 1.0, jax.random.fold_in(stream_key, 6)
    for dim, shards_of in cuts:
        steps = jnp.exp(jax.random.uniform(jax.random.fold_in(own, dim), (shards_of,), jnp.float32, low / len(cuts), top_value / len(cuts)))
        level = level * jnp.repeat(steps, shape[dim] // shards_of).reshape([-1 if axis == dim else 1 for axis in range(len(shape))])
    return level


def setup_inputs(seed: int = 0) -> dict:
    key_list = jax.random.split(jax.random.key(seed), 6)
    policy_logp = jnp.clip(-2.0 + 2.0 * jax.random.uniform(key_list[0], (K, PROMPTS, LMAX), jnp.float32) ** level_of(key_list[0], (K, PROMPTS, LMAX), ((0, 8), (1, 4)), -0.2, 0.2), -2.0, 0.0)
    anchor_logp = jnp.clip(-2.0 + 2.0 * jax.random.uniform(key_list[1], (K, PROMPTS, LMAX), jnp.float32) ** level_of(key_list[1], (K, PROMPTS, LMAX), ((0, 8), (1, 4)), -0.2, 0.2), -2.0, 0.0)
    lengths = with_ends(jax.random.randint(key_list[2], (K, PROMPTS), LMAX // 8, LMAX + 1), jax.random.fold_in(key_list[2], 1), LMAX // 8, LMAX).astype(jnp.int32)
    rewards = with_ends(jax.random.randint(key_list[3], (K, PROMPTS), 0, 9), jax.random.fold_in(key_list[3], 1), 0, 8).astype(jnp.int32)
    slot_prompt = draw_slot_prompt(jax.random.fold_in(key_list[5], 71), 0)
    return dict(policy_logp=policy_logp, anchor_logp=anchor_logp, lengths=lengths, rewards=rewards, slot_prompt=slot_prompt)


kl_weight = 0.1


def reference(policy_logp, anchor_logp, lengths, rewards, slot_prompt):
    member_rows = jnp.arange(K, dtype=jnp.int32)[:, None]
    slot_ids = jnp.broadcast_to(jnp.arange(PROMPTS, dtype=jnp.int32)[None, :], (K, PROMPTS))
    inverse = jnp.zeros((K, PROMPTS), jnp.int32).at[member_rows, slot_prompt].set(slot_ids)
    policy = jnp.take_along_axis(policy_logp, inverse[:, :, None], axis=1)
    anchor = jnp.take_along_axis(anchor_logp, inverse[:, :, None], axis=1)
    seq_len = jnp.take_along_axis(lengths, inverse, axis=1)
    reward = jnp.take_along_axis(rewards, inverse, axis=1).astype(jnp.float32) * 0.25
    total = jnp.sum(reward, axis=0)
    advantage = (K * reward - total[None, :]) / (K - 1)
    ntok = jnp.sum(lengths).astype(jnp.float32)
    positions = jnp.arange(LMAX, dtype=jnp.int32)[None, None, :]
    valid = positions < seq_len[:, :, None]
    log_ratio = anchor - policy
    ratio = jnp.exp(log_ratio)
    token_term = -advantage[:, :, None] * policy + kl_weight * (ratio - log_ratio - 1.0)
    token_grad = jnp.where(valid, -advantage[:, :, None] + kl_weight * (1.0 - ratio), 0.0) * (SAMPLES * LMAX / ntok)
    sample_loss = jnp.sum(jnp.where(valid, token_term, 0.0), axis=2) * (SAMPLES / ntok)
    return token_grad, sample_loss, advantage
```

```python
import functools

import jax
import jax.numpy as jnp
from jax import lax
from jax.experimental import pallas as pl
from jax.experimental.pallas import tpu as pltpu
from jax.sharding import PartitionSpec as P

kl_weight = 0.1
LANES = 128
CHUNKS = 8
MESH = pl.DeviceIdType.MESH
ROLES = 4
STRIPS = 8
SHIFTS = 5
STRIP_BLOCKS = 98
SEND_ORDER = (2, 4, 3, 5, 6, 7, 1)


def partner(index, off, count):
    out, bit = index, 1
    while bit < count:
        if off & bit:
            out = out + bit - 2 * bit * lax.rem(index // bit, 2)
        bit *= 2
    return out


def offsets_by_distance(count):
    far = max(bin(off // 2).count("1") for off in range(1, count))
    near = [off for off in range(1, count) if bin(off // 2).count("1") < far]
    return near, [off for off in range(1, count) if off not in near]


def permuted(onehot, rows):
    high = rows.astype(jnp.bfloat16)
    rest = rows - high.astype(jnp.float32)
    middle = rest.astype(jnp.bfloat16)
    low = (rest - middle.astype(jnp.float32)).astype(jnp.bfloat16)
    dot = functools.partial(jnp.dot, preferred_element_type=jnp.float32)
    return dot(onehot, high) + dot(onehot, middle) + dot(onehot, low)


def folded(x):
    out = x[:, :LANES]
    for start in range(LANES, x.shape[1], LANES):
        out = out + x[:, start : start + LANES]
    return out


def exchange(
    n_gx, n_gy, policy_hbm, anchor_hbm, len_ref, reward_ref, prompt_ref,
    raw_hbm, heads_ref, tails_ref, ntok_ref,
    policy, anchor, sendbuf, onehot, len_col, sum_policy, sum_kl,
    heads_send, heads_recv, tails_send, tails_recv, counts,
    load_sem, send_sem, recv_sem, own_sem,
    head_send_sem, head_recv_sem, tail_send_sem, tail_recv_sem, count_send_sem, count_recv_sem,
):
    gx, gy = lax.axis_index("gx"), lax.axis_index("gy")
    members_dev, slots, seq = policy_hbm.shape
    part = slots // n_gy
    width = seq // CHUNKS

    near, far = offsets_by_distance(n_gy)
    barrier = pltpu.get_barrier_semaphore()
    for off in range(1, n_gy):
        pl.semaphore_signal(barrier, inc=1, device_id=(gx, partner(gy, off, n_gy)), device_id_type=MESH)
    for off in range(1, n_gx):
        pl.semaphore_signal(barrier, inc=1, device_id=(lax.rem(gx + off, n_gx), gy), device_id_type=MESH)

    def loads(c):
        cols = pl.ds(pl.multiple_of(c * width, LANES), width)
        return (
            pltpu.make_async_copy(policy_hbm.at[:, :, cols], policy.at[c], load_sem.at[0, c]),
            pltpu.make_async_copy(anchor_hbm.at[:, :, cols], anchor.at[c], load_sem.at[1, c]),
        )

    for c in range(CHUNKS):
        for copy in loads(c):
            copy.start()

    sublane = lax.broadcasted_iota(jnp.int32, (slots, slots), 0)
    lane = lax.broadcasted_iota(jnp.int32, (slots, slots), 1)
    column = lax.broadcasted_iota(jnp.int32, (slots, LANES), 1)
    local_tokens = jnp.sum(len_ref[...].astype(jnp.float32))
    for m in range(members_dev):
        seq_len = len_ref[m : m + 1, :].astype(jnp.float32)
        reward = reward_ref[m : m + 1, :].astype(jnp.float32) * 0.25
        match = sublane == lax.rem(prompt_ref[m : m + 1, :], slots)
        onehot[m] = jnp.where(match, 1.0, 0.0).astype(jnp.bfloat16)
        len_col[m] = jnp.broadcast_to(
            jnp.sum(jnp.where(sublane == lane, seq_len, 0.0), axis=1, keepdims=True), (slots, LANES)
        )
        sorted_len = jnp.sum(jnp.where(match, seq_len, 0.0), axis=1, keepdims=True)
        sorted_reward = jnp.sum(jnp.where(match, reward, 0.0), axis=1, keepdims=True)
        heads_send[m] = jnp.where(
            column == 0, sorted_len, jnp.where(column == 1, sorted_reward, local_tokens)
        )
    sum_policy[...] = jnp.zeros_like(sum_policy)
    sum_kl[...] = jnp.zeros_like(sum_kl)

    def compute(c):
        for copy in loads(c):
            copy.wait()
        positions = (lax.broadcasted_iota(jnp.int32, (slots, width), 1) + c * width).astype(jnp.float32)
        for m in range(members_dev):
            pol = policy[c, m]
            log_ratio = anchor[c, m] - pol
            ratio = jnp.exp(log_ratio)
            valid = positions < len_col[m][:, :1]
            sum_policy[m] += folded(jnp.where(valid, pol, 0.0))
            sum_kl[m] += folded(jnp.where(valid, kl_weight * (ratio - log_ratio - 1.0), 0.0))
            sendbuf[c, m] = permuted(onehot[m], kl_weight * (1.0 - ratio))

    def rows_of(device):
        return pl.ds(pl.multiple_of(device * part, part), part)

    my_members = pl.ds(gy * members_dev, members_dev)

    def sends(c, offs):
        cols = pl.ds(pl.multiple_of(c * width, LANES), width)
        copies = []
        for off in offs:
            peer = partner(gy, off, n_gy)
            copies.append(
                pltpu.make_async_remote_copy(
                    src_ref=sendbuf.at[c, :, rows_of(peer), :],
                    dst_ref=raw_hbm.at[my_members, :, cols],
                    send_sem=send_sem.at[off - 1],
                    recv_sem=recv_sem.at[off - 1],
                    device_id=(gx, peer),
                    device_id_type=MESH,
                )
            )
        return copies

    def own(c):
        cols = pl.ds(pl.multiple_of(c * width, LANES), width)
        return pltpu.make_async_copy(
            sendbuf.at[c, :, rows_of(gy), :], raw_hbm.at[my_members, :, cols], own_sem.at[c]
        )

    def small_sends(src, dst, send, recv):
        copies = []
        for off in range(1, n_gy):
            peer = partner(gy, off, n_gy)
            copies.append(
                pltpu.make_async_remote_copy(
                    src_ref=src.at[:, rows_of(peer), :],
                    dst_ref=dst.at[my_members],
                    send_sem=send.at[off - 1],
                    recv_sem=recv.at[off - 1],
                    device_id=(gx, peer),
                    device_id_type=MESH,
                )
            )
        copies.append(pltpu.make_async_copy(src.at[:, rows_of(gy), :], dst.at[my_members], send.at[n_gy - 1]))
        return copies

    def count_sends():
        return [
            pltpu.make_async_remote_copy(
                src_ref=counts.at[0],
                dst_ref=counts.at[off],
                send_sem=count_send_sem.at[off - 1],
                recv_sem=count_recv_sem.at[off - 1],
                device_id=(lax.rem(gx + off, n_gx), gy),
                device_id_type=MESH,
            )
            for off in range(1, n_gx)
        ]

    compute(0)
    pl.semaphore_wait(barrier, n_gy - 1 + n_gx - 1)
    head_copies = small_sends(heads_send, heads_recv, head_send_sem, head_recv_sem)
    for copy in head_copies:
        copy.start()

    def step(c, carry):
        for copy in sends(c - 1, near):
            copy.start()
        own(c - 1).start()
        compute(c)
        return carry

    lax.fori_loop(1, CHUNKS, step, 0)
    for copy in sends(CHUNKS - 1, near):
        copy.start()

    def far_step(c, carry):
        for copy in sends(c, far):
            copy.start()
        return carry

    lax.fori_loop(0, CHUNKS, far_step, 0)
    own(CHUNKS - 1).start()

    for m in range(members_dev):
        s1 = jnp.sum(permuted(onehot[m], sum_policy[m]), axis=1, keepdims=True)
        s2 = jnp.sum(permuted(onehot[m], sum_kl[m]), axis=1, keepdims=True)
        tails_send[m] = jnp.where(column == 0, s1, s2)
    for copy in head_copies:
        copy.wait()
    tokens = jnp.zeros((8, LANES), jnp.float32)
    for source in range(n_gy):
        tokens = tokens + heads_recv[source * members_dev, :8, :]
    counts[0] = tokens
    heads_ref[...] = heads_recv[...]
    tail_copies = small_sends(tails_send, tails_recv, tail_send_sem, tail_recv_sem)
    for copy in tail_copies:
        copy.start()
    count_copies = count_sends()
    for copy in count_copies:
        copy.start()
    for copy in count_copies:
        copy.wait()
    ntok_ref[...] = jnp.sum(counts[...], axis=0)
    for copy in tail_copies:
        copy.wait()
    tails_ref[...] = tails_recv[...]
    for c in range(CHUNKS):
        own(c).wait()
    for off in range(1, n_gy):
        source = partner(gy, off, n_gy)
        landed = raw_hbm.at[pl.ds(source * members_dev, members_dev)]
        pltpu.make_async_copy(landed, landed, recv_sem.at[off - 1]).wait()
        pltpu.make_async_copy(landed, landed, send_sem.at[off - 1]).wait()


def finish(samples, raw, heads, tails, ntok, grad, loss, adv, done, done_sem):
    members, part, seq = raw.shape
    tokens = ntok[:1, 2:3]
    total = jnp.sum(heads[...], axis=0)
    advantage = (members * heads[:, :, 1:2] - total[None, :, 1:2]) / (members - 1)
    positions = lax.broadcasted_iota(jnp.int32, (part, seq), 1).astype(jnp.float32)
    scale = samples * seq / tokens

    def store(k):
        return pltpu.make_async_copy(done.at[k], grad.at[k], done_sem.at[k])

    for k in range(members):
        done[k] = jnp.where(positions < heads[k, :, :1], raw[k] - advantage[k], 0.0) * scale
        if k > 0:
            store(k - 1).start()
    shape = (members, part, LANES)
    eye = lax.broadcasted_iota(jnp.int32, shape, 1) == lax.broadcasted_iota(jnp.int32, shape, 2)
    store(members - 1).start()
    value = (tails[:, :, 1:2] - advantage * tails[:, :, :1]) * (samples / tokens)[None]
    loss[...] = jnp.sum(jnp.where(eye, value, 0.0), axis=1)[:, :part]
    adv[...] = jnp.sum(jnp.where(eye, advantage, 0.0), axis=1)[:, :part]
    for k in range(members):
        store(k).wait()


def unpacked_body(n_gx, n_gy, policy_logp, anchor_logp, lengths, rewards, slot_prompt):
    members_dev, slots, seq = policy_logp.shape
    members, part = members_dev * n_gy, slots // n_gy
    f32 = jnp.float32
    chunked = (CHUNKS, members_dev, slots, seq // CHUNKS)
    small = (members, part, LANES)
    hbm_spec = pl.BlockSpec(memory_space=pltpu.HBM)
    vmem_spec = pl.BlockSpec(memory_space=pltpu.VMEM)
    dma = pltpu.SemaphoreType.DMA
    raw, heads, tails, ntok = pl.pallas_call(
        functools.partial(exchange, n_gx, n_gy),
        out_shape=(
            pltpu.VMEM((members, part, seq), f32),
            pltpu.VMEM(small, f32),
            pltpu.VMEM(small, f32),
            pltpu.VMEM((8, LANES), f32),
        ),
        in_specs=[hbm_spec, hbm_spec, vmem_spec, vmem_spec, vmem_spec],
        out_specs=(vmem_spec, vmem_spec, vmem_spec, vmem_spec),
        scratch_shapes=[
            pltpu.VMEM(chunked, f32),
            pltpu.VMEM(chunked, f32),
            pltpu.VMEM(chunked, f32),
            pltpu.VMEM((members_dev, slots, slots), jnp.bfloat16),
            pltpu.VMEM((members_dev, slots, LANES), f32),
            pltpu.VMEM((members_dev, slots, LANES), f32),
            pltpu.VMEM((members_dev, slots, LANES), f32),
            pltpu.VMEM((members_dev, slots, LANES), f32),
            pltpu.VMEM(small, f32),
            pltpu.VMEM((members_dev, slots, LANES), f32),
            pltpu.VMEM(small, f32),
            pltpu.VMEM((n_gx, 8, LANES), f32),
            dma((2, CHUNKS)),
            dma((n_gy - 1,)),
            dma((n_gy - 1,)),
            dma((CHUNKS,)),
            dma((n_gy,)),
            dma((n_gy - 1,)),
            dma((n_gy,)),
            dma((n_gy - 1,)),
            dma((n_gx - 1,)),
            dma((n_gx - 1,)),
        ],
        compiler_params=pltpu.CompilerParams(collective_id=1, has_side_effects=True, vmem_limit_bytes=56 * 2**20),
    )(policy_logp, anchor_logp, lengths, rewards, slot_prompt)
    samples = members * slots * n_gx
    return pl.pallas_call(
        functools.partial(finish, samples),
        out_shape=(
            jax.ShapeDtypeStruct((members, part, seq), f32),
            jax.ShapeDtypeStruct((members, part), f32),
            jax.ShapeDtypeStruct((members, part), f32),
        ),
        in_specs=[vmem_spec] * 4,
        out_specs=(hbm_spec, vmem_spec, vmem_spec),
        scratch_shapes=[pltpu.VMEM((members, part, seq), f32), dma((members,))],
        compiler_params=pltpu.CompilerParams(vmem_limit_bytes=32 * 2**20),
    )(raw, heads, tails, ntok)


def column_of(row):
    n = row.shape[1]
    eye = lax.broadcasted_iota(jnp.int32, (n, n), 0) == lax.broadcasted_iota(jnp.int32, (n, n), 1)
    return jnp.sum(jnp.where(eye, row, 0.0), axis=1, keepdims=True)


def row_of(column):
    n = column.shape[0]
    eye = lax.broadcasted_iota(jnp.int32, (n, n), 0) == lax.broadcasted_iota(jnp.int32, (n, n), 1)
    return jnp.sum(jnp.where(eye, column, 0.0), axis=0, keepdims=True)


def blocks_of(lens):
    return jnp.floor((lens + (LANES - 1)) * (1.0 / LANES))


def strip_targets(lens, groups, index, n_groups, seq):
    rows = ROLES * STRIPS
    keys = [groups[m] * ((seq + 1) * rows) + lens[m] * rows + index[m] for m in range(len(lens))]
    columns = [column_of(key) for key in keys]
    targets = []
    for m, key in enumerate(keys):
        above = sum(jnp.sum(jnp.where(column > key, 1.0, 0.0), axis=0, keepdims=True) for column in columns)
        rank = above - rows * (n_groups - 1 - groups[m])
        first, second, third = rank < STRIPS, rank < 2 * STRIPS, rank < 3 * STRIPS
        strip = jnp.where(
            first, rank, jnp.where(second, 2 * STRIPS - 1 - rank, jnp.where(third, rank - 2 * STRIPS, 4 * STRIPS - 1 - rank))
        )
        role = jnp.where(first, 0.0, jnp.where(second, 3.0, jnp.where(third, 2.0, 1.0)))
        targets.append((role * n_groups + groups[m]) * STRIPS + strip)
    return targets


def strip_counts(targets, lens, total_rows):
    counts = None
    for target, length in zip(targets, lens):
        place = lax.broadcasted_iota(jnp.int32, (total_rows, target.shape[1]), 0).astype(jnp.float32)
        here = jnp.sum(jnp.where(place == target, blocks_of(length), 0.0), axis=1, keepdims=True)
        counts = here if counts is None else counts + here
    return counts


def shift_bits(count):
    shift = count.astype(jnp.int32) - 1
    return [(lax.shift_right_logical(shift, k) & 1) == 1 for k in range(SHIFTS)]


def shifted_up(blocks, bits):
    for k in range(SHIFTS):
        step, n = 2**k, len(blocks)
        moved = []
        for p in range(n + step):
            if p < step:
                moved.append(blocks[p])
            elif p >= n:
                moved.append(blocks[p - step])
            else:
                moved.append(jnp.where(bits[k], blocks[p - step], blocks[p]))
        blocks = moved
    return blocks


def shifted_down(blocks, bits):
    for k in reversed(range(SHIFTS)):
        step = 2**k
        blocks = [jnp.where(bits[k], blocks[p + step], blocks[p]) for p in range(len(blocks) - step)]
    return blocks


def peer_of(index, off, count):
    out, bit = 0, 1
    while bit < count:
        a, b = lax.rem(index // bit, 2), lax.rem(off // bit, 2)
        out = out + bit * (a + b - 2 * a * b)
        bit *= 2
    return out


def packed_exchange(
    n_gx, n_gy, policy_hbm, anchor_hbm, len_ref, reward_ref, prompt_ref,
    done, loss_ref, adv_ref, need_ref,
    policy, anchor, onehot, perm, sendbuf, recvbuf, roles, cnt, rcnt, unperm,
    len_col, sum_policy, sum_kl, len_rows, adv_rows,
    heads_send, heads_recv, tails_send, tails_recv, counts,
    load_sem, send_sem, recv_sem,
    head_send_sem, head_recv_sem, tail_send_sem, tail_recv_sem, count_send_sem, count_recv_sem,
):
    gx, gy = lax.axis_index("gx"), lax.axis_index("gy")
    members_dev, slots, seq = policy_hbm.shape
    members, part = members_dev * n_gy, slots // n_gy
    width = seq // CHUNKS
    nblocks = seq // LANES
    group_rows = n_gy * STRIPS
    samples = members * slots * n_gx
    f32 = jnp.float32

    barrier = pltpu.get_barrier_semaphore()
    for off in range(1, n_gy):
        pl.semaphore_signal(barrier, inc=1, device_id=(gx, partner(gy, off, n_gy)), device_id_type=MESH)
    for off in range(1, n_gx):
        pl.semaphore_signal(barrier, inc=1, device_id=(lax.rem(gx + off, n_gx), gy), device_id_type=MESH)

    def loads(c):
        cols = pl.ds(pl.multiple_of(c * width, LANES), width)
        return (
            pltpu.make_async_copy(policy_hbm.at[:, :, cols], policy.at[c], load_sem.at[0, c]),
            pltpu.make_async_copy(anchor_hbm.at[:, :, cols], anchor.at[c], load_sem.at[1, c]),
        )

    for c in range(CHUNKS):
        for copy in loads(c):
            copy.start()

    sublane = lax.broadcasted_iota(jnp.int32, (slots, slots), 0)
    column = lax.broadcasted_iota(jnp.int32, (slots, LANES), 1)
    lens = [len_ref[m : m + 1, :].astype(f32) for m in range(members_dev)]
    prompts = [lax.rem(prompt_ref[m : m + 1, :], slots) for m in range(members_dev)]
    spots = [prompt.astype(f32) for prompt in prompts]
    groups = [jnp.floor(spot * (1.0 / part)) for spot in spots]
    index = [m * part + spots[m] - part * groups[m] for m in range(members_dev)]
    targets = strip_targets(lens, groups, index, n_gy, seq)
    place = lax.broadcasted_iota(jnp.int32, (ROLES * group_rows, slots), 0).astype(f32)
    for m in range(members_dev):
        onehot[:, m * slots : (m + 1) * slots] = jnp.where(place == targets[m], 1.0, 0.0).astype(jnp.bfloat16)

    def placed(c):
        for copy in loads(c):
            copy.wait()
        rows = kl_weight * (1.0 - jnp.exp(anchor[c] - policy[c]))
        out = permuted(onehot[...], rows.reshape(members_dev * slots, width))
        cols = pl.ds(pl.multiple_of(c * width, LANES), width)
        for role in range(ROLES):
            perm[role, :, cols] = out[role * group_rows : (role + 1) * group_rows]
        return out

    ends = placed(0)
    first, last = ends[:group_rows], ends[3 * group_rows :]
    sendbuf[:, :, :width] = first.reshape(n_gy, STRIPS, width)
    edge = width // LANES
    for j in range(edge):
        at = (STRIP_BLOCKS - 1 - j) * LANES
        sendbuf[:, :, at : at + LANES] = last[:, j * LANES : (j + 1) * LANES].reshape(n_gy, STRIPS, LANES)

    strip_n = strip_counts(targets, lens, ROLES * group_rows)
    cnt[...] = jnp.broadcast_to(strip_n, cnt.shape)
    strip_total = strip_n[:group_rows]
    for role in range(1, ROLES):
        strip_total = strip_total + strip_n[role * group_rows : (role + 1) * group_rows]
    local_need = jnp.max(strip_total)
    local_tokens = sum(jnp.sum(length) for length in lens)
    heads = jnp.where(column == 2 * members_dev, local_tokens, local_need)
    for m in range(members_dev):
        match = sublane == prompts[m]
        sorted_len = jnp.sum(jnp.where(match, lens[m], 0.0), axis=1, keepdims=True)
        reward = reward_ref[m : m + 1, :].astype(f32) * 0.25
        sorted_reward = jnp.sum(jnp.where(match, reward, 0.0), axis=1, keepdims=True)
        heads = jnp.where(column == m, sorted_len, heads)
        heads = jnp.where(column == members_dev + m, sorted_reward, heads)
    heads_send[...] = heads

    def rows_of(device):
        return pl.ds(pl.multiple_of(device * part, part), part)

    def small_sends(src, dst, send, recv):
        copies = []
        for off in range(1, n_gy):
            peer = partner(gy, off, n_gy)
            copies.append(
                pltpu.make_async_remote_copy(
                    src_ref=src.at[rows_of(peer), :],
                    dst_ref=dst.at[gy],
                    send_sem=send.at[off - 1],
                    recv_sem=recv.at[off - 1],
                    device_id=(gx, peer),
                    device_id_type=MESH,
                )
            )
        return copies

    def strip_send(off, peer, lo, hi):
        cols = pl.ds(lo * LANES, (hi - lo) * LANES)
        return pltpu.make_async_remote_copy(
            src_ref=sendbuf.at[peer, :, cols],
            dst_ref=recvbuf.at[gy, :, cols],
            send_sem=send_sem.at[off - 1],
            recv_sem=recv_sem.at[off - 1],
            device_id=(gx, peer),
            device_id_type=MESH,
        )

    pl.semaphore_wait(barrier, n_gy - 1 + n_gx - 1)
    head_copies = small_sends(heads_send, heads_recv, head_send_sem, head_recv_sem)
    for copy in head_copies:
        copy.start()
    for off in SEND_ORDER:
        strip_send(off, partner(gy, off, n_gy), 0, edge).start()
    for off in SEND_ORDER:
        strip_send(off, partner(gy, off, n_gy), STRIP_BLOCKS - edge, STRIP_BLOCKS).start()

    def place_step(c, carry):
        placed(c)
        return carry

    lax.fori_loop(1, CHUNKS, place_step, 0)

    def pack(dst, peer, lo, hi):
        def count(role):
            return cnt[pl.ds(pl.multiple_of(role * group_rows + peer * STRIPS, STRIPS), STRIPS), :]

        def blocks(role):
            rows = pl.ds(pl.multiple_of(peer * STRIPS, STRIPS), STRIPS)
            return [perm[role, rows, j * LANES : (j + 1) * LANES] for j in range(nblocks)]

        def side(outer, inner):
            n = count(outer)
            near_end = blocks(outer)
            behind = shifted_up(blocks(inner), shift_bits(n))
            merged = [near_end[0]]
            for p in range(1, nblocks):
                merged.append(jnp.where(n > p, near_end[p], behind[p - 1]))
            return merged + behind[nblocks - 1 :]

        left, right = side(0, 1), side(3, 2)
        left_n = count(0) + count(1)
        reach = len(left)
        for p in range(lo, hi):
            q = STRIP_BLOCKS - 1 - p
            if q >= reach:
                value = left[p]
            elif p >= reach:
                value = right[q]
            else:
                value = jnp.where(left_n > p, left[p], right[q])
            dst[:, p * LANES : (p + 1) * LANES] = value

    def near_step(t, carry):
        off = 2 + 2 * lax.rem(t, 2) + t // 2
        peer = peer_of(gy, off, n_gy)
        pack(sendbuf.at[peer], peer, edge, STRIP_BLOCKS - edge)
        strip_send(off, peer, edge, STRIP_BLOCKS - edge).start()
        return carry

    lax.fori_loop(0, 4, near_step, 0)

    heads_recv[gy] = heads_send[rows_of(gy), :]
    for copy in head_copies:
        copy.wait()
    lane8 = lax.broadcasted_iota(jnp.int32, (8, LANES), 1)
    tokens = jnp.zeros((8, LANES), f32)
    need = jnp.zeros((8, LANES), f32)
    for source in range(n_gy):
        tile = heads_recv[source, :8, :]
        tokens = tokens + tile
        need = jnp.maximum(need, tile)
    counts[0] = jnp.where(lane8 == 2 * members_dev, tokens, need)
    count_copies = [
        pltpu.make_async_remote_copy(
            src_ref=counts.at[0],
            dst_ref=counts.at[off],
            send_sem=count_send_sem.at[off - 1],
            recv_sem=count_recv_sem.at[off - 1],
            device_id=(lax.rem(gx + off, n_gx), gy),
            device_id_type=MESH,
        )
        for off in range(1, n_gx)
    ]
    for copy in count_copies:
        copy.start()

    for m in range(members_dev):
        len_col[m] = jnp.broadcast_to(column_of(lens[m]), (slots, LANES))
    sum_policy[...] = jnp.zeros_like(sum_policy)
    sum_kl[...] = jnp.zeros_like(sum_kl)

    def sum_step(c, carry):
        positions = (lax.broadcasted_iota(jnp.int32, (slots, width), 1) + c * width).astype(f32)
        for m in range(members_dev):
            pol = policy[c, m]
            log_ratio = anchor[c, m] - pol
            ratio = jnp.exp(log_ratio)
            valid = positions < len_col[m][:, :1]
            sum_policy[m] += folded(jnp.where(valid, pol, 0.0))
            sum_kl[m] += folded(jnp.where(valid, kl_weight * (ratio - log_ratio - 1.0), 0.0))
        return carry

    lax.fori_loop(0, CHUNKS, sum_step, 0)
    tails = jnp.zeros((slots, LANES), f32)
    for m in range(members_dev):
        match = sublane == prompts[m]
        for k, sums in enumerate((sum_policy, sum_kl)):
            total = row_of(jnp.sum(sums[m], axis=1, keepdims=True))
            ordered = jnp.sum(jnp.where(match, total, 0.0), axis=1, keepdims=True)
            tails = jnp.where(column == k * members_dev + m, ordered, tails)
    tails_send[...] = tails
    tails_recv[gy] = tails_send[rows_of(gy), :]
    tail_copies = small_sends(tails_send, tails_recv, tail_send_sem, tail_recv_sem)
    for copy in tail_copies:
        copy.start()

    def far_step(t, carry):
        off = 1 + t + 4 * ((t + 1) // 2)
        peer = peer_of(gy, off, n_gy)
        pack(sendbuf.at[peer], peer, edge, STRIP_BLOCKS - edge)
        strip_send(off, peer, edge, STRIP_BLOCKS - edge).start()
        return carry

    lax.fori_loop(0, 3, far_step, 0)
    pack(recvbuf.at[gy], gy, 0, STRIP_BLOCKS)

    for copy in count_copies:
        copy.wait()
    tokens, need = counts[0], counts[0]
    for off in range(1, n_gx):
        tokens = tokens + counts[off]
        need = jnp.maximum(need, counts[off])
    ntok = tokens[:1, 2 * members_dev : 2 * members_dev + 1]
    need_ref[...] = jnp.broadcast_to(need[:1, 2 * members_dev + 1 : 2 * members_dev + 2], need_ref.shape)
    scale = samples * seq / ntok
    arrived = heads_recv[...]
    total = jnp.sum(arrived, axis=0)
    total = sum(total[:, members_dev + m : members_dev + m + 1] for m in range(members_dev))
    arrived_rows = arrived.reshape(slots, LANES)
    lane = lax.broadcasted_iota(jnp.int32, (1, slots), 1).astype(f32)
    sources = jnp.floor(lane * (1.0 / part))
    got_lens = [row_of(arrived_rows[:, m : m + 1]) for m in range(members_dev)]
    got_index = [m * part + lane - part * sources for m in range(members_dev)]
    got_targets = strip_targets(got_lens, [sources] * members_dev, got_index, n_gy, seq)
    rcnt[...] = jnp.broadcast_to(strip_counts(got_targets, got_lens, ROLES * group_rows), rcnt.shape)
    advantages = []
    for m in range(members_dev):
        reward = arrived[:, :, members_dev + m : members_dev + m + 1]
        advantage = (members * reward - total[None]) / (members - 1)
        advantages.append(advantage)
        adv_rows[m] = jnp.broadcast_to(advantage, (n_gy, part, LANES))
        len_rows[m] = jnp.broadcast_to(arrived[:, :, m : m + 1], (n_gy, part, LANES))
        spot = got_targets[m]
        role = jnp.floor(spot * (1.0 / group_rows))
        inner = spot - role * group_rows - sources * STRIPS + role * STRIPS
        pick = column_of(inner) == lax.broadcasted_iota(jnp.int32, (slots, LANES), 1).astype(f32)
        unperm[:, m] = jnp.where(pick, 1.0, 0.0).astype(jnp.bfloat16).reshape(n_gy, part, LANES)

    def strip_wait(off, peer):
        landed = recvbuf.at[peer]
        pltpu.make_async_copy(landed, landed, recv_sem.at[off - 1]).wait()

    def unpack_step(off, carry):
        source = peer_of(gy, off, n_gy)

        @pl.when(off > 0)
        def _():
            strip_wait(off, source)

        def count(role):
            return rcnt[pl.ds(pl.multiple_of(role * group_rows + source * STRIPS, STRIPS), STRIPS), :]

        def block(p):
            return recvbuf[source, :, p * LANES : (p + 1) * LANES]

        for outer, inner, at in ((0, 1, lambda p: p), (3, 2, lambda p: STRIP_BLOCKS - 1 - p)):
            for j in range(nblocks):
                roles[outer * STRIPS : (outer + 1) * STRIPS, j * LANES : (j + 1) * LANES] = block(at(j))
            behind = [block(at(p)) for p in range(1, 2 * nblocks)]
            behind = shifted_down(behind, shift_bits(count(outer)))
            for j in range(nblocks):
                roles[inner * STRIPS : (inner + 1) * STRIPS, j * LANES : (j + 1) * LANES] = behind[j]
        pick = unperm[source].reshape(members_dev * part, LANES)[:, : ROLES * STRIPS]

        def finish_step(c, inner_carry):
            cols = pl.ds(pl.multiple_of(c * width, LANES), width)
            rows = permuted(pick, roles[:, cols])
            positions = (lax.broadcasted_iota(jnp.int32, (part, width), 1) + c * width).astype(f32)
            for m in range(members_dev):
                value = rows[m * part : (m + 1) * part] - adv_rows[m, source][:, :1]
                valid = positions < len_rows[m, source][:, :1]
                done[source * members_dev + m, :, cols] = jnp.where(valid, value, 0.0) * scale
            return inner_carry

        for c in range(CHUNKS):
            finish_step(c, 0)
        return carry

    lax.fori_loop(0, n_gy, unpack_step, 0)

    for copy in tail_copies:
        copy.wait()
    eye = lax.broadcasted_iota(jnp.int32, (part, LANES), 0) == lax.broadcasted_iota(jnp.int32, (part, LANES), 1)
    for m in range(members_dev):
        first_sum = tails_recv[:, :, m : m + 1]
        second_sum = tails_recv[:, :, members_dev + m : members_dev + m + 1]
        value = (second_sum - advantages[m] * first_sum) * (samples / ntok)[None]
        for source in range(n_gy):
            k = source * members_dev + m
            loss_ref[k : k + 1, :] = jnp.sum(jnp.where(eye, value[source], 0.0), axis=0, keepdims=True)[:, :part]
            adv_ref[k : k + 1, :] = jnp.sum(jnp.where(eye, advantages[m][source], 0.0), axis=0, keepdims=True)[:, :part]
    for off in range(1, n_gy):
        sent = sendbuf.at[0]
        pltpu.make_async_copy(sent, sent, send_sem.at[off - 1]).wait()


def store(done, loss, adv, grad, loss_out, adv_out, sem):
    copy = pltpu.make_async_copy(done, grad, sem)
    copy.start()
    loss_out[...] = loss[...]
    adv_out[...] = adv[...]
    copy.wait()


def packed_body(n_gx, n_gy, policy_logp, anchor_logp, lengths, rewards, slot_prompt):
    members_dev, slots, seq = policy_logp.shape
    members, part = members_dev * n_gy, slots // n_gy
    f32 = jnp.float32
    chunked = (CHUNKS, members_dev, slots, seq // CHUNKS)
    strips = (n_gy, STRIPS, STRIP_BLOCKS * LANES)
    hbm_spec = pl.BlockSpec(memory_space=pltpu.HBM)
    vmem_spec = pl.BlockSpec(memory_space=pltpu.VMEM)
    dma = pltpu.SemaphoreType.DMA
    per_slot = (members_dev, slots, LANES)
    per_source = (members_dev, n_gy, part, LANES)
    rows = ROLES * n_gy * STRIPS
    done, loss, adv, need = pl.pallas_call(
        functools.partial(packed_exchange, n_gx, n_gy),
        out_shape=(
            pltpu.VMEM((members, part, seq), f32),
            pltpu.VMEM((members, part), f32),
            pltpu.VMEM((members, part), f32),
            pltpu.VMEM((8, LANES), f32),
        ),
        in_specs=[hbm_spec, hbm_spec, vmem_spec, vmem_spec, vmem_spec],
        out_specs=(vmem_spec,) * 4,
        scratch_shapes=[
            pltpu.VMEM(chunked, f32),
            pltpu.VMEM(chunked, f32),
            pltpu.VMEM((rows, members_dev * slots), jnp.bfloat16),
            pltpu.VMEM((ROLES, n_gy * STRIPS, seq), f32),
            pltpu.VMEM(strips, f32),
            pltpu.VMEM(strips, f32),
            pltpu.VMEM((ROLES * STRIPS, seq), f32),
            pltpu.VMEM((rows, LANES), f32),
            pltpu.VMEM((rows, LANES), f32),
            pltpu.VMEM((n_gy, members_dev, part, LANES), jnp.bfloat16),
            pltpu.VMEM(per_slot, f32),
            pltpu.VMEM(per_slot, f32),
            pltpu.VMEM(per_slot, f32),
            pltpu.VMEM(per_source, f32),
            pltpu.VMEM(per_source, f32),
            pltpu.VMEM((slots, LANES), f32),
            pltpu.VMEM((n_gy, part, LANES), f32),
            pltpu.VMEM((slots, LANES), f32),
            pltpu.VMEM((n_gy, part, LANES), f32),
            pltpu.VMEM((n_gx, 8, LANES), f32),
            dma((2, CHUNKS)),
            dma((n_gy - 1,)),
            dma((n_gy - 1,)),
            dma((n_gy - 1,)),
            dma((n_gy - 1,)),
            dma((n_gy - 1,)),
            dma((n_gy - 1,)),
            dma((n_gx - 1,)),
            dma((n_gx - 1,)),
        ],
        compiler_params=pltpu.CompilerParams(collective_id=0, has_side_effects=True, vmem_limit_bytes=56 * 2**20),
    )(policy_logp, anchor_logp, lengths, rewards, slot_prompt)

    def fits(policy_logp, anchor_logp, lengths, rewards, slot_prompt, done, loss, adv):
        small = jax.ShapeDtypeStruct((members, part), f32)
        return tuple(pl.pallas_call(
            store,
            out_shape=(jax.ShapeDtypeStruct((members, part, seq), f32), small, small),
            in_specs=[vmem_spec] * 3,
            out_specs=(hbm_spec, vmem_spec, vmem_spec),
            scratch_shapes=[dma(())],
            compiler_params=pltpu.CompilerParams(vmem_limit_bytes=16 * 2**20),
        )(done, loss, adv))

    def overflows(policy_logp, anchor_logp, lengths, rewards, slot_prompt, done, loss, adv):
        return tuple(unpacked_body(n_gx, n_gy, policy_logp, anchor_logp, lengths, rewards, slot_prompt))

    return lax.cond(
        need[0, 0] > STRIP_BLOCKS, overflows, fits,
        policy_logp, anchor_logp, lengths, rewards, slot_prompt, done, loss, adv,
    )


def body(n_gx, n_gy, *args):
    members_dev, slots, seq = args[0].shape
    rows = members_dev * slots // n_gy
    packs = n_gy == 8 and rows == ROLES * STRIPS and slots == LANES and seq == LANES * 2**SHIFTS
    return (packed_body if packs else unpacked_body)(n_gx, n_gy, *args)


def solution(mesh):
    placed = (P("gy", "gx", None), P("gy", "gx", None), P("gy", "gx"), P("gy", "gx"), P("gy", "gx"))
    return jax.shard_map(
        functools.partial(body, mesh.shape["gx"], mesh.shape["gy"]),
        mesh=mesh,
        in_specs=placed,
        out_specs=(P(None, ("gx", "gy"), None), P(None, ("gx", "gy")), P(None, ("gx", "gy"))),
        check_vma=False,
    )
```

```python
import functools

import jax
import jax.numpy as jnp
from jax import lax
from jax.experimental import pallas as pl
from jax.experimental.pallas import tpu as pltpu
from jax.sharding import PartitionSpec as P

kl_weight = 0.1
LANES = 128
CHUNKS = 8
MESH = pl.DeviceIdType.MESH
ROLES = 4
STRIPS = 16
SHIFTS = 5
HEAD_BLOCKS = 4
STRIP_BLOCKS = 75
FIRST_ORDER = (2, 4, 3, 5, 6, 7)


def partner(index, off, count):
    out, bit = index, 1
    while bit < count:
        if off & bit:
            out = out + bit - 2 * bit * lax.rem(index // bit, 2)
        bit *= 2
    return out


def offsets_by_distance(count):
    far = max(bin(off // 2).count("1") for off in range(1, count))
    near = [off for off in range(1, count) if bin(off // 2).count("1") < far]
    return near, [off for off in range(1, count) if off not in near]


def permuted(onehot, rows):
    high = rows.astype(jnp.bfloat16)
    rest = rows - high.astype(jnp.float32)
    middle = rest.astype(jnp.bfloat16)
    low = (rest - middle.astype(jnp.float32)).astype(jnp.bfloat16)
    dot = functools.partial(jnp.dot, preferred_element_type=jnp.float32)
    return dot(onehot, high) + dot(onehot, middle) + dot(onehot, low)


def folded(x):
    out = x[:, :LANES]
    for start in range(LANES, x.shape[1], LANES):
        out = out + x[:, start : start + LANES]
    return out


def exchange(
    n_gx, n_gy, policy_hbm, anchor_hbm, len_ref, reward_ref, prompt_ref,
    raw_hbm, heads_ref, tails_ref, ntok_ref,
    policy, anchor, sendbuf, onehot, len_col, sum_policy, sum_kl,
    heads_send, heads_recv, tails_send, tails_recv, counts,
    load_sem, send_sem, recv_sem, own_sem,
    head_send_sem, head_recv_sem, tail_send_sem, tail_recv_sem, count_send_sem, count_recv_sem,
):
    gx, gy = lax.axis_index("gx"), lax.axis_index("gy")
    members_dev, slots, seq = policy_hbm.shape
    part = slots // n_gy
    width = seq // CHUNKS

    near, far = offsets_by_distance(n_gy)
    barrier = pltpu.get_barrier_semaphore()
    for off in range(1, n_gy):
        pl.semaphore_signal(barrier, inc=1, device_id=(gx, partner(gy, off, n_gy)), device_id_type=MESH)
    for off in range(1, n_gx):
        pl.semaphore_signal(barrier, inc=1, device_id=(lax.rem(gx + off, n_gx), gy), device_id_type=MESH)

    def loads(c):
        cols = pl.ds(pl.multiple_of(c * width, LANES), width)
        return (
            pltpu.make_async_copy(policy_hbm.at[:, :, cols], policy.at[c], load_sem.at[0, c]),
            pltpu.make_async_copy(anchor_hbm.at[:, :, cols], anchor.at[c], load_sem.at[1, c]),
        )

    for c in range(CHUNKS):
        for copy in loads(c):
            copy.start()

    sublane = lax.broadcasted_iota(jnp.int32, (slots, slots), 0)
    lane = lax.broadcasted_iota(jnp.int32, (slots, slots), 1)
    column = lax.broadcasted_iota(jnp.int32, (slots, LANES), 1)
    local_tokens = jnp.sum(len_ref[...].astype(jnp.float32))
    for m in range(members_dev):
        seq_len = len_ref[m : m + 1, :].astype(jnp.float32)
        reward = reward_ref[m : m + 1, :].astype(jnp.float32) * 0.25
        match = sublane == lax.rem(prompt_ref[m : m + 1, :], slots)
        onehot[m] = jnp.where(match, 1.0, 0.0).astype(jnp.bfloat16)
        len_col[m] = jnp.broadcast_to(
            jnp.sum(jnp.where(sublane == lane, seq_len, 0.0), axis=1, keepdims=True), (slots, LANES)
        )
        sorted_len = jnp.sum(jnp.where(match, seq_len, 0.0), axis=1, keepdims=True)
        sorted_reward = jnp.sum(jnp.where(match, reward, 0.0), axis=1, keepdims=True)
        heads_send[m] = jnp.where(
            column == 0, sorted_len, jnp.where(column == 1, sorted_reward, local_tokens)
        )
    sum_policy[...] = jnp.zeros_like(sum_policy)
    sum_kl[...] = jnp.zeros_like(sum_kl)

    def compute(c):
        for copy in loads(c):
            copy.wait()
        positions = (lax.broadcasted_iota(jnp.int32, (slots, width), 1) + c * width).astype(jnp.float32)
        for m in range(members_dev):
            pol = policy[c, m]
            log_ratio = anchor[c, m] - pol
            ratio = jnp.exp(log_ratio)
            valid = positions < len_col[m][:, :1]
            sum_policy[m] += folded(jnp.where(valid, pol, 0.0))
            sum_kl[m] += folded(jnp.where(valid, kl_weight * (ratio - log_ratio - 1.0), 0.0))
            sendbuf[c, m] = permuted(onehot[m], kl_weight * (1.0 - ratio))

    def rows_of(device):
        return pl.ds(pl.multiple_of(device * part, part), part)

    my_members = pl.ds(gy * members_dev, members_dev)

    def sends(c, offs):
        cols = pl.ds(pl.multiple_of(c * width, LANES), width)
        copies = []
        for off in offs:
            peer = partner(gy, off, n_gy)
            copies.append(
                pltpu.make_async_remote_copy(
                    src_ref=sendbuf.at[c, :, rows_of(peer), :],
                    dst_ref=raw_hbm.at[my_members, :, cols],
                    send_sem=send_sem.at[off - 1],
                    recv_sem=recv_sem.at[off - 1],
                    device_id=(gx, peer),
                    device_id_type=MESH,
                )
            )
        return copies

    def own(c):
        cols = pl.ds(pl.multiple_of(c * width, LANES), width)
        return pltpu.make_async_copy(
            sendbuf.at[c, :, rows_of(gy), :], raw_hbm.at[my_members, :, cols], own_sem.at[c]
        )

    def small_sends(src, dst, send, recv):
        copies = []
        for off in range(1, n_gy):
            peer = partner(gy, off, n_gy)
            copies.append(
                pltpu.make_async_remote_copy(
                    src_ref=src.at[:, rows_of(peer), :],
                    dst_ref=dst.at[my_members],
                    send_sem=send.at[off - 1],
                    recv_sem=recv.at[off - 1],
                    device_id=(gx, peer),
                    device_id_type=MESH,
                )
            )
        copies.append(pltpu.make_async_copy(src.at[:, rows_of(gy), :], dst.at[my_members], send.at[n_gy - 1]))
        return copies

    def count_sends():
        return [
            pltpu.make_async_remote_copy(
                src_ref=counts.at[0],
                dst_ref=counts.at[off],
                send_sem=count_send_sem.at[off - 1],
                recv_sem=count_recv_sem.at[off - 1],
                device_id=(lax.rem(gx + off, n_gx), gy),
                device_id_type=MESH,
            )
            for off in range(1, n_gx)
        ]

    compute(0)
    pl.semaphore_wait(barrier, n_gy - 1 + n_gx - 1)
    head_copies = small_sends(heads_send, heads_recv, head_send_sem, head_recv_sem)
    for copy in head_copies:
        copy.start()

    def step(c, carry):
        for copy in sends(c - 1, near):
            copy.start()
        own(c - 1).start()
        compute(c)
        return carry

    lax.fori_loop(1, CHUNKS, step, 0)
    for copy in sends(CHUNKS - 1, near):
        copy.start()

    def far_step(c, carry):
        for copy in sends(c, far):
            copy.start()
        return carry

    lax.fori_loop(0, CHUNKS, far_step, 0)
    own(CHUNKS - 1).start()

    for m in range(members_dev):
        s1 = jnp.sum(permuted(onehot[m], sum_policy[m]), axis=1, keepdims=True)
        s2 = jnp.sum(permuted(onehot[m], sum_kl[m]), axis=1, keepdims=True)
        tails_send[m] = jnp.where(column == 0, s1, s2)
    for copy in head_copies:
        copy.wait()
    tokens = jnp.zeros((8, LANES), jnp.float32)
    for source in range(n_gy):
        tokens = tokens + heads_recv[source * members_dev, :8, :]
    counts[0] = tokens
    heads_ref[...] = heads_recv[...]
    tail_copies = small_sends(tails_send, tails_recv, tail_send_sem, tail_recv_sem)
    for copy in tail_copies:
        copy.start()
    count_copies = count_sends()
    for copy in count_copies:
        copy.start()
    for copy in count_copies:
        copy.wait()
    ntok_ref[...] = jnp.sum(counts[...], axis=0)
    for copy in tail_copies:
        copy.wait()
    tails_ref[...] = tails_recv[...]
    for c in range(CHUNKS):
        own(c).wait()
    for off in range(1, n_gy):
        source = partner(gy, off, n_gy)
        landed = raw_hbm.at[pl.ds(source * members_dev, members_dev)]
        pltpu.make_async_copy(landed, landed, recv_sem.at[off - 1]).wait()
        pltpu.make_async_copy(landed, landed, send_sem.at[off - 1]).wait()


def finish(samples, raw, heads, tails, ntok, grad, loss, adv, done, done_sem):
    members, part, seq = raw.shape
    tokens = ntok[:1, 2:3]
    total = jnp.sum(heads[...], axis=0)
    advantage = (members * heads[:, :, 1:2] - total[None, :, 1:2]) / (members - 1)
    positions = lax.broadcasted_iota(jnp.int32, (part, seq), 1).astype(jnp.float32)
    scale = samples * seq / tokens

    def store(k):
        return pltpu.make_async_copy(done.at[k], grad.at[k], done_sem.at[k])

    for k in range(members):
        done[k] = jnp.where(positions < heads[k, :, :1], raw[k] - advantage[k], 0.0) * scale
        if k > 0:
            store(k - 1).start()
    shape = (members, part, LANES)
    eye = lax.broadcasted_iota(jnp.int32, shape, 1) == lax.broadcasted_iota(jnp.int32, shape, 2)
    store(members - 1).start()
    value = (tails[:, :, 1:2] - advantage * tails[:, :, :1]) * (samples / tokens)[None]
    loss[...] = jnp.sum(jnp.where(eye, value, 0.0), axis=1)[:, :part]
    adv[...] = jnp.sum(jnp.where(eye, advantage, 0.0), axis=1)[:, :part]
    for k in range(members):
        store(k).wait()


def unpacked_body(n_gx, n_gy, policy_logp, anchor_logp, lengths, rewards, slot_prompt):
    members_dev, slots, seq = policy_logp.shape
    members, part = members_dev * n_gy, slots // n_gy
    f32 = jnp.float32
    chunked = (CHUNKS, members_dev, slots, seq // CHUNKS)
    small = (members, part, LANES)
    hbm_spec = pl.BlockSpec(memory_space=pltpu.HBM)
    vmem_spec = pl.BlockSpec(memory_space=pltpu.VMEM)
    dma = pltpu.SemaphoreType.DMA
    raw, heads, tails, ntok = pl.pallas_call(
        functools.partial(exchange, n_gx, n_gy),
        out_shape=(
            pltpu.VMEM((members, part, seq), f32),
            pltpu.VMEM(small, f32),
            pltpu.VMEM(small, f32),
            pltpu.VMEM((8, LANES), f32),
        ),
        in_specs=[hbm_spec, hbm_spec, vmem_spec, vmem_spec, vmem_spec],
        out_specs=(vmem_spec, vmem_spec, vmem_spec, vmem_spec),
        scratch_shapes=[
            pltpu.VMEM(chunked, f32),
            pltpu.VMEM(chunked, f32),
            pltpu.VMEM(chunked, f32),
            pltpu.VMEM((members_dev, slots, slots), jnp.bfloat16),
            pltpu.VMEM((members_dev, slots, LANES), f32),
            pltpu.VMEM((members_dev, slots, LANES), f32),
            pltpu.VMEM((members_dev, slots, LANES), f32),
            pltpu.VMEM((members_dev, slots, LANES), f32),
            pltpu.VMEM(small, f32),
            pltpu.VMEM((members_dev, slots, LANES), f32),
            pltpu.VMEM(small, f32),
            pltpu.VMEM((n_gx, 8, LANES), f32),
            dma((2, CHUNKS)),
            dma((n_gy - 1,)),
            dma((n_gy - 1,)),
            dma((CHUNKS,)),
            dma((n_gy,)),
            dma((n_gy - 1,)),
            dma((n_gy,)),
            dma((n_gy - 1,)),
            dma((n_gx - 1,)),
            dma((n_gx - 1,)),
        ],
        compiler_params=pltpu.CompilerParams(collective_id=1, has_side_effects=True, vmem_limit_bytes=56 * 2**20),
    )(policy_logp, anchor_logp, lengths, rewards, slot_prompt)
    samples = members * slots * n_gx
    return pl.pallas_call(
        functools.partial(finish, samples),
        out_shape=(
            jax.ShapeDtypeStruct((members, part, seq), f32),
            jax.ShapeDtypeStruct((members, part), f32),
            jax.ShapeDtypeStruct((members, part), f32),
        ),
        in_specs=[vmem_spec] * 4,
        out_specs=(hbm_spec, vmem_spec, vmem_spec),
        scratch_shapes=[pltpu.VMEM((members, part, seq), f32), dma((members,))],
        compiler_params=pltpu.CompilerParams(vmem_limit_bytes=32 * 2**20),
    )(raw, heads, tails, ntok)


def row_of(column):
    n = column.shape[0]
    eye = lax.broadcasted_iota(jnp.int32, (n, n), 0) == lax.broadcasted_iota(jnp.int32, (n, n), 1)
    return jnp.sum(jnp.where(eye, column, 0.0), axis=0, keepdims=True)


def row_sums(place, targets, values):
    out = None
    for target, value in zip(targets, values):
        here = jnp.sum(jnp.where(place == target, value, 0.0), axis=1, keepdims=True)
        out = here if out is None else out + here
    return out


def strip_spot(rank):
    first, second, third = rank < STRIPS, rank < 2 * STRIPS, rank < 3 * STRIPS
    strip = jnp.where(
        first, rank, jnp.where(second, 2 * STRIPS - 1 - rank, jnp.where(third, rank - 2 * STRIPS, 4 * STRIPS - 1 - rank))
    )
    return jnp.where(first, 0.0, jnp.where(second, 3.0, jnp.where(third, 2.0, 1.0))) * STRIPS + strip


def strip_plan(len_row, len_column, group_row, group_column, index_row, index_column, n_groups, seq):
    rows = ROLES * STRIPS
    key_row = group_row * ((seq + 1) * rows) + len_row * rows + index_row
    key_column = group_column * ((seq + 1) * rows) + len_column * rows + index_column
    above_row = jnp.sum(jnp.where(key_column > key_row, 1.0, 0.0), axis=0, keepdims=True)
    above_column = jnp.sum(jnp.where(key_row > key_column, 1.0, 0.0), axis=1, keepdims=True)
    return (
        strip_spot(above_row - rows * (n_groups - 1 - group_row)),
        strip_spot(above_column - rows * (n_groups - 1 - group_column)),
    )


def tail_blocks(lens):
    return jnp.floor((lens + (LANES - 1)) * (1.0 / LANES)) - HEAD_BLOCKS


def shift_bits(count):
    shift = count.astype(jnp.int32)
    return [(lax.shift_right_logical(shift, k) & 1) == 1 for k in range(SHIFTS)]


def shifted_up(blocks, bits, reach):
    for k in range(SHIFTS):
        step, n = 2**k, len(blocks)
        moved = []
        for p in range(min(n + step, reach)):
            if p < step:
                moved.append(blocks[p])
            elif p >= n:
                moved.append(blocks[p - step])
            else:
                moved.append(jnp.where(bits[k], blocks[p - step], blocks[p]))
        blocks = moved
    return blocks


def shifted_down(blocks, bits, count):
    for k in reversed(range(SHIFTS)):
        step = 2**k
        keep = min(len(blocks), count + step - 1)
        blocks = [
            jnp.where(bits[k], blocks[p + step], blocks[p]) if p + step < len(blocks) else blocks[p] for p in range(keep)
        ]
    return blocks


def peer_of(index, off, count):
    out, bit = 0, 1
    while bit < count:
        a, b = lax.rem(index // bit, 2), lax.rem(off // bit, 2)
        out = out + bit * (a + b - 2 * a * b)
        bit *= 2
    return out


def packed_exchange(
    n_gx, n_gy, policy_hbm, anchor_hbm, len_hbm, reward_hbm, prompt_hbm,
    done, loss_ref, adv_ref, over_ref,
    policy, anchor, len_ref, reward_ref, prompt_ref, onehot, ordered, got, heads_in, sendbuf, recvbuf, roles,
    deal, undeal, cnt, rcnt, len_col, sum_policy, sum_kl, len_rows, adv_rows,
    info_send, info_got, info_recv, tails_send, tails_recv, counts, needs,
    small_sem, load_sem, give_send_sem, give_recv_sem, first_send_sem, first_recv_sem, strip_send_sem, strip_recv_sem,
    info_send_sem, info_recv_sem, tail_send_sem, tail_recv_sem, count_send_sem, count_recv_sem, need_send_sem, need_recv_sem,
):
    gx, gy = lax.axis_index("gx"), lax.axis_index("gy")
    core, chip = lax.rem(gy, 2), gy // 2
    mate = chip * 2 + 1 - core
    members_dev, slots, seq = policy_hbm.shape
    members, part = members_dev * n_gy, slots // n_gy
    chips = n_gy // 2
    width = seq // CHUNKS
    nblocks = seq // LANES - HEAD_BLOCKS
    rows = members_dev * part
    pool = 2 * rows
    total_rows = chips * pool
    samples = members * slots * n_gx
    info_lane, fill_lane = 16, 17
    f32 = jnp.float32

    small_loads = [
        pltpu.make_async_copy(src, dst, small_sem.at[k])
        for k, (src, dst) in enumerate(((len_hbm, len_ref), (prompt_hbm, prompt_ref), (reward_hbm, reward_ref)))
    ]
    for copy in small_loads:
        copy.start()

    def loads(c):
        cols = pl.ds(pl.multiple_of(c * width, LANES), width)
        return (
            pltpu.make_async_copy(policy_hbm.at[:, :, cols], policy.at[c], load_sem.at[0, c]),
            pltpu.make_async_copy(anchor_hbm.at[:, :, cols], anchor.at[c], load_sem.at[1, c]),
        )

    for copy in loads(0):
        copy.start()
    barrier = pltpu.get_barrier_semaphore()
    for off in range(1, n_gy):
        pl.semaphore_signal(barrier, inc=1, device_id=(gx, partner(gy, off, n_gy)), device_id_type=MESH)
    for off in range(1, n_gx):
        pl.semaphore_signal(barrier, inc=1, device_id=(lax.rem(gx + off, n_gx), gy), device_id_type=MESH)
    for c in range(1, CHUNKS):
        for copy in loads(c):
            copy.start()
    for copy in small_loads:
        copy.wait()

    lens = [len_ref[m : m + 1, :].astype(f32) for m in range(members_dev)]
    targets = []
    for m in range(members_dev):
        spot = lax.rem(prompt_ref[m : m + 1, :], slots)
        device = spot // part
        other = lax.rem(device + core, 2)
        target = (other * chips + device // 2) * rows + m * part + spot - device * part
        targets.append(target.astype(f32))
    place = lax.broadcasted_iota(jnp.int32, (total_rows, slots), 0).astype(f32)
    for m in range(members_dev):
        onehot[:, m * slots : (m + 1) * slots] = jnp.where(place == targets[m], 1.0, 0.0).astype(jnp.bfloat16)

    def put_in_order(c):
        for copy in loads(c):
            copy.wait()
        values = kl_weight * (1.0 - jnp.exp(anchor[c] - policy[c]))
        out = permuted(onehot[...], values.reshape(members_dev * slots, width))
        cols = pl.ds(pl.multiple_of(c * width, LANES), width)
        ordered[:, :, :, cols] = out.reshape(2, chips, rows, width)

    def give(c):
        cols = pl.ds(pl.multiple_of(c * width, LANES), width)
        return pltpu.make_async_remote_copy(
            src_ref=ordered.at[1, :, :, cols],
            dst_ref=got.at[:, :, cols],
            send_sem=give_send_sem,
            recv_sem=give_recv_sem,
            device_id=(gx, mate),
            device_id_type=MESH,
        )

    def first_send(off):
        peer = partner(gy, off, n_gy)
        return pltpu.make_async_remote_copy(
            src_ref=ordered.at[off % 2, peer // 2, :, pl.ds(0, width)],
            dst_ref=heads_in.at[gy],
            send_sem=first_send_sem.at[off - 2],
            recv_sem=first_recv_sem.at[off - 2],
            device_id=(gx, peer),
            device_id_type=MESH,
        )

    put_in_order(0)
    pl.semaphore_wait(barrier, n_gy - 1 + n_gx - 1)
    first_copies = [first_send(off) for off in FIRST_ORDER]
    for copy in first_copies:
        copy.start()
    give(0).start()

    tile_lane = lax.broadcasted_iota(jnp.int32, (n_gy, 8, LANES), 2)
    groups = rows // 8
    local_tokens = sum(jnp.sum(length) for length in lens)

    def tiles(columns, base):
        out = base
        for f, column in enumerate(columns):
            split = column.reshape(n_gy, groups, 8, 1)
            for g in range(groups):
                out = jnp.where(tile_lane == g * 4 + f, split[:, g], out)
        return out

    def column_in(tile, f):
        parts = [tile[:, :, g * 4 + f : g * 4 + f + 1][:, None] for g in range(groups)]
        return jnp.concatenate(parts, axis=1)

    own_len = row_sums(place, targets, lens)
    rewards = [reward_ref[m : m + 1, :].astype(f32) * 0.25 for m in range(members_dev)]
    own_reward = row_sums(place, targets, rewards)
    info_send[...] = tiles((own_len, own_reward), jnp.broadcast_to(local_tokens, (n_gy, 8, LANES)))

    def tile_sends(src, dst, send, recv, offs):
        copies = []
        for off in offs:
            peer = partner(gy, off, n_gy)
            copies.append(
                pltpu.make_async_remote_copy(
                    src_ref=src.at[off % 2 * chips + peer // 2],
                    dst_ref=dst.at[gy],
                    send_sem=send.at[off - 1],
                    recv_sem=recv.at[off - 1],
                    device_id=(gx, peer),
                    device_id_type=MESH,
                )
            )
        return copies

    mate_info = pltpu.make_async_remote_copy(
        src_ref=info_send.at[pl.ds(chips, chips)],
        dst_ref=info_got,
        send_sem=info_send_sem.at[0],
        recv_sem=info_recv_sem.at[0],
        device_id=(gx, mate),
        device_id_type=MESH,
    )
    info_copies = [mate_info] + tile_sends(info_send, info_recv, info_send_sem, info_recv_sem, range(2, n_gy))
    for copy in info_copies:
        copy.start()

    def order_step(c, carry):
        put_in_order(c)
        give(c).start()
        return carry

    lax.fori_loop(1, CHUNKS, order_step, 0)

    mate_info.wait()
    pair_lens = jnp.concatenate(
        [own_len[: chips * rows].reshape(chips, 1, rows, 1), column_in(info_got[...], 0).reshape(chips, 1, rows, 1)], axis=1
    ).reshape(total_rows, 1)
    row = lax.broadcasted_iota(jnp.int32, (1, total_rows), 1)
    column = lax.broadcasted_iota(jnp.int32, (total_rows, 1), 0)

    def pair_index(i):
        inside = lax.rem(i, pool)
        return (lax.rem(inside // rows + core, 2) * rows + lax.rem(inside, rows)).astype(f32)

    pair_row = row_of(pair_lens)
    spot_row, _ = strip_plan(
        pair_row, pair_lens, (row // pool).astype(f32), (column // pool).astype(f32), pair_index(row), pair_index(column),
        chips, seq,
    )
    wide = lax.broadcasted_iota(jnp.int32, (total_rows, total_rows), 0).astype(f32)

    def strip_counts(spots, lens_row):
        return row_sums(wide, [spots + (row // pool).astype(f32) * pool], [tail_blocks(lens_row)])

    pair_counts = strip_counts(spot_row, pair_row)
    cnt[...] = jnp.broadcast_to(pair_counts, cnt.shape)
    fill = jnp.sum(pair_counts.reshape(chips, ROLES, STRIPS, 1), axis=1)
    sent_chip = lax.broadcasted_iota(jnp.int32, (chips, STRIPS, 1), 0) != chip
    local_fill = jnp.max(jnp.where(sent_chip, fill, 0.0))
    square = lax.broadcasted_iota(jnp.int32, (pool, pool), 0).astype(f32)
    for s in range(chips):
        deal[s] = jnp.where(square == spot_row[:, s * pool : (s + 1) * pool], 1.0, 0.0).astype(jnp.bfloat16)
    pltpu.make_async_copy(got, got, give_recv_sem).wait()

    def strip_send(t, there):
        return pltpu.make_async_remote_copy(
            src_ref=sendbuf.at[there],
            dst_ref=recvbuf.at[chip],
            send_sem=strip_send_sem.at[t],
            recv_sem=strip_recv_sem.at[t],
            device_id=(gx, there * 2 + core),
            device_id_type=MESH,
        )

    reach = 2 * nblocks

    def pack(there):
        for c in range(1, CHUNKS):
            both = jnp.concatenate(
                [ordered[0, there, :, c * width : (c + 1) * width], got[there, :, c * width : (c + 1) * width]], axis=0
            )
            roles[:, (c - 1) * width : c * width] = permuted(deal[there], both)
        for half in range(STRIPS // 8):

            def count(role):
                at = there * pool + role * STRIPS + half * 8
                return cnt[pl.ds(pl.multiple_of(at, 8), 8), :]

            def blocks(role):
                at = role * STRIPS + half * 8
                return [roles[at : at + 8, j * LANES : (j + 1) * LANES] for j in range(nblocks)]

            def side(outer, inner):
                n = count(outer)
                behind = shifted_up(blocks(inner), shift_bits(n), reach)
                near_end = blocks(outer)
                return [jnp.where(n > p, near_end[p], behind[p]) for p in range(nblocks)] + behind[nblocks:]

            left, right = side(0, 1), side(3, 2)
            left_n = count(0) + count(1)
            for p in range(STRIP_BLOCKS):
                q = STRIP_BLOCKS - 1 - p
                if q >= reach:
                    value = left[p]
                elif p >= reach:
                    value = right[q]
                else:
                    value = jnp.where(left_n > p, left[p], right[q])
                sendbuf[there, half * 8 : half * 8 + 8, p * LANES : (p + 1) * LANES] = value

    def near_step(t, carry):
        there = peer_of(chip, t + 1, chips)
        pack(there)
        strip_send(t, there).start()
        return carry

    lax.fori_loop(0, 2, near_step, 0)

    info_recv[gy] = info_send[chip]
    for copy in info_copies[1:]:
        copy.wait()
    info_recv[mate] = info_got[chip]
    arrived = info_recv[...]
    counts[0] = jnp.sum(arrived, axis=0)

    def axis_sends(buf, send, recv):
        return [
            pltpu.make_async_remote_copy(
                src_ref=buf.at[0],
                dst_ref=buf.at[off],
                send_sem=send.at[off - 1],
                recv_sem=recv.at[off - 1],
                device_id=(lax.rem(gx + off, n_gx), gy),
                device_id_type=MESH,
            )
            for off in range(1, n_gx)
        ]

    count_copies = axis_sends(counts, count_send_sem, count_recv_sem)
    for copy in count_copies:
        copy.start()

    eye = lax.broadcasted_iota(jnp.int32, (slots, slots), 0) == lax.broadcasted_iota(jnp.int32, (slots, slots), 1)
    for m in range(members_dev):
        len_col[m] = jnp.broadcast_to(jnp.sum(jnp.where(eye, lens[m], 0.0), axis=1, keepdims=True), (slots, LANES))
    sum_policy[...] = jnp.zeros_like(sum_policy)
    sum_kl[...] = jnp.zeros_like(sum_kl)

    def sum_step(c, carry):
        positions = (lax.broadcasted_iota(jnp.int32, (slots, width), 1) + c * width).astype(f32)
        for m in range(members_dev):
            pol = policy[c, m]
            log_ratio = anchor[c, m] - pol
            ratio = jnp.exp(log_ratio)
            valid = positions < len_col[m][:, :1]
            sum_policy[m] += folded(jnp.where(valid, pol, 0.0))
            sum_kl[m] += folded(jnp.where(valid, kl_weight * (ratio - log_ratio - 1.0), 0.0))
        return carry

    lax.fori_loop(0, CHUNKS, sum_step, 0)
    sums = []
    for buf in (sum_policy, sum_kl):
        per_member = [row_of(jnp.sum(buf[m], axis=1, keepdims=True)) for m in range(members_dev)]
        sums.append(row_sums(place, targets, per_member))
    tails_send[...] = tiles(sums, jnp.broadcast_to(local_fill, (n_gy, 8, LANES)))
    tail_copies = tile_sends(tails_send, tails_recv, tail_send_sem, tail_recv_sem, range(1, n_gy))
    for copy in tail_copies:
        copy.start()
    tails_recv[gy] = tails_send[chip]

    far = peer_of(chip, chips - 1, chips)
    pack(far)
    strip_send(chips - 2, far).start()

    for copy in count_copies:
        copy.wait()
    tokens = counts[0]
    for off in range(1, n_gx):
        tokens = tokens + counts[off]
    ntok = tokens[:1, info_lane : info_lane + 1]
    scale = samples * seq / ntok
    got_len = column_in(arrived, 0).reshape(total_rows, 1)
    got_row = row_of(got_len)
    reward = column_in(arrived, 1).reshape(members, part, 1)
    advantage = (members * reward - jnp.sum(reward, axis=0)[None]) / (members - 1)
    adv_rows[...] = jnp.broadcast_to(advantage, adv_rows.shape)
    len_rows[...] = jnp.broadcast_to(got_len.reshape(members, part, 1), len_rows.shape)
    got_spot_row, got_spot = strip_plan(
        got_row, got_len, (row // pool).astype(f32), (column // pool).astype(f32),
        lax.rem(row, pool).astype(f32), lax.rem(column, pool).astype(f32), chips, seq,
    )
    rcnt[...] = jnp.broadcast_to(strip_counts(got_spot_row, got_row), rcnt.shape)
    pick = got_spot == lax.broadcasted_iota(jnp.int32, (total_rows, LANES), 1).astype(f32)
    undeal[...] = jnp.where(pick, 1.0, 0.0).astype(jnp.bfloat16).reshape(chips, pool, LANES)
    lane_width = lax.broadcasted_iota(jnp.int32, (part, width), 1).astype(f32)

    def finish_rows(k, start, value):
        value = (value - adv_rows[k][:, :1]) * scale
        valid = lane_width < len_rows[k][:, :1] - start
        done[k, :, start : start + width] = jnp.where(valid, value, 0.0)

    def own_step(which, source):
        for m in range(members_dev):
            for c in range(CHUNKS):
                finish_rows(source * members_dev + m, c * width, which(m * part, c * width))

    own_step(lambda r, s: ordered[0, chip, r : r + part, s : s + width], gy)
    own_step(lambda r, s: got[chip, r : r + part, s : s + width], mate)

    def first_wait(off):
        landed = heads_in.at[0]
        pltpu.make_async_copy(landed, landed, first_recv_sem.at[off - 2]).wait()

    def first_step(off, carry):
        first_wait(off)
        source = peer_of(gy, off, n_gy)
        for m in range(members_dev):
            finish_rows(source * members_dev + m, 0, heads_in[source, m * part : (m + 1) * part, :])
        return carry

    lax.fori_loop(2, n_gy, first_step, 0)

    def unpack(t):
        there = peer_of(chip, t + 1, chips)
        landed = recvbuf.at[0]
        pltpu.make_async_copy(landed, landed, strip_recv_sem.at[t]).wait()
        for half in range(STRIPS // 8):

            def count(role):
                at = there * pool + role * STRIPS + half * 8
                return rcnt[pl.ds(pl.multiple_of(at, 8), 8), :]

            def block(p):
                return recvbuf[there, half * 8 : half * 8 + 8, p * LANES : (p + 1) * LANES]

            for outer, inner, at in ((0, 1, lambda p: p), (3, 2, lambda p: STRIP_BLOCKS - 1 - p)):
                top = outer * STRIPS + half * 8
                for j in range(nblocks):
                    roles[top : top + 8, j * LANES : (j + 1) * LANES] = block(at(j))
                behind = [block(at(p)) for p in range(reach)]
                behind = shifted_down(behind, shift_bits(count(outer)), nblocks)
                top = inner * STRIPS + half * 8
                for j in range(nblocks):
                    roles[top : top + 8, j * LANES : (j + 1) * LANES] = behind[j]
        order = undeal[there][:, :pool]
        for c in range(1, CHUNKS):
            out = permuted(order, roles[:, (c - 1) * width : c * width])
            for r in range(2 * members_dev):
                finish_rows(there * 2 * members_dev + r, c * width, out[r * part : (r + 1) * part])

    def unpack_step(t, carry):
        unpack(t)
        return carry

    lax.fori_loop(0, 2, unpack_step, 0)

    for copy in tail_copies:
        copy.wait()
    ends = tails_recv[...]
    needs[0] = jnp.max(ends, axis=0)
    need_copies = axis_sends(needs, need_send_sem, need_recv_sem)
    for copy in need_copies:
        copy.start()
    first_sum = column_in(ends, 0).reshape(members, part, 1)
    second_sum = column_in(ends, 1).reshape(members, part, 1)
    value = (second_sum - advantage * first_sum) * (samples / ntok)[None]
    shape = (members, part, LANES)
    spread = lax.broadcasted_iota(jnp.int32, shape, 1) == lax.broadcasted_iota(jnp.int32, shape, 2)
    loss_ref[...] = jnp.sum(jnp.where(spread, value, 0.0), axis=1)[:, :part]
    adv_ref[...] = jnp.sum(jnp.where(spread, advantage, 0.0), axis=1)[:, :part]
    for copy in need_copies:
        copy.wait()
    fullest = needs[0]
    for off in range(1, n_gx):
        fullest = jnp.maximum(fullest, needs[off])
    over_ref[0, 0] = (jnp.max(fullest[:, fill_lane : fill_lane + 1]) > STRIP_BLOCKS).astype(jnp.int32)
    for copy in first_copies:
        copy.wait_send()
    pltpu.make_async_copy(got, got, give_send_sem).wait()

    unpack(chips - 2)
    for t in range(chips - 1):
        sent = sendbuf.at[0]
        pltpu.make_async_copy(sent, sent, strip_send_sem.at[t]).wait()


def store(done, loss, adv, grad, loss_out, adv_out, sem):
    copies = [
        pltpu.make_async_copy(src, dst, sem.at[k])
        for k, (src, dst) in enumerate(((done, grad), (loss, loss_out), (adv, adv_out)))
    ]
    for copy in copies:
        copy.start()
    for copy in copies:
        copy.wait()


def packed_body(n_gx, n_gy, policy_logp, anchor_logp, lengths, rewards, slot_prompt):
    members_dev, slots, seq = policy_logp.shape
    members, part = members_dev * n_gy, slots // n_gy
    f32, bf16 = jnp.float32, jnp.bfloat16
    chips, rows = n_gy // 2, members_dev * part
    pool = 2 * rows
    width = seq // CHUNKS
    chunked = (CHUNKS, members_dev, slots, width)
    strips = (chips, STRIPS, STRIP_BLOCKS * LANES)
    per_slot = (members_dev, slots, LANES)
    per_sample = (members, part, LANES)
    tile = (n_gy, 8, LANES)
    hbm_spec = pl.BlockSpec(memory_space=pltpu.HBM)
    vmem_spec = pl.BlockSpec(memory_space=pltpu.VMEM)
    dma = pltpu.SemaphoreType.DMA
    done, loss, adv, over = pl.pallas_call(
        functools.partial(packed_exchange, n_gx, n_gy),
        out_shape=(
            pltpu.VMEM((members, part, seq), f32),
            pltpu.VMEM((members, part), f32),
            pltpu.VMEM((members, part), f32),
            jax.ShapeDtypeStruct((1, 1), jnp.int32),
        ),
        in_specs=[hbm_spec] * 5,
        out_specs=(vmem_spec,) * 3 + (pl.BlockSpec(memory_space=pltpu.SMEM),),
        scratch_shapes=[
            pltpu.VMEM(chunked, f32),
            pltpu.VMEM(chunked, f32),
            pltpu.VMEM((members_dev, slots), jnp.int32),
            pltpu.VMEM((members_dev, slots), jnp.int32),
            pltpu.VMEM((members_dev, slots), jnp.int32),
            pltpu.VMEM((2 * chips * rows, members_dev * slots), bf16),
            pltpu.VMEM((2, chips, rows, seq), f32),
            pltpu.VMEM((chips, rows, seq), f32),
            pltpu.VMEM((n_gy, rows, width), f32),
            pltpu.VMEM(strips, f32),
            pltpu.VMEM(strips, f32),
            pltpu.VMEM((pool, seq - width), f32),
            pltpu.VMEM((chips, pool, pool), bf16),
            pltpu.VMEM((chips, pool, LANES), bf16),
            pltpu.VMEM((chips * pool, LANES), f32),
            pltpu.VMEM((chips * pool, LANES), f32),
            pltpu.VMEM(per_slot, f32),
            pltpu.VMEM(per_slot, f32),
            pltpu.VMEM(per_slot, f32),
            pltpu.VMEM(per_sample, f32),
            pltpu.VMEM(per_sample, f32),
            pltpu.VMEM(tile, f32),
            pltpu.VMEM((chips, 8, LANES), f32),
            pltpu.VMEM(tile, f32),
            pltpu.VMEM(tile, f32),
            pltpu.VMEM(tile, f32),
            pltpu.VMEM((n_gx, 8, LANES), f32),
            pltpu.VMEM((n_gx, 8, LANES), f32),
            dma((3,)),
            dma((2, CHUNKS)),
            dma(()),
            dma(()),
            dma((n_gy - 2,)),
            dma((n_gy - 2,)),
            dma((chips - 1,)),
            dma((chips - 1,)),
            dma((n_gy - 1,)),
            dma((n_gy - 1,)),
            dma((n_gy - 1,)),
            dma((n_gy - 1,)),
            dma((n_gx - 1,)),
            dma((n_gx - 1,)),
            dma((n_gx - 1,)),
            dma((n_gx - 1,)),
        ],
        compiler_params=pltpu.CompilerParams(collective_id=0, has_side_effects=True, vmem_limit_bytes=56 * 2**20),
    )(policy_logp, anchor_logp, lengths, rewards, slot_prompt)

    def fits(policy_logp, anchor_logp, lengths, rewards, slot_prompt, done, loss, adv):
        small = jax.ShapeDtypeStruct((members, part), f32)
        return tuple(pl.pallas_call(
            store,
            out_shape=(jax.ShapeDtypeStruct((members, part, seq), f32), small, small),
            in_specs=[vmem_spec] * 3,
            out_specs=(hbm_spec,) * 3,
            scratch_shapes=[dma((3,))],
            compiler_params=pltpu.CompilerParams(vmem_limit_bytes=16 * 2**20),
        )(done, loss, adv))

    def overflows(policy_logp, anchor_logp, lengths, rewards, slot_prompt, done, loss, adv):
        return tuple(unpacked_body(n_gx, n_gy, policy_logp, anchor_logp, lengths, rewards, slot_prompt))

    return lax.cond(
        over[0, 0] > 0, overflows, fits,
        policy_logp, anchor_logp, lengths, rewards, slot_prompt, done, loss, adv,
    )


def body(n_gx, n_gy, *args):
    members_dev, slots, seq = args[0].shape
    pool = 2 * members_dev * slots // n_gy
    packs = n_gy == 8 and pool == ROLES * STRIPS and slots == LANES and seq == LANES * 32 and seq == CHUNKS * HEAD_BLOCKS * LANES
    return (packed_body if packs else unpacked_body)(n_gx, n_gy, *args)


def solution(mesh):
    placed = (P("gy", "gx", None), P("gy", "gx", None), P("gy", "gx"), P("gy", "gx"), P("gy", "gx"))
    return jax.shard_map(
        functools.partial(body, mesh.shape["gx"], mesh.shape["gy"]),
        mesh=mesh,
        in_specs=placed,
        out_specs=(P(None, ("gx", "gy"), None), P(None, ("gx", "gy")), P(None, ("gx", "gy"))),
        check_vma=False,
    )
```

```python
import functools

import jax
import jax.numpy as jnp
from jax import lax
from jax.experimental import pallas as pl
from jax.experimental.pallas import tpu as pltpu
from jax.sharding import PartitionSpec as P

kl_weight = 0.1
LANES = 128
CHUNKS = 8
MESH = pl.DeviceIdType.MESH
ROLES = 4
STRIPS = 16
SHIFTS = 5
HEAD_BLOCKS = 4
STRIP_BLOCKS = 74
FIRST_ORDER = (2, 4, 3, 5, 6, 7)


def partner(index, off, count):
    out, bit = index, 1
    while bit < count:
        if off & bit:
            out = out + bit - 2 * bit * lax.rem(index // bit, 2)
        bit *= 2
    return out


def offsets_by_distance(count):
    far = max(bin(off // 2).count("1") for off in range(1, count))
    near = [off for off in range(1, count) if bin(off // 2).count("1") < far]
    return near, [off for off in range(1, count) if off not in near]


def permuted(onehot, rows):
    high = rows.astype(jnp.bfloat16)
    rest = rows - high.astype(jnp.float32)
    middle = rest.astype(jnp.bfloat16)
    low = (rest - middle.astype(jnp.float32)).astype(jnp.bfloat16)
    dot = functools.partial(jnp.dot, preferred_element_type=jnp.float32)
    return dot(onehot, high) + dot(onehot, middle) + dot(onehot, low)


def folded(x):
    out = x[:, :LANES]
    for start in range(LANES, x.shape[1], LANES):
        out = out + x[:, start : start + LANES]
    return out


def exchange(
    n_gx, n_gy, policy_hbm, anchor_hbm, len_ref, reward_ref, prompt_ref,
    raw_hbm, heads_ref, tails_ref, ntok_ref,
    policy, anchor, sendbuf, onehot, len_col, sum_policy, sum_kl,
    heads_send, heads_recv, tails_send, tails_recv, counts,
    load_sem, send_sem, recv_sem, own_sem,
    head_send_sem, head_recv_sem, tail_send_sem, tail_recv_sem, count_send_sem, count_recv_sem,
):
    gx, gy = lax.axis_index("gx"), lax.axis_index("gy")
    members_dev, slots, seq = policy_hbm.shape
    part = slots // n_gy
    width = seq // CHUNKS

    near, far = offsets_by_distance(n_gy)
    barrier = pltpu.get_barrier_semaphore()
    for off in range(1, n_gy):
        pl.semaphore_signal(barrier, inc=1, device_id=(gx, partner(gy, off, n_gy)), device_id_type=MESH)
    for off in range(1, n_gx):
        pl.semaphore_signal(barrier, inc=1, device_id=(lax.rem(gx + off, n_gx), gy), device_id_type=MESH)

    def loads(c):
        cols = pl.ds(pl.multiple_of(c * width, LANES), width)
        return (
            pltpu.make_async_copy(policy_hbm.at[:, :, cols], policy.at[c], load_sem.at[0, c]),
            pltpu.make_async_copy(anchor_hbm.at[:, :, cols], anchor.at[c], load_sem.at[1, c]),
        )

    for c in range(CHUNKS):
        for copy in loads(c):
            copy.start()

    sublane = lax.broadcasted_iota(jnp.int32, (slots, slots), 0)
    lane = lax.broadcasted_iota(jnp.int32, (slots, slots), 1)
    column = lax.broadcasted_iota(jnp.int32, (slots, LANES), 1)
    local_tokens = jnp.sum(len_ref[...].astype(jnp.float32))
    for m in range(members_dev):
        seq_len = len_ref[m : m + 1, :].astype(jnp.float32)
        reward = reward_ref[m : m + 1, :].astype(jnp.float32) * 0.25
        match = sublane == lax.rem(prompt_ref[m : m + 1, :], slots)
        onehot[m] = jnp.where(match, 1.0, 0.0).astype(jnp.bfloat16)
        len_col[m] = jnp.broadcast_to(
            jnp.sum(jnp.where(sublane == lane, seq_len, 0.0), axis=1, keepdims=True), (slots, LANES)
        )
        sorted_len = jnp.sum(jnp.where(match, seq_len, 0.0), axis=1, keepdims=True)
        sorted_reward = jnp.sum(jnp.where(match, reward, 0.0), axis=1, keepdims=True)
        heads_send[m] = jnp.where(
            column == 0, sorted_len, jnp.where(column == 1, sorted_reward, local_tokens)
        )
    sum_policy[...] = jnp.zeros_like(sum_policy)
    sum_kl[...] = jnp.zeros_like(sum_kl)

    def compute(c):
        for copy in loads(c):
            copy.wait()
        positions = (lax.broadcasted_iota(jnp.int32, (slots, width), 1) + c * width).astype(jnp.float32)
        for m in range(members_dev):
            pol = policy[c, m]
            log_ratio = anchor[c, m] - pol
            ratio = jnp.exp(log_ratio)
            valid = positions < len_col[m][:, :1]
            sum_policy[m] += folded(jnp.where(valid, pol, 0.0))
            sum_kl[m] += folded(jnp.where(valid, kl_weight * (ratio - log_ratio - 1.0), 0.0))
            sendbuf[c, m] = permuted(onehot[m], kl_weight * (1.0 - ratio))

    def rows_of(device):
        return pl.ds(pl.multiple_of(device * part, part), part)

    my_members = pl.ds(gy * members_dev, members_dev)

    def sends(c, offs):
        cols = pl.ds(pl.multiple_of(c * width, LANES), width)
        copies = []
        for off in offs:
            peer = partner(gy, off, n_gy)
            copies.append(
                pltpu.make_async_remote_copy(
                    src_ref=sendbuf.at[c, :, rows_of(peer), :],
                    dst_ref=raw_hbm.at[my_members, :, cols],
                    send_sem=send_sem.at[off - 1],
                    recv_sem=recv_sem.at[off - 1],
                    device_id=(gx, peer),
                    device_id_type=MESH,
                )
            )
        return copies

    def own(c):
        cols = pl.ds(pl.multiple_of(c * width, LANES), width)
        return pltpu.make_async_copy(
            sendbuf.at[c, :, rows_of(gy), :], raw_hbm.at[my_members, :, cols], own_sem.at[c]
        )

    def small_sends(src, dst, send, recv):
        copies = []
        for off in range(1, n_gy):
            peer = partner(gy, off, n_gy)
            copies.append(
                pltpu.make_async_remote_copy(
                    src_ref=src.at[:, rows_of(peer), :],
                    dst_ref=dst.at[my_members],
                    send_sem=send.at[off - 1],
                    recv_sem=recv.at[off - 1],
                    device_id=(gx, peer),
                    device_id_type=MESH,
                )
            )
        copies.append(pltpu.make_async_copy(src.at[:, rows_of(gy), :], dst.at[my_members], send.at[n_gy - 1]))
        return copies

    def count_sends():
        return [
            pltpu.make_async_remote_copy(
                src_ref=counts.at[0],
                dst_ref=counts.at[off],
                send_sem=count_send_sem.at[off - 1],
                recv_sem=count_recv_sem.at[off - 1],
                device_id=(lax.rem(gx + off, n_gx), gy),
                device_id_type=MESH,
            )
            for off in range(1, n_gx)
        ]

    compute(0)
    pl.semaphore_wait(barrier, n_gy - 1 + n_gx - 1)
    head_copies = small_sends(heads_send, heads_recv, head_send_sem, head_recv_sem)
    for copy in head_copies:
        copy.start()

    def step(c, carry):
        for copy in sends(c - 1, near):
            copy.start()
        own(c - 1).start()
        compute(c)
        return carry

    lax.fori_loop(1, CHUNKS, step, 0)
    for copy in sends(CHUNKS - 1, near):
        copy.start()

    def far_step(c, carry):
        for copy in sends(c, far):
            copy.start()
        return carry

    lax.fori_loop(0, CHUNKS, far_step, 0)
    own(CHUNKS - 1).start()

    for m in range(members_dev):
        s1 = jnp.sum(permuted(onehot[m], sum_policy[m]), axis=1, keepdims=True)
        s2 = jnp.sum(permuted(onehot[m], sum_kl[m]), axis=1, keepdims=True)
        tails_send[m] = jnp.where(column == 0, s1, s2)
    for copy in head_copies:
        copy.wait()
    tokens = jnp.zeros((8, LANES), jnp.float32)
    for source in range(n_gy):
        tokens = tokens + heads_recv[source * members_dev, :8, :]
    counts[0] = tokens
    heads_ref[...] = heads_recv[...]
    tail_copies = small_sends(tails_send, tails_recv, tail_send_sem, tail_recv_sem)
    for copy in tail_copies:
        copy.start()
    count_copies = count_sends()
    for copy in count_copies:
        copy.start()
    for copy in count_copies:
        copy.wait()
    ntok_ref[...] = jnp.sum(counts[...], axis=0)
    for copy in tail_copies:
        copy.wait()
    tails_ref[...] = tails_recv[...]
    for c in range(CHUNKS):
        own(c).wait()
    for off in range(1, n_gy):
        source = partner(gy, off, n_gy)
        landed = raw_hbm.at[pl.ds(source * members_dev, members_dev)]
        pltpu.make_async_copy(landed, landed, recv_sem.at[off - 1]).wait()
        pltpu.make_async_copy(landed, landed, send_sem.at[off - 1]).wait()


def finish(samples, raw, heads, tails, ntok, grad, loss, adv, done, done_sem):
    members, part, seq = raw.shape
    tokens = ntok[:1, 2:3]
    total = jnp.sum(heads[...], axis=0)
    advantage = (members * heads[:, :, 1:2] - total[None, :, 1:2]) / (members - 1)
    positions = lax.broadcasted_iota(jnp.int32, (part, seq), 1).astype(jnp.float32)
    scale = samples * seq / tokens

    def store(k):
        return pltpu.make_async_copy(done.at[k], grad.at[k], done_sem.at[k])

    for k in range(members):
        done[k] = jnp.where(positions < heads[k, :, :1], raw[k] - advantage[k], 0.0) * scale
        if k > 0:
            store(k - 1).start()
    shape = (members, part, LANES)
    eye = lax.broadcasted_iota(jnp.int32, shape, 1) == lax.broadcasted_iota(jnp.int32, shape, 2)
    store(members - 1).start()
    value = (tails[:, :, 1:2] - advantage * tails[:, :, :1]) * (samples / tokens)[None]
    loss[...] = jnp.sum(jnp.where(eye, value, 0.0), axis=1)[:, :part]
    adv[...] = jnp.sum(jnp.where(eye, advantage, 0.0), axis=1)[:, :part]
    for k in range(members):
        store(k).wait()


def unpacked_body(n_gx, n_gy, policy_logp, anchor_logp, lengths, rewards, slot_prompt):
    members_dev, slots, seq = policy_logp.shape
    members, part = members_dev * n_gy, slots // n_gy
    f32 = jnp.float32
    chunked = (CHUNKS, members_dev, slots, seq // CHUNKS)
    small = (members, part, LANES)
    hbm_spec = pl.BlockSpec(memory_space=pltpu.HBM)
    vmem_spec = pl.BlockSpec(memory_space=pltpu.VMEM)
    dma = pltpu.SemaphoreType.DMA
    raw, heads, tails, ntok = pl.pallas_call(
        functools.partial(exchange, n_gx, n_gy),
        out_shape=(
            pltpu.VMEM((members, part, seq), f32),
            pltpu.VMEM(small, f32),
            pltpu.VMEM(small, f32),
            pltpu.VMEM((8, LANES), f32),
        ),
        in_specs=[hbm_spec, hbm_spec, vmem_spec, vmem_spec, vmem_spec],
        out_specs=(vmem_spec, vmem_spec, vmem_spec, vmem_spec),
        scratch_shapes=[
            pltpu.VMEM(chunked, f32),
            pltpu.VMEM(chunked, f32),
            pltpu.VMEM(chunked, f32),
            pltpu.VMEM((members_dev, slots, slots), jnp.bfloat16),
            pltpu.VMEM((members_dev, slots, LANES), f32),
            pltpu.VMEM((members_dev, slots, LANES), f32),
            pltpu.VMEM((members_dev, slots, LANES), f32),
            pltpu.VMEM((members_dev, slots, LANES), f32),
            pltpu.VMEM(small, f32),
            pltpu.VMEM((members_dev, slots, LANES), f32),
            pltpu.VMEM(small, f32),
            pltpu.VMEM((n_gx, 8, LANES), f32),
            dma((2, CHUNKS)),
            dma((n_gy - 1,)),
            dma((n_gy - 1,)),
            dma((CHUNKS,)),
            dma((n_gy,)),
            dma((n_gy - 1,)),
            dma((n_gy,)),
            dma((n_gy - 1,)),
            dma((n_gx - 1,)),
            dma((n_gx - 1,)),
        ],
        compiler_params=pltpu.CompilerParams(collective_id=1, has_side_effects=True, vmem_limit_bytes=56 * 2**20),
    )(policy_logp, anchor_logp, lengths, rewards, slot_prompt)
    samples = members * slots * n_gx
    return pl.pallas_call(
        functools.partial(finish, samples),
        out_shape=(
            jax.ShapeDtypeStruct((members, part, seq), f32),
            jax.ShapeDtypeStruct((members, part), f32),
            jax.ShapeDtypeStruct((members, part), f32),
        ),
        in_specs=[vmem_spec] * 4,
        out_specs=(hbm_spec, vmem_spec, vmem_spec),
        scratch_shapes=[pltpu.VMEM((members, part, seq), f32), dma((members,))],
        compiler_params=pltpu.CompilerParams(vmem_limit_bytes=32 * 2**20),
    )(raw, heads, tails, ntok)


def row_of(column):
    n = column.shape[0]
    eye = lax.broadcasted_iota(jnp.int32, (n, n), 0) == lax.broadcasted_iota(jnp.int32, (n, n), 1)
    return jnp.sum(jnp.where(eye, column, 0.0), axis=0, keepdims=True)


def row_sums(place, targets, values):
    out = None
    for target, value in zip(targets, values):
        here = jnp.sum(jnp.where(place == target, value, 0.0), axis=1, keepdims=True)
        out = here if out is None else out + here
    return out


def strip_spot(rank):
    first, second, third = rank < STRIPS, rank < 2 * STRIPS, rank < 3 * STRIPS
    strip = jnp.where(
        first, rank, jnp.where(second, 2 * STRIPS - 1 - rank, jnp.where(third, 3 * STRIPS - 1 - rank, rank - 3 * STRIPS))
    )
    role = jnp.where(first, 0.0, jnp.where(second, 3.0, jnp.where(third, 2.0, 1.0)))
    half = jnp.floor(strip * (1.0 / 8))
    return half * (ROLES * 8) + role * 8 + strip - half * 8


def strip_plan(len_row, len_column, group_row, group_column, index_row, index_column, n_groups, seq):
    rows = ROLES * STRIPS
    key_row = group_row * ((seq + 1) * rows) + len_row * rows + index_row
    key_column = group_column * ((seq + 1) * rows) + len_column * rows + index_column
    above_row = jnp.sum(jnp.where(key_column > key_row, 1.0, 0.0), axis=0, keepdims=True)
    above_column = jnp.sum(jnp.where(key_row > key_column, 1.0, 0.0), axis=1, keepdims=True)
    return (
        strip_spot(above_row - rows * (n_groups - 1 - group_row)),
        strip_spot(above_column - rows * (n_groups - 1 - group_column)),
    )


def tail_blocks(lens):
    return jnp.floor((lens + (LANES - 1)) * (1.0 / LANES)) - HEAD_BLOCKS


def shift_bits(count):
    shift = count.astype(jnp.int32)
    return [(lax.shift_right_logical(shift, k) & 1) == 1 for k in range(SHIFTS)]


def shifted_up(blocks, bits, reach):
    for k in range(SHIFTS):
        step, n = 2**k, len(blocks)
        moved = []
        for p in range(min(n + step, reach)):
            if p < step:
                moved.append(blocks[p])
            elif p >= n:
                moved.append(blocks[p - step])
            else:
                moved.append(jnp.where(bits[k], blocks[p - step], blocks[p]))
        blocks = moved
    return blocks


def shifted_down(blocks, bits, count):
    for k in reversed(range(SHIFTS)):
        step = 2**k
        keep = min(len(blocks), count + step - 1)
        blocks = [
            jnp.where(bits[k], blocks[p + step], blocks[p]) if p + step < len(blocks) else blocks[p] for p in range(keep)
        ]
    return blocks


def peer_of(index, off, count):
    out, bit = 0, 1
    while bit < count:
        a, b = lax.rem(index // bit, 2), lax.rem(off // bit, 2)
        out = out + bit * (a + b - 2 * a * b)
        bit *= 2
    return out


def packed_exchange(
    n_gx, n_gy, policy_hbm, anchor_hbm, len_hbm, reward_hbm, prompt_hbm,
    done, loss_ref, adv_ref, over_ref,
    policy, anchor, len_ref, reward_ref, prompt_ref, onehot, ordered, got, heads_in, sendbuf, recvbuf, roles,
    deal, undeal, cnt, rcnt, len_col, sum_policy, sum_kl, len_rows, adv_rows, half_rows,
    info_send, info_got, info_recv, tails_send, tails_recv, counts, needs,
    small_sem, load_sem, give_send_sem, give_recv_sem, first_send_sem, first_recv_sem, strip_send_sem, strip_recv_sem,
    info_send_sem, info_recv_sem, tail_send_sem, tail_recv_sem, count_send_sem, count_recv_sem, need_send_sem, need_recv_sem,
):
    gx, gy = lax.axis_index("gx"), lax.axis_index("gy")
    core, chip = lax.rem(gy, 2), gy // 2
    mate = chip * 2 + 1 - core
    members_dev, slots, seq = policy_hbm.shape
    members, part = members_dev * n_gy, slots // n_gy
    chips = n_gy // 2
    width = seq // CHUNKS
    nblocks = seq // LANES - HEAD_BLOCKS
    rows = members_dev * part
    pool = 2 * rows
    total_rows = chips * pool
    samples = members * slots * n_gx
    info_lane, fill_lane = 16, 17
    f32 = jnp.float32

    small_loads = [
        pltpu.make_async_copy(src, dst, small_sem.at[k])
        for k, (src, dst) in enumerate(((len_hbm, len_ref), (prompt_hbm, prompt_ref), (reward_hbm, reward_ref)))
    ]
    for copy in small_loads:
        copy.start()

    def loads(c):
        cols = pl.ds(pl.multiple_of(c * width, LANES), width)
        return (
            pltpu.make_async_copy(policy_hbm.at[:, :, cols], policy.at[c], load_sem.at[0, c]),
            pltpu.make_async_copy(anchor_hbm.at[:, :, cols], anchor.at[c], load_sem.at[1, c]),
        )

    for copy in loads(0):
        copy.start()
    barrier = pltpu.get_barrier_semaphore()
    for off in range(1, n_gy):
        pl.semaphore_signal(barrier, inc=1, device_id=(gx, partner(gy, off, n_gy)), device_id_type=MESH)
    for off in range(1, n_gx):
        pl.semaphore_signal(barrier, inc=1, device_id=(lax.rem(gx + off, n_gx), gy), device_id_type=MESH)
    for c in range(1, CHUNKS):
        for copy in loads(c):
            copy.start()
    for copy in small_loads:
        copy.wait()

    lens = [len_ref[m : m + 1, :].astype(f32) for m in range(members_dev)]
    targets = []
    for m in range(members_dev):
        spot = lax.rem(prompt_ref[m : m + 1, :], slots)
        device = spot // part
        other = lax.rem(device + core, 2)
        target = (other * chips + device // 2) * rows + m * part + spot - device * part
        targets.append(target.astype(f32))
    place = lax.broadcasted_iota(jnp.int32, (total_rows, slots), 0).astype(f32)
    for m in range(members_dev):
        onehot[:, m * slots : (m + 1) * slots] = jnp.where(place == targets[m], 1.0, 0.0).astype(jnp.bfloat16)

    def put_in_order(c):
        for copy in loads(c):
            copy.wait()
        values = kl_weight * (1.0 - jnp.exp(anchor[c] - policy[c]))
        out = permuted(onehot[...], values.reshape(members_dev * slots, width))
        cols = pl.ds(pl.multiple_of(c * width, LANES), width)
        ordered[:, :, :, cols] = out.reshape(2, chips, rows, width)

    def give(c, there):
        cols = pl.ds(pl.multiple_of(c * width, LANES), width)
        return pltpu.make_async_remote_copy(
            src_ref=ordered.at[1, there, :, cols],
            dst_ref=got.at[there, :, cols],
            send_sem=give_send_sem.at[0],
            recv_sem=give_recv_sem.at[0],
            device_id=(gx, mate),
            device_id_type=MESH,
        )

    give_own = pltpu.make_async_remote_copy(
        src_ref=ordered.at[1, chip],
        dst_ref=got.at[chip],
        send_sem=give_send_sem.at[1],
        recv_sem=give_recv_sem.at[1],
        device_id=(gx, mate),
        device_id_type=MESH,
    )
    given = got.at[pl.ds(0, chips - 1), :, pl.ds(width, seq - width)]

    def first_send(off):
        peer = partner(gy, off, n_gy)
        return pltpu.make_async_remote_copy(
            src_ref=ordered.at[off % 2, peer // 2, :, pl.ds(0, width)],
            dst_ref=heads_in.at[gy],
            send_sem=first_send_sem.at[off - 2],
            recv_sem=first_recv_sem.at[off - 2],
            device_id=(gx, peer),
            device_id_type=MESH,
        )

    put_in_order(0)
    pl.semaphore_wait(barrier, n_gy - 1 + n_gx - 1)
    first_copies = [first_send(off) for off in FIRST_ORDER]
    for copy in first_copies:
        copy.start()

    tile_lane = lax.broadcasted_iota(jnp.int32, (n_gy, 8, LANES), 2)
    groups = rows // 8
    local_tokens = sum(jnp.sum(length) for length in lens)

    def tiles(columns, base):
        out = base
        for f, column in enumerate(columns):
            split = column.reshape(n_gy, groups, 8, 1)
            for g in range(groups):
                out = jnp.where(tile_lane == g * 4 + f, split[:, g], out)
        return out

    def column_in(tile, f):
        parts = [tile[:, :, g * 4 + f : g * 4 + f + 1][:, None] for g in range(groups)]
        return jnp.concatenate(parts, axis=1)

    own_len = row_sums(place, targets, lens)
    rewards = [reward_ref[m : m + 1, :].astype(f32) * 0.25 for m in range(members_dev)]
    own_reward = row_sums(place, targets, rewards)
    info_send[...] = tiles((own_len, own_reward), jnp.broadcast_to(local_tokens, (n_gy, 8, LANES)))

    def tile_sends(src, dst, send, recv, offs):
        copies = []
        for off in offs:
            peer = partner(gy, off, n_gy)
            copies.append(
                pltpu.make_async_remote_copy(
                    src_ref=src.at[off % 2 * chips + peer // 2],
                    dst_ref=dst.at[gy],
                    send_sem=send.at[off - 1],
                    recv_sem=recv.at[off - 1],
                    device_id=(gx, peer),
                    device_id_type=MESH,
                )
            )
        return copies

    mate_info = pltpu.make_async_remote_copy(
        src_ref=info_send.at[pl.ds(chips, chips)],
        dst_ref=info_got,
        send_sem=info_send_sem.at[0],
        recv_sem=info_recv_sem.at[0],
        device_id=(gx, mate),
        device_id_type=MESH,
    )
    info_copies = [mate_info] + tile_sends(info_send, info_recv, info_send_sem, info_recv_sem, range(2, n_gy))
    for copy in info_copies:
        copy.start()

    def order_step(c, carry):
        put_in_order(c)
        for t in range(1, chips):
            give(c, peer_of(chip, t, chips)).start()
        return carry

    lax.fori_loop(1, CHUNKS, order_step, 0)
    give_own.start()

    mate_info.wait()
    pair_lens = jnp.concatenate(
        [own_len[: chips * rows].reshape(chips, 1, rows, 1), column_in(info_got[...], 0).reshape(chips, 1, rows, 1)], axis=1
    ).reshape(total_rows, 1)
    row = lax.broadcasted_iota(jnp.int32, (1, total_rows), 1)
    column = lax.broadcasted_iota(jnp.int32, (total_rows, 1), 0)

    def pair_index(i):
        inside = lax.rem(i, pool)
        return (lax.rem(inside // rows + core, 2) * rows + lax.rem(inside, rows)).astype(f32)

    pair_row = row_of(pair_lens)
    spot_row, _ = strip_plan(
        pair_row, pair_lens, (row // pool).astype(f32), (column // pool).astype(f32), pair_index(row), pair_index(column),
        chips, seq,
    )
    wide = lax.broadcasted_iota(jnp.int32, (total_rows, total_rows), 0).astype(f32)

    def strip_counts(spots, lens_row):
        return row_sums(wide, [spots + (row // pool).astype(f32) * pool], [tail_blocks(lens_row)])

    pair_counts = strip_counts(spot_row, pair_row)
    cnt[...] = jnp.broadcast_to(pair_counts, cnt.shape)
    fill = jnp.sum(pair_counts.reshape(chips, STRIPS // 8, ROLES, 8, 1), axis=2)
    sent_chip = lax.broadcasted_iota(jnp.int32, fill.shape, 0) != chip
    local_fill = jnp.max(jnp.where(sent_chip, fill, 0.0))
    square = lax.broadcasted_iota(jnp.int32, (pool, pool), 0).astype(f32)
    for s in range(chips):
        deal[s] = jnp.where(square == spot_row[:, s * pool : (s + 1) * pool], 1.0, 0.0).astype(jnp.bfloat16)
    pltpu.make_async_copy(given, given, give_recv_sem.at[0]).wait()

    def strip_sends(t, there):
        return [
            pltpu.make_async_remote_copy(
                src_ref=sendbuf.at[there, half],
                dst_ref=recvbuf.at[chip, half],
                send_sem=strip_send_sem.at[t, half],
                recv_sem=strip_recv_sem.at[t, half],
                device_id=(gx, there * 2 + core),
                device_id_type=MESH,
            )
            for half in range(STRIPS // 8)
        ]

    reach = 2 * nblocks

    def pack(t, there):
        for c in range(1, CHUNKS):
            both = jnp.concatenate(
                [ordered[0, there, :, c * width : (c + 1) * width], got[there, :, c * width : (c + 1) * width]], axis=0
            )
            roles[:, (c - 1) * width : c * width] = permuted(deal[there], both)
        for half, copy in enumerate(strip_sends(t, there)):

            def count(role):
                at = there * pool + half * ROLES * 8 + role * 8
                return cnt[pl.ds(pl.multiple_of(at, 8), 8), :]

            def blocks(role):
                at = half * ROLES * 8 + role * 8
                return [roles[at : at + 8, j * LANES : (j + 1) * LANES] for j in range(nblocks)]

            def side(outer, inner):
                n = count(outer)
                behind = shifted_up(blocks(inner), shift_bits(n), reach)
                near_end = blocks(outer)
                return [jnp.where(n > p, near_end[p], behind[p]) for p in range(nblocks)] + behind[nblocks:]

            left, right = side(0, 1), side(3, 2)
            left_n = count(0) + count(1)
            for p in range(STRIP_BLOCKS):
                q = STRIP_BLOCKS - 1 - p
                if q >= reach:
                    value = left[p]
                elif p >= reach:
                    value = right[q]
                else:
                    value = jnp.where(left_n > p, left[p], right[q])
                sendbuf[there, half, :, p * LANES : (p + 1) * LANES] = value

    def near_step(t, carry):
        there = peer_of(chip, t + 1, chips)
        pack(t, there)
        return carry

    far = peer_of(chip, chips - 1, chips)
    pack(chips - 2, far)
    for copy in strip_sends(chips - 2, far):
        copy.start()


    lax.fori_loop(0, 2, near_step, 0)
    info_recv[gy] = info_send[chip]
    for copy in info_copies[1:]:
        copy.wait()
    info_recv[mate] = info_got[chip]
    arrived = info_recv[...]
    counts[0] = jnp.sum(arrived, axis=0)

    def axis_sends(buf, send, recv):
        return [
            pltpu.make_async_remote_copy(
                src_ref=buf.at[0],
                dst_ref=buf.at[off],
                send_sem=send.at[off - 1],
                recv_sem=recv.at[off - 1],
                device_id=(lax.rem(gx + off, n_gx), gy),
                device_id_type=MESH,
            )
            for off in range(1, n_gx)
        ]

    count_copies = axis_sends(counts, count_send_sem, count_recv_sem)
    for copy in count_copies:
        copy.start()

    eye = lax.broadcasted_iota(jnp.int32, (slots, slots), 0) == lax.broadcasted_iota(jnp.int32, (slots, slots), 1)
    for m in range(members_dev):
        len_col[m] = jnp.broadcast_to(jnp.sum(jnp.where(eye, lens[m], 0.0), axis=1, keepdims=True), (slots, LANES))
    sum_policy[...] = jnp.zeros_like(sum_policy)
    sum_kl[...] = jnp.zeros_like(sum_kl)

    def sum_step(c, carry):
        positions = (lax.broadcasted_iota(jnp.int32, (slots, width), 1) + c * width).astype(f32)
        for m in range(members_dev):
            pol = policy[c, m]
            log_ratio = anchor[c, m] - pol
            ratio = jnp.exp(log_ratio)
            valid = positions < len_col[m][:, :1]
            sum_policy[m] += folded(jnp.where(valid, pol, 0.0))
            sum_kl[m] += folded(jnp.where(valid, kl_weight * (ratio - log_ratio - 1.0), 0.0))
        return carry

    lax.fori_loop(0, CHUNKS, sum_step, 0)
    sums = []
    for buf in (sum_policy, sum_kl):
        per_member = [row_of(jnp.sum(buf[m], axis=1, keepdims=True)) for m in range(members_dev)]
        sums.append(row_sums(place, targets, per_member))
    tails_send[...] = tiles(sums, jnp.broadcast_to(local_fill, (n_gy, 8, LANES)))
    tail_copies = tile_sends(tails_send, tails_recv, tail_send_sem, tail_recv_sem, range(1, n_gy))
    for copy in tail_copies:
        copy.start()
    tails_recv[gy] = tails_send[chip]

    near_copies = [strip_sends(t, peer_of(chip, t + 1, chips)) for t in range(2)]
    for half in range(2):
        for t in range(2):
            near_copies[t][half].start()


    for copy in count_copies:
        copy.wait()
    tokens = counts[0]
    for off in range(1, n_gx):
        tokens = tokens + counts[off]
    ntok = tokens[:1, info_lane : info_lane + 1]
    scale = samples * seq / ntok
    got_len = column_in(arrived, 0).reshape(total_rows, 1)
    got_row = row_of(got_len)
    reward = column_in(arrived, 1).reshape(members, part, 1)
    advantage = (members * reward - jnp.sum(reward, axis=0)[None]) / (members - 1)
    adv_rows[...] = jnp.broadcast_to(advantage, adv_rows.shape)
    len_rows[...] = jnp.broadcast_to(got_len.reshape(members, part, 1), len_rows.shape)
    got_spot_row, got_spot = strip_plan(
        got_row, got_len, (row // pool).astype(f32), (column // pool).astype(f32),
        lax.rem(row, pool).astype(f32), lax.rem(column, pool).astype(f32), chips, seq,
    )
    rcnt[...] = jnp.broadcast_to(strip_counts(got_spot_row, got_row), rcnt.shape)
    lane = lax.broadcasted_iota(jnp.int32, (total_rows, LANES), 1).astype(f32)
    for half in range(STRIPS // 8):
        pick = got_spot - half * ROLES * 8 == lane
        pick = jnp.where(pick & (lane < ROLES * 8), 1.0, 0.0).astype(jnp.bfloat16)
        undeal[:, half] = pick.reshape(chips, pool, LANES)
    half_rows[...] = jnp.broadcast_to(jnp.where(got_spot < ROLES * 8, 0.0, 1.0).reshape(members, part, 1), half_rows.shape)
    lane_width = lax.broadcasted_iota(jnp.int32, (part, width), 1).astype(f32)

    def finish_rows(k, start, value, only=None):
        value = (value - adv_rows[k][:, :1]) * scale
        valid = lane_width < len_rows[k][:, :1] - start
        value = jnp.where(valid, value, 0.0)
        if only is not None:
            value = jnp.where(only, value, done[k, :, start : start + width])
        done[k, :, start : start + width] = value

    def own_step(which, source):
        for m in range(members_dev):
            for c in range(CHUNKS):
                finish_rows(source * members_dev + m, c * width, which(m * part, c * width))

    own_step(lambda r, s: ordered[0, chip, r : r + part, s : s + width], gy)
    give_own.wait_recv()
    own_step(lambda r, s: got[chip, r : r + part, s : s + width], mate)

    def first_wait(off):
        landed = heads_in.at[0]
        pltpu.make_async_copy(landed, landed, first_recv_sem.at[off - 2]).wait()

    def first_step(off, carry):
        first_wait(off)
        source = peer_of(gy, off, n_gy)
        for m in range(members_dev):
            finish_rows(source * members_dev + m, 0, heads_in[source, m * part : (m + 1) * part, :])
        return carry

    lax.fori_loop(2, n_gy, first_step, 0)

    def unpack(t, half):
        there = peer_of(chip, t + 1, chips)
        landed = recvbuf.at[0, 0]
        pltpu.make_async_copy(landed, landed, strip_recv_sem.at[t, half]).wait()

        def count(role):
            at = there * pool + half * ROLES * 8 + role * 8
            return rcnt[pl.ds(pl.multiple_of(at, 8), 8), :]

        def block(p):
            return recvbuf[there, half, :, p * LANES : (p + 1) * LANES]

        for outer, inner, at in ((0, 1, lambda p: p), (3, 2, lambda p: STRIP_BLOCKS - 1 - p)):
            for j in range(nblocks):
                roles[outer * 8 : outer * 8 + 8, j * LANES : (j + 1) * LANES] = block(at(j))
            behind = [block(at(p)) for p in range(reach)]
            behind = shifted_down(behind, shift_bits(count(outer)), nblocks)
            for j in range(nblocks):
                roles[inner * 8 : inner * 8 + 8, j * LANES : (j + 1) * LANES] = behind[j]
        order = undeal[there, half][:, : ROLES * 8]
        for c in range(1, CHUNKS):
            out = permuted(order, roles[: ROLES * 8, (c - 1) * width : c * width])
            for r in range(2 * members_dev):
                k = there * 2 * members_dev + r
                finish_rows(k, c * width, out[r * part : (r + 1) * part], half_rows[k][:, :1] > 0.5 if half else None)

    def unpack_step(t, carry):
        for half in range(STRIPS // 8):
            unpack(t, half)
        return carry

    for half in range(STRIPS // 8):
        unpack(chips - 2, half)

    for copy in tail_copies:
        copy.wait()
    ends = tails_recv[...]
    needs[0] = jnp.max(ends, axis=0)
    need_copies = axis_sends(needs, need_send_sem, need_recv_sem)
    for copy in need_copies:
        copy.start()
    first_sum = column_in(ends, 0).reshape(members, part, 1)
    second_sum = column_in(ends, 1).reshape(members, part, 1)
    value = (second_sum - advantage * first_sum) * (samples / ntok)[None]
    shape = (members, part, LANES)
    spread = lax.broadcasted_iota(jnp.int32, shape, 1) == lax.broadcasted_iota(jnp.int32, shape, 2)
    loss_ref[...] = jnp.sum(jnp.where(spread, value, 0.0), axis=1)[:, :part]
    adv_ref[...] = jnp.sum(jnp.where(spread, advantage, 0.0), axis=1)[:, :part]
    for copy in need_copies:
        copy.wait()
    fullest = needs[0]
    for off in range(1, n_gx):
        fullest = jnp.maximum(fullest, needs[off])
    over_ref[0, 0] = (jnp.max(fullest[:, fill_lane : fill_lane + 1]) > STRIP_BLOCKS).astype(jnp.int32)
    for copy in first_copies:
        copy.wait_send()
    pltpu.make_async_copy(given, given, give_send_sem.at[0]).wait()
    give_own.wait_send()

    lax.fori_loop(0, 2, unpack_step, 0)
    for t in range(chips - 1):
        for half in range(STRIPS // 8):
            sent = sendbuf.at[0, 0]
            pltpu.make_async_copy(sent, sent, strip_send_sem.at[t, half]).wait()


def store(done, loss, adv, grad, loss_out, adv_out, sem):
    copies = [
        pltpu.make_async_copy(src, dst, sem.at[k])
        for k, (src, dst) in enumerate(((done, grad), (loss, loss_out), (adv, adv_out)))
    ]
    for copy in copies:
        copy.start()
    for copy in copies:
        copy.wait()


def packed_body(n_gx, n_gy, policy_logp, anchor_logp, lengths, rewards, slot_prompt):
    members_dev, slots, seq = policy_logp.shape
    members, part = members_dev * n_gy, slots // n_gy
    f32, bf16 = jnp.float32, jnp.bfloat16
    chips, rows = n_gy // 2, members_dev * part
    pool = 2 * rows
    width = seq // CHUNKS
    chunked = (CHUNKS, members_dev, slots, width)
    strips = (chips, STRIPS // 8, 8, STRIP_BLOCKS * LANES)
    per_slot = (members_dev, slots, LANES)
    per_sample = (members, part, LANES)
    tile = (n_gy, 8, LANES)
    hbm_spec = pl.BlockSpec(memory_space=pltpu.HBM)
    vmem_spec = pl.BlockSpec(memory_space=pltpu.VMEM)
    dma = pltpu.SemaphoreType.DMA
    done, loss, adv, over = pl.pallas_call(
        functools.partial(packed_exchange, n_gx, n_gy),
        out_shape=(
            pltpu.VMEM((members, part, seq), f32),
            pltpu.VMEM((members, part), f32),
            pltpu.VMEM((members, part), f32),
            pltpu.SMEM((1, 1), jnp.int32),
        ),
        in_specs=[hbm_spec] * 5,
        out_specs=(vmem_spec,) * 3 + (pl.BlockSpec(memory_space=pltpu.SMEM),),
        scratch_shapes=[
            pltpu.VMEM(chunked, f32),
            pltpu.VMEM(chunked, f32),
            pltpu.VMEM((members_dev, slots), jnp.int32),
            pltpu.VMEM((members_dev, slots), jnp.int32),
            pltpu.VMEM((members_dev, slots), jnp.int32),
            pltpu.VMEM((2 * chips * rows, members_dev * slots), bf16),
            pltpu.VMEM((2, chips, rows, seq), f32),
            pltpu.VMEM((chips, rows, seq), f32),
            pltpu.VMEM((n_gy, rows, width), f32),
            pltpu.VMEM(strips, f32),
            pltpu.VMEM(strips, f32),
            pltpu.VMEM((pool, seq - width), f32),
            pltpu.VMEM((chips, pool, pool), bf16),
            pltpu.VMEM((chips, STRIPS // 8, pool, LANES), bf16),
            pltpu.VMEM((chips * pool, LANES), f32),
            pltpu.VMEM((chips * pool, LANES), f32),
            pltpu.VMEM(per_slot, f32),
            pltpu.VMEM(per_slot, f32),
            pltpu.VMEM(per_slot, f32),
            pltpu.VMEM(per_sample, f32),
            pltpu.VMEM(per_sample, f32),
            pltpu.VMEM(per_sample, f32),
            pltpu.VMEM(tile, f32),
            pltpu.VMEM((chips, 8, LANES), f32),
            pltpu.VMEM(tile, f32),
            pltpu.VMEM(tile, f32),
            pltpu.VMEM(tile, f32),
            pltpu.VMEM((n_gx, 8, LANES), f32),
            pltpu.VMEM((n_gx, 8, LANES), f32),
            dma((3,)),
            dma((2, CHUNKS)),
            dma((2,)),
            dma((2,)),
            dma((n_gy - 2,)),
            dma((n_gy - 2,)),
            dma((chips - 1, STRIPS // 8)),
            dma((chips - 1, STRIPS // 8)),
            dma((n_gy - 1,)),
            dma((n_gy - 1,)),
            dma((n_gy - 1,)),
            dma((n_gy - 1,)),
            dma((n_gx - 1,)),
            dma((n_gx - 1,)),
            dma((n_gx - 1,)),
            dma((n_gx - 1,)),
        ],
        compiler_params=pltpu.CompilerParams(collective_id=0, has_side_effects=True, vmem_limit_bytes=56 * 2**20),
    )(policy_logp, anchor_logp, lengths, rewards, slot_prompt)

    def fits(policy_logp, anchor_logp, lengths, rewards, slot_prompt, done, loss, adv):
        small = jax.ShapeDtypeStruct((members, part), f32)
        return tuple(pl.pallas_call(
            store,
            out_shape=(jax.ShapeDtypeStruct((members, part, seq), f32), small, small),
            in_specs=[vmem_spec] * 3,
            out_specs=(hbm_spec,) * 3,
            scratch_shapes=[dma((3,))],
            compiler_params=pltpu.CompilerParams(vmem_limit_bytes=16 * 2**20),
        )(done, loss, adv))

    def overflows(policy_logp, anchor_logp, lengths, rewards, slot_prompt, done, loss, adv):
        return tuple(unpacked_body(n_gx, n_gy, policy_logp, anchor_logp, lengths, rewards, slot_prompt))

    return lax.cond(
        over[0, 0] > 0, overflows, fits,
        policy_logp, anchor_logp, lengths, rewards, slot_prompt, done, loss, adv,
    )


def body(n_gx, n_gy, *args):
    members_dev, slots, seq = args[0].shape
    pool = 2 * members_dev * slots // n_gy
    packs = n_gy == 8 and pool == ROLES * STRIPS and slots == LANES and seq == LANES * 32 and seq == CHUNKS * HEAD_BLOCKS * LANES
    return (packed_body if packs else unpacked_body)(n_gx, n_gy, *args)


def solution(mesh):
    placed = (P("gy", "gx", None), P("gy", "gx", None), P("gy", "gx"), P("gy", "gx"), P("gy", "gx"))
    return jax.shard_map(
        functools.partial(body, mesh.shape["gx"], mesh.shape["gy"]),
        mesh=mesh,
        in_specs=placed,
        out_specs=(P(None, ("gx", "gy"), None), P(None, ("gx", "gy")), P(None, ("gx", "gy"))),
        check_vma=False,
    )
```

```python
import functools

import jax
import jax.numpy as jnp
from jax import lax
from jax.experimental import pallas as pl
from jax.experimental.pallas import tpu as pltpu
from jax.sharding import PartitionSpec as P

kl_weight = 0.1
LANES = 128
CHUNKS = 8
MESH = pl.DeviceIdType.MESH
ROLES = 4
STRIPS = 16
HALVES = STRIPS // 8
SHIFTS = 5
HEAD_BLOCKS = 4
STRIP_BLOCKS = 74
FIRST_ORDER = (2, 4, 3, 5, 6, 7)


def partner(index, off, count):
    out, bit = index, 1
    while bit < count:
        if off & bit:
            out = out + bit - 2 * bit * lax.rem(index // bit, 2)
        bit *= 2
    return out


def offsets_by_distance(count):
    far = max(bin(off // 2).count("1") for off in range(1, count))
    near = [off for off in range(1, count) if bin(off // 2).count("1") < far]
    return near, [off for off in range(1, count) if off not in near]


def permuted(onehot, rows):
    high = rows.astype(jnp.bfloat16)
    rest = rows - high.astype(jnp.float32)
    middle = rest.astype(jnp.bfloat16)
    low = (rest - middle.astype(jnp.float32)).astype(jnp.bfloat16)
    dot = functools.partial(jnp.dot, preferred_element_type=jnp.float32)
    return dot(onehot, high) + dot(onehot, middle) + dot(onehot, low)


def folded(x):
    out = x[:, :LANES]
    for start in range(LANES, x.shape[1], LANES):
        out = out + x[:, start : start + LANES]
    return out


def exchange(
    n_gx, n_gy, policy_hbm, anchor_hbm, len_ref, reward_ref, prompt_ref,
    raw_hbm, heads_ref, tails_ref, ntok_ref,
    policy, anchor, sendbuf, onehot, len_col, sum_policy, sum_kl,
    heads_send, heads_recv, tails_send, tails_recv, counts,
    load_sem, send_sem, recv_sem, own_sem,
    head_send_sem, head_recv_sem, tail_send_sem, tail_recv_sem, count_send_sem, count_recv_sem,
):
    gx, gy = lax.axis_index("gx"), lax.axis_index("gy")
    members_dev, slots, seq = policy_hbm.shape
    part = slots // n_gy
    width = seq // CHUNKS

    near, far = offsets_by_distance(n_gy)
    barrier = pltpu.get_barrier_semaphore()
    for off in range(1, n_gy):
        pl.semaphore_signal(barrier, inc=1, device_id=(gx, partner(gy, off, n_gy)), device_id_type=MESH)
    for off in range(1, n_gx):
        pl.semaphore_signal(barrier, inc=1, device_id=(lax.rem(gx + off, n_gx), gy), device_id_type=MESH)

    def loads(c):
        cols = pl.ds(pl.multiple_of(c * width, LANES), width)
        return (
            pltpu.make_async_copy(policy_hbm.at[:, :, cols], policy.at[c], load_sem.at[0, c]),
            pltpu.make_async_copy(anchor_hbm.at[:, :, cols], anchor.at[c], load_sem.at[1, c]),
        )

    for c in range(CHUNKS):
        for copy in loads(c):
            copy.start()

    sublane = lax.broadcasted_iota(jnp.int32, (slots, slots), 0)
    lane = lax.broadcasted_iota(jnp.int32, (slots, slots), 1)
    column = lax.broadcasted_iota(jnp.int32, (slots, LANES), 1)
    local_tokens = jnp.sum(len_ref[...].astype(jnp.float32))
    for m in range(members_dev):
        seq_len = len_ref[m : m + 1, :].astype(jnp.float32)
        reward = reward_ref[m : m + 1, :].astype(jnp.float32) * 0.25
        match = sublane == lax.rem(prompt_ref[m : m + 1, :], slots)
        onehot[m] = jnp.where(match, 1.0, 0.0).astype(jnp.bfloat16)
        len_col[m] = jnp.broadcast_to(
            jnp.sum(jnp.where(sublane == lane, seq_len, 0.0), axis=1, keepdims=True), (slots, LANES)
        )
        sorted_len = jnp.sum(jnp.where(match, seq_len, 0.0), axis=1, keepdims=True)
        sorted_reward = jnp.sum(jnp.where(match, reward, 0.0), axis=1, keepdims=True)
        heads_send[m] = jnp.where(
            column == 0, sorted_len, jnp.where(column == 1, sorted_reward, local_tokens)
        )
    sum_policy[...] = jnp.zeros_like(sum_policy)
    sum_kl[...] = jnp.zeros_like(sum_kl)

    def compute(c):
        for copy in loads(c):
            copy.wait()
        positions = (lax.broadcasted_iota(jnp.int32, (slots, width), 1) + c * width).astype(jnp.float32)
        for m in range(members_dev):
            pol = policy[c, m]
            log_ratio = anchor[c, m] - pol
            ratio = jnp.exp(log_ratio)
            valid = positions < len_col[m][:, :1]
            sum_policy[m] += folded(jnp.where(valid, pol, 0.0))
            sum_kl[m] += folded(jnp.where(valid, kl_weight * (ratio - log_ratio - 1.0), 0.0))
            sendbuf[c, m] = permuted(onehot[m], kl_weight * (1.0 - ratio))

    def rows_of(device):
        return pl.ds(pl.multiple_of(device * part, part), part)

    my_members = pl.ds(gy * members_dev, members_dev)

    def sends(c, offs):
        cols = pl.ds(pl.multiple_of(c * width, LANES), width)
        copies = []
        for off in offs:
            peer = partner(gy, off, n_gy)
            copies.append(
                pltpu.make_async_remote_copy(
                    src_ref=sendbuf.at[c, :, rows_of(peer), :],
                    dst_ref=raw_hbm.at[my_members, :, cols],
                    send_sem=send_sem.at[off - 1],
                    recv_sem=recv_sem.at[off - 1],
                    device_id=(gx, peer),
                    device_id_type=MESH,
                )
            )
        return copies

    def own(c):
        cols = pl.ds(pl.multiple_of(c * width, LANES), width)
        return pltpu.make_async_copy(
            sendbuf.at[c, :, rows_of(gy), :], raw_hbm.at[my_members, :, cols], own_sem.at[c]
        )

    def small_sends(src, dst, send, recv):
        copies = []
        for off in range(1, n_gy):
            peer = partner(gy, off, n_gy)
            copies.append(
                pltpu.make_async_remote_copy(
                    src_ref=src.at[:, rows_of(peer), :],
                    dst_ref=dst.at[my_members],
                    send_sem=send.at[off - 1],
                    recv_sem=recv.at[off - 1],
                    device_id=(gx, peer),
                    device_id_type=MESH,
                )
            )
        copies.append(pltpu.make_async_copy(src.at[:, rows_of(gy), :], dst.at[my_members], send.at[n_gy - 1]))
        return copies

    def count_sends():
        return [
            pltpu.make_async_remote_copy(
                src_ref=counts.at[0],
                dst_ref=counts.at[off],
                send_sem=count_send_sem.at[off - 1],
                recv_sem=count_recv_sem.at[off - 1],
                device_id=(lax.rem(gx + off, n_gx), gy),
                device_id_type=MESH,
            )
            for off in range(1, n_gx)
        ]

    compute(0)
    pl.semaphore_wait(barrier, n_gy - 1 + n_gx - 1)
    head_copies = small_sends(heads_send, heads_recv, head_send_sem, head_recv_sem)
    for copy in head_copies:
        copy.start()

    def step(c, carry):
        for copy in sends(c - 1, near):
            copy.start()
        own(c - 1).start()
        compute(c)
        return carry

    lax.fori_loop(1, CHUNKS, step, 0)
    for copy in sends(CHUNKS - 1, near):
        copy.start()

    def far_step(c, carry):
        for copy in sends(c, far):
            copy.start()
        return carry

    lax.fori_loop(0, CHUNKS, far_step, 0)
    own(CHUNKS - 1).start()

    for m in range(members_dev):
        s1 = jnp.sum(permuted(onehot[m], sum_policy[m]), axis=1, keepdims=True)
        s2 = jnp.sum(permuted(onehot[m], sum_kl[m]), axis=1, keepdims=True)
        tails_send[m] = jnp.where(column == 0, s1, s2)
    for copy in head_copies:
        copy.wait()
    tokens = jnp.zeros((8, LANES), jnp.float32)
    for source in range(n_gy):
        tokens = tokens + heads_recv[source * members_dev, :8, :]
    counts[0] = tokens
    heads_ref[...] = heads_recv[...]
    tail_copies = small_sends(tails_send, tails_recv, tail_send_sem, tail_recv_sem)
    for copy in tail_copies:
        copy.start()
    count_copies = count_sends()
    for copy in count_copies:
        copy.start()
    for copy in count_copies:
        copy.wait()
    ntok_ref[...] = jnp.sum(counts[...], axis=0)
    for copy in tail_copies:
        copy.wait()
    tails_ref[...] = tails_recv[...]
    for c in range(CHUNKS):
        own(c).wait()
    for off in range(1, n_gy):
        source = partner(gy, off, n_gy)
        landed = raw_hbm.at[pl.ds(source * members_dev, members_dev)]
        pltpu.make_async_copy(landed, landed, recv_sem.at[off - 1]).wait()
        pltpu.make_async_copy(landed, landed, send_sem.at[off - 1]).wait()


def finish(samples, raw, heads, tails, ntok, grad, loss, adv, done, done_sem):
    members, part, seq = raw.shape
    tokens = ntok[:1, 2:3]
    total = jnp.sum(heads[...], axis=0)
    advantage = (members * heads[:, :, 1:2] - total[None, :, 1:2]) / (members - 1)
    positions = lax.broadcasted_iota(jnp.int32, (part, seq), 1).astype(jnp.float32)
    scale = samples * seq / tokens

    def store(k):
        return pltpu.make_async_copy(done.at[k], grad.at[k], done_sem.at[k])

    for k in range(members):
        done[k] = jnp.where(positions < heads[k, :, :1], raw[k] - advantage[k], 0.0) * scale
        if k > 0:
            store(k - 1).start()
    shape = (members, part, LANES)
    eye = lax.broadcasted_iota(jnp.int32, shape, 1) == lax.broadcasted_iota(jnp.int32, shape, 2)
    store(members - 1).start()
    value = (tails[:, :, 1:2] - advantage * tails[:, :, :1]) * (samples / tokens)[None]
    loss[...] = jnp.sum(jnp.where(eye, value, 0.0), axis=1)[:, :part]
    adv[...] = jnp.sum(jnp.where(eye, advantage, 0.0), axis=1)[:, :part]
    for k in range(members):
        store(k).wait()


def unpacked_body(n_gx, n_gy, policy_logp, anchor_logp, lengths, rewards, slot_prompt):
    members_dev, slots, seq = policy_logp.shape
    members, part = members_dev * n_gy, slots // n_gy
    f32 = jnp.float32
    chunked = (CHUNKS, members_dev, slots, seq // CHUNKS)
    small = (members, part, LANES)
    hbm_spec = pl.BlockSpec(memory_space=pltpu.HBM)
    vmem_spec = pl.BlockSpec(memory_space=pltpu.VMEM)
    dma = pltpu.SemaphoreType.DMA
    raw, heads, tails, ntok = pl.pallas_call(
        functools.partial(exchange, n_gx, n_gy),
        out_shape=(
            pltpu.VMEM((members, part, seq), f32),
            pltpu.VMEM(small, f32),
            pltpu.VMEM(small, f32),
            pltpu.VMEM((8, LANES), f32),
        ),
        in_specs=[hbm_spec, hbm_spec, vmem_spec, vmem_spec, vmem_spec],
        out_specs=(vmem_spec, vmem_spec, vmem_spec, vmem_spec),
        scratch_shapes=[
            pltpu.VMEM(chunked, f32),
            pltpu.VMEM(chunked, f32),
            pltpu.VMEM(chunked, f32),
            pltpu.VMEM((members_dev, slots, slots), jnp.bfloat16),
            pltpu.VMEM((members_dev, slots, LANES), f32),
            pltpu.VMEM((members_dev, slots, LANES), f32),
            pltpu.VMEM((members_dev, slots, LANES), f32),
            pltpu.VMEM((members_dev, slots, LANES), f32),
            pltpu.VMEM(small, f32),
            pltpu.VMEM((members_dev, slots, LANES), f32),
            pltpu.VMEM(small, f32),
            pltpu.VMEM((n_gx, 8, LANES), f32),
            dma((2, CHUNKS)),
            dma((n_gy - 1,)),
            dma((n_gy - 1,)),
            dma((CHUNKS,)),
            dma((n_gy,)),
            dma((n_gy - 1,)),
            dma((n_gy,)),
            dma((n_gy - 1,)),
            dma((n_gx - 1,)),
            dma((n_gx - 1,)),
        ],
        compiler_params=pltpu.CompilerParams(collective_id=1, has_side_effects=True, vmem_limit_bytes=36 * 2**20),
    )(policy_logp, anchor_logp, lengths, rewards, slot_prompt)
    samples = members * slots * n_gx
    return pl.pallas_call(
        functools.partial(finish, samples),
        out_shape=(
            jax.ShapeDtypeStruct((members, part, seq), f32),
            jax.ShapeDtypeStruct((members, part), f32),
            jax.ShapeDtypeStruct((members, part), f32),
        ),
        in_specs=[vmem_spec] * 4,
        out_specs=(hbm_spec, vmem_spec, vmem_spec),
        scratch_shapes=[pltpu.VMEM((members, part, seq), f32), dma((members,))],
        compiler_params=pltpu.CompilerParams(vmem_limit_bytes=32 * 2**20),
    )(raw, heads, tails, ntok)


def row_of(column):
    n = column.shape[0]
    eye = lax.broadcasted_iota(jnp.int32, (n, n), 0) == lax.broadcasted_iota(jnp.int32, (n, n), 1)
    return jnp.sum(jnp.where(eye, column, 0.0), axis=0, keepdims=True)


def row_sums(place, targets, values):
    out = None
    for target, value in zip(targets, values):
        here = jnp.sum(jnp.where(place == target, value, 0.0), axis=1, keepdims=True)
        out = here if out is None else out + here
    return out


def strip_spot(rank):
    first, second, third = rank < STRIPS, rank < 2 * STRIPS, rank < 3 * STRIPS
    strip = jnp.where(
        first, rank, jnp.where(second, 2 * STRIPS - 1 - rank, jnp.where(third, 3 * STRIPS - 1 - rank, rank - 3 * STRIPS))
    )
    role = jnp.where(first, 0.0, jnp.where(second, 3.0, jnp.where(third, 2.0, 1.0)))
    half = jnp.floor(strip * (1.0 / 8))
    return half * (ROLES * 8) + role * 8 + strip - half * 8


def strip_plan(len_row, len_column, group_row, group_column, index_row, index_column, n_groups, seq):
    rows = ROLES * STRIPS
    key_row = group_row * ((seq + 1) * rows) + len_row * rows + index_row
    key_column = group_column * ((seq + 1) * rows) + len_column * rows + index_column
    above_row = jnp.sum(jnp.where(key_column > key_row, 1.0, 0.0), axis=0, keepdims=True)
    above_column = jnp.sum(jnp.where(key_row > key_column, 1.0, 0.0), axis=1, keepdims=True)
    return (
        strip_spot(above_row - rows * (n_groups - 1 - group_row)),
        strip_spot(above_column - rows * (n_groups - 1 - group_column)),
    )


def tail_blocks(lens):
    return jnp.floor((lens + (LANES - 1)) * (1.0 / LANES)) - HEAD_BLOCKS


def shift_bits(count):
    shift = count.astype(jnp.int32)
    return [(lax.shift_right_logical(shift, k) & 1) == 1 for k in range(SHIFTS)]


def shifted_up(blocks, bits, reach):
    for k in range(SHIFTS):
        step, n = 2**k, len(blocks)
        moved = []
        for p in range(min(n + step, reach)):
            if p < step:
                moved.append(blocks[p])
            elif p >= n:
                moved.append(blocks[p - step])
            else:
                moved.append(jnp.where(bits[k], blocks[p - step], blocks[p]))
        blocks = moved
    return blocks


def shifted_down(blocks, bits, count):
    for k in reversed(range(SHIFTS)):
        step = 2**k
        keep = min(len(blocks), count + step - 1)
        blocks = [
            jnp.where(bits[k], blocks[p + step], blocks[p]) if p + step < len(blocks) else blocks[p] for p in range(keep)
        ]
    return blocks


def peer_of(index, off, count):
    out, bit = 0, 1
    while bit < count:
        a, b = lax.rem(index // bit, 2), lax.rem(off // bit, 2)
        out = out + bit * (a + b - 2 * a * b)
        bit *= 2
    return out


def unpack_strips(recvbuf, roles, undeal, rcnt, there, half, width, part, put):
    pool, seq_tail = undeal.shape[2], roles.shape[1]
    nblocks = seq_tail // LANES

    def count(role):
        at = there * pool + half * ROLES * 8 + role * 8
        return rcnt[pl.ds(pl.multiple_of(at, 8), 8), :]

    def block(p):
        return recvbuf[there, half, :, p * LANES : (p + 1) * LANES]

    for outer, inner, at in ((0, 1, lambda p: p), (3, 2, lambda p: STRIP_BLOCKS - 1 - p)):
        for j in range(nblocks):
            roles[outer * 8 : outer * 8 + 8, j * LANES : (j + 1) * LANES] = block(at(j))
        behind = [block(at(p)) for p in range(2 * nblocks)]
        behind = shifted_down(behind, shift_bits(count(outer)), nblocks)
        for j in range(nblocks):
            roles[inner * 8 : inner * 8 + 8, j * LANES : (j + 1) * LANES] = behind[j]
    order = undeal[there, half][:, : ROLES * 8]
    for c in range(seq_tail // width):
        out = permuted(order, roles[: ROLES * 8, c * width : (c + 1) * width])
        for r in range(pool // part):
            put(r, c + 1, out[r * part : (r + 1) * part])


def packed_exchange(
    n_gx, n_gy, policy_hbm, anchor_hbm, len_hbm, reward_hbm, prompt_hbm,
    done, loss_ref, adv_ref, over_ref, recvbuf, undeal, rcnt, len_rows, adv_rows, half_rows, scale_ref,
    policy, anchor, len_ref, reward_ref, prompt_ref, onehot, ordered, got, heads_in, sendbuf, passing, roles,
    deal, cnt, len_col, sum_policy, sum_kl,
    info_send, info_got, info_recv, tails_send, tails_recv, counts, needs,
    small_sem, load_sem, give_send_sem, give_recv_sem, first_send_sem, first_recv_sem, strip_send_sem, strip_recv_sem, first_leg_send_sem, first_leg_recv_sem,
    info_send_sem, info_recv_sem, tail_send_sem, tail_recv_sem, count_send_sem, count_recv_sem, need_send_sem, need_recv_sem,
):
    gx, gy = lax.axis_index("gx"), lax.axis_index("gy")
    core, chip = lax.rem(gy, 2), gy // 2
    mate = chip * 2 + 1 - core
    members_dev, slots, seq = policy_hbm.shape
    members, part = members_dev * n_gy, slots // n_gy
    chips = n_gy // 2
    width = seq // CHUNKS
    nblocks = seq // LANES - HEAD_BLOCKS
    rows = members_dev * part
    pool = 2 * rows
    total_rows = chips * pool
    samples = members * slots * n_gx
    info_lane, fill_lane = 16, 17
    f32 = jnp.float32

    small_loads = [
        pltpu.make_async_copy(src, dst, small_sem.at[k])
        for k, (src, dst) in enumerate(((len_hbm, len_ref), (prompt_hbm, prompt_ref), (reward_hbm, reward_ref)))
    ]
    for copy in small_loads:
        copy.start()

    def loads(c):
        cols = pl.ds(pl.multiple_of(c * width, LANES), width)
        return (
            pltpu.make_async_copy(policy_hbm.at[:, :, cols], policy.at[c], load_sem.at[0, c]),
            pltpu.make_async_copy(anchor_hbm.at[:, :, cols], anchor.at[c], load_sem.at[1, c]),
        )

    for copy in loads(0):
        copy.start()
    barrier = pltpu.get_barrier_semaphore()
    for off in range(1, n_gy):
        pl.semaphore_signal(barrier, inc=1, device_id=(gx, partner(gy, off, n_gy)), device_id_type=MESH)
    for off in range(1, n_gx):
        pl.semaphore_signal(barrier, inc=1, device_id=(lax.rem(gx + off, n_gx), gy), device_id_type=MESH)
    for c in range(1, CHUNKS):
        for copy in loads(c):
            copy.start()
    for copy in small_loads:
        copy.wait()

    lens = [len_ref[m : m + 1, :].astype(f32) for m in range(members_dev)]
    targets = []
    for m in range(members_dev):
        spot = lax.rem(prompt_ref[m : m + 1, :], slots)
        device = spot // part
        other = lax.rem(device + core, 2)
        target = (other * chips + device // 2) * rows + m * part + spot - device * part
        targets.append(target.astype(f32))
    place = lax.broadcasted_iota(jnp.int32, (total_rows, slots), 0).astype(f32)
    for m in range(members_dev):
        onehot[:, m * slots : (m + 1) * slots] = jnp.where(place == targets[m], 1.0, 0.0).astype(jnp.bfloat16)

    def put_in_order(c):
        for copy in loads(c):
            copy.wait()
        values = kl_weight * (1.0 - jnp.exp(anchor[c] - policy[c]))
        out = permuted(onehot[...], values.reshape(members_dev * slots, width))
        cols = pl.ds(pl.multiple_of(c * width, LANES), width)
        ordered[:, :, :, cols] = out.reshape(2, chips, rows, width)

    def give(c, there):
        cols = pl.ds(pl.multiple_of(c * width, LANES), width)
        return pltpu.make_async_remote_copy(
            src_ref=ordered.at[1, there, :, cols],
            dst_ref=got.at[there, :, cols],
            send_sem=give_send_sem.at[0],
            recv_sem=give_recv_sem.at[0],
            device_id=(gx, mate),
            device_id_type=MESH,
        )

    give_own = pltpu.make_async_remote_copy(
        src_ref=ordered.at[1, chip],
        dst_ref=got.at[chip],
        send_sem=give_send_sem.at[1],
        recv_sem=give_recv_sem.at[1],
        device_id=(gx, mate),
        device_id_type=MESH,
    )
    given = got.at[pl.ds(0, chips - 1), :, pl.ds(width, seq - width)]

    def first_send(off):
        peer = partner(gy, off, n_gy)
        return pltpu.make_async_remote_copy(
            src_ref=ordered.at[off % 2, peer // 2, :, pl.ds(0, width)],
            dst_ref=heads_in.at[gy],
            send_sem=first_send_sem.at[off - 2],
            recv_sem=first_recv_sem.at[off - 2],
            device_id=(gx, peer),
            device_id_type=MESH,
        )

    put_in_order(0)
    pl.semaphore_wait(barrier, n_gy - 1 + n_gx - 1)
    first_copies = [first_send(off) for off in FIRST_ORDER]
    for copy in first_copies:
        copy.start()

    tile_lane = lax.broadcasted_iota(jnp.int32, (n_gy, 8, LANES), 2)
    groups = rows // 8
    local_tokens = sum(jnp.sum(length) for length in lens)

    def tiles(columns, base):
        out = base
        for f, column in enumerate(columns):
            split = column.reshape(n_gy, groups, 8, 1)
            for g in range(groups):
                out = jnp.where(tile_lane == g * 4 + f, split[:, g], out)
        return out

    def column_in(tile, f):
        parts = [tile[:, :, g * 4 + f : g * 4 + f + 1][:, None] for g in range(groups)]
        return jnp.concatenate(parts, axis=1)

    own_len = row_sums(place, targets, lens)
    rewards = [reward_ref[m : m + 1, :].astype(f32) * 0.25 for m in range(members_dev)]
    own_reward = row_sums(place, targets, rewards)
    info_send[...] = tiles((own_len, own_reward), jnp.broadcast_to(local_tokens, (n_gy, 8, LANES)))

    def tile_sends(src, dst, send, recv, offs):
        copies = []
        for off in offs:
            peer = partner(gy, off, n_gy)
            copies.append(
                pltpu.make_async_remote_copy(
                    src_ref=src.at[off % 2 * chips + peer // 2],
                    dst_ref=dst.at[gy],
                    send_sem=send.at[off - 1],
                    recv_sem=recv.at[off - 1],
                    device_id=(gx, peer),
                    device_id_type=MESH,
                )
            )
        return copies

    mate_info = pltpu.make_async_remote_copy(
        src_ref=info_send.at[pl.ds(chips, chips)],
        dst_ref=info_got,
        send_sem=info_send_sem.at[0],
        recv_sem=info_recv_sem.at[0],
        device_id=(gx, mate),
        device_id_type=MESH,
    )
    info_copies = [mate_info] + tile_sends(info_send, info_recv, info_send_sem, info_recv_sem, range(2, n_gy))
    for copy in info_copies:
        copy.start()

    def order_step(c, carry):
        put_in_order(c)
        for t in range(1, chips):
            give(c, peer_of(chip, t, chips)).start()
        return carry

    lax.fori_loop(1, CHUNKS, order_step, 0)
    give_own.start()

    mate_info.wait()
    pair_lens = jnp.concatenate(
        [own_len[: chips * rows].reshape(chips, 1, rows, 1), column_in(info_got[...], 0).reshape(chips, 1, rows, 1)], axis=1
    ).reshape(total_rows, 1)
    row = lax.broadcasted_iota(jnp.int32, (1, total_rows), 1)
    column = lax.broadcasted_iota(jnp.int32, (total_rows, 1), 0)

    def pair_index(i):
        inside = lax.rem(i, pool)
        return (lax.rem(inside // rows + core, 2) * rows + lax.rem(inside, rows)).astype(f32)

    pair_row = row_of(pair_lens)
    spot_row, _ = strip_plan(
        pair_row, pair_lens, (row // pool).astype(f32), (column // pool).astype(f32), pair_index(row), pair_index(column),
        chips, seq,
    )
    wide = lax.broadcasted_iota(jnp.int32, (total_rows, total_rows), 0).astype(f32)

    def strip_counts(spots, lens_row):
        return row_sums(wide, [spots + (row // pool).astype(f32) * pool], [tail_blocks(lens_row)])

    pair_counts = strip_counts(spot_row, pair_row)
    cnt[...] = jnp.broadcast_to(pair_counts, cnt.shape)
    fill = jnp.sum(pair_counts.reshape(chips, HALVES, ROLES, 8, 1), axis=2)
    sent_chip = lax.broadcasted_iota(jnp.int32, fill.shape, 0) != chip
    local_fill = jnp.max(jnp.where(sent_chip, fill, 0.0))
    square = lax.broadcasted_iota(jnp.int32, (pool, pool), 0).astype(f32)
    for s in range(chips):
        deal[s] = jnp.where(square == spot_row[:, s * pool : (s + 1) * pool], 1.0, 0.0).astype(jnp.bfloat16)
    pltpu.make_async_copy(given, given, give_recv_sem.at[0]).wait()

    chip_x, chip_y = peer_of(chip, 1, chips), peer_of(chip, 2, chips)

    def relay(src, dst, there, send, recv, half):
        return pltpu.make_async_remote_copy(
            src_ref=src,
            dst_ref=dst,
            send_sem=send.at[half],
            recv_sem=recv.at[half],
            device_id=(gx, there * 2 + core),
            device_id_type=MESH,
        )

    def near_sends(there, t):
        return [
            relay(sendbuf.at[there, half], recvbuf.at[chip, half], there, strip_send_sem.at[t], strip_recv_sem.at[t], half)
            for half in range(HALVES)
        ]

    reach = 2 * nblocks

    def pack(there):
        for c in range(1, CHUNKS):
            both = jnp.concatenate(
                [ordered[0, there, :, c * width : (c + 1) * width], got[there, :, c * width : (c + 1) * width]], axis=0
            )
            roles[:, (c - 1) * width : c * width] = permuted(deal[there], both)
        for half in range(HALVES):

            def count(role):
                at = there * pool + half * ROLES * 8 + role * 8
                return cnt[pl.ds(pl.multiple_of(at, 8), 8), :]

            def blocks(role):
                at = half * ROLES * 8 + role * 8
                return [roles[at : at + 8, j * LANES : (j + 1) * LANES] for j in range(nblocks)]

            def side(outer, inner):
                n = count(outer)
                behind = shifted_up(blocks(inner), shift_bits(n), reach)
                near_end = blocks(outer)
                return [jnp.where(n > p, near_end[p], behind[p]) for p in range(nblocks)] + behind[nblocks:]

            left, right = side(0, 1), side(3, 2)
            left_n = count(0) + count(1)
            for p in range(STRIP_BLOCKS):
                q = STRIP_BLOCKS - 1 - p
                if q >= reach:
                    value = left[p]
                elif p >= reach:
                    value = right[q]
                else:
                    value = jnp.where(left_n > p, left[p], right[q])
                sendbuf[there, half, :, p * LANES : (p + 1) * LANES] = value

    far = peer_of(chip, chips - 1, chips)
    pack(far)
    first_legs = [relay(sendbuf.at[far, half], passing.at[half], chip_x, first_leg_send_sem, first_leg_recv_sem, half) for half in range(HALVES)]
    for copy in first_legs:
        copy.start()

    def near_step(t, carry):
        pack(peer_of(chip, 2 - t, chips))

        @pl.when(t == 0)
        def _():
            for copy in near_sends(chip_y, 1):
                copy.start()

        return carry

    lax.fori_loop(0, 2, near_step, 0)

    info_recv[gy] = info_send[chip]
    for copy in info_copies[1:]:
        copy.wait()
    info_recv[mate] = info_got[chip]
    arrived = info_recv[...]
    counts[0] = jnp.sum(arrived, axis=0)

    def axis_sends(buf, send, recv):
        return [
            pltpu.make_async_remote_copy(
                src_ref=buf.at[0],
                dst_ref=buf.at[off],
                send_sem=send.at[off - 1],
                recv_sem=recv.at[off - 1],
                device_id=(lax.rem(gx + off, n_gx), gy),
                device_id_type=MESH,
            )
            for off in range(1, n_gx)
        ]

    count_copies = axis_sends(counts, count_send_sem, count_recv_sem)
    for copy in count_copies:
        copy.start()

    eye = lax.broadcasted_iota(jnp.int32, (slots, slots), 0) == lax.broadcasted_iota(jnp.int32, (slots, slots), 1)
    for m in range(members_dev):
        len_col[m] = jnp.broadcast_to(jnp.sum(jnp.where(eye, lens[m], 0.0), axis=1, keepdims=True), (slots, LANES))
    sum_policy[...] = jnp.zeros_like(sum_policy)
    sum_kl[...] = jnp.zeros_like(sum_kl)

    def sum_step(c, carry):
        positions = (lax.broadcasted_iota(jnp.int32, (slots, width), 1) + c * width).astype(f32)
        for m in range(members_dev):
            pol = policy[c, m]
            log_ratio = anchor[c, m] - pol
            ratio = jnp.exp(log_ratio)
            valid = positions < len_col[m][:, :1]
            sum_policy[m] += folded(jnp.where(valid, pol, 0.0))
            sum_kl[m] += folded(jnp.where(valid, kl_weight * (ratio - log_ratio - 1.0), 0.0))
        return carry

    lax.fori_loop(0, CHUNKS, sum_step, 0)
    sums = []
    for buf in (sum_policy, sum_kl):
        per_member = [row_of(jnp.sum(buf[m], axis=1, keepdims=True)) for m in range(members_dev)]
        sums.append(row_sums(place, targets, per_member))
    tails_send[...] = tiles(sums, jnp.broadcast_to(local_fill, (n_gy, 8, LANES)))
    tail_copies = tile_sends(tails_send, tails_recv, tail_send_sem, tail_recv_sem, range(1, n_gy))
    for copy in tail_copies:
        copy.start()
    tails_recv[gy] = tails_send[chip]

    for copy in near_sends(chip_x, 0):
        copy.start()


    for copy in count_copies:
        copy.wait()
    tokens = counts[0]
    for off in range(1, n_gx):
        tokens = tokens + counts[off]
    ntok = tokens[:1, info_lane : info_lane + 1]
    scale = samples * seq / ntok
    got_len = column_in(arrived, 0).reshape(total_rows, 1)
    got_row = row_of(got_len)
    reward = column_in(arrived, 1).reshape(members, part, 1)
    advantage = (members * reward - jnp.sum(reward, axis=0)[None]) / (members - 1)
    adv_rows[...] = jnp.broadcast_to(advantage, adv_rows.shape)
    len_rows[...] = jnp.broadcast_to(got_len.reshape(members, part, 1), len_rows.shape)
    got_spot_row, got_spot = strip_plan(
        got_row, got_len, (row // pool).astype(f32), (column // pool).astype(f32),
        lax.rem(row, pool).astype(f32), lax.rem(column, pool).astype(f32), chips, seq,
    )
    rcnt[...] = jnp.broadcast_to(strip_counts(got_spot_row, got_row), rcnt.shape)
    lane = lax.broadcasted_iota(jnp.int32, (total_rows, LANES), 1).astype(f32)
    for half in range(HALVES):
        pick = got_spot - half * ROLES * 8 == lane
        pick = jnp.where(pick & (lane < ROLES * 8), 1.0, 0.0).astype(jnp.bfloat16)
        undeal[:, half] = pick.reshape(chips, pool, LANES)
    half_rows[...] = jnp.broadcast_to(jnp.where(got_spot < ROLES * 8, 0.0, 1.0).reshape(members, part, 1), half_rows.shape)
    lane_width = lax.broadcasted_iota(jnp.int32, (part, width), 1).astype(f32)

    def finish_rows(k, start, value, only=None):
        value = (value - adv_rows[k][:, :1]) * scale
        valid = lane_width < len_rows[k][:, :1] - start
        value = jnp.where(valid, value, 0.0)
        if only is not None:
            value = jnp.where(only, value, done[k, :, start : start + width])
        done[k, :, start : start + width] = value

    def own_step(which, source):
        for m in range(members_dev):
            for c in range(CHUNKS):
                finish_rows(source * members_dev + m, c * width, which(m * part, c * width))

    own_step(lambda r, s: ordered[0, chip, r : r + part, s : s + width], gy)
    give_own.wait_recv()
    own_step(lambda r, s: got[chip, r : r + part, s : s + width], mate)

    def first_wait(off):
        landed = heads_in.at[0]
        pltpu.make_async_copy(landed, landed, first_recv_sem.at[off - 2]).wait()

    def first_step(off, carry):
        first_wait(off)
        source = peer_of(gy, off, n_gy)
        for m in range(members_dev):
            finish_rows(source * members_dev + m, 0, heads_in[source, m * part : (m + 1) * part, :])
        return carry

    lax.fori_loop(2, n_gy, first_step, 0)

    def unpack(there, t, half):
        landed = recvbuf.at[0, 0]
        pltpu.make_async_copy(landed, landed, strip_recv_sem.at[t, half]).wait()

        def put(r, c, rows):
            k = there * 2 * members_dev + r
            finish_rows(k, c * width, rows, half_rows[k][:, :1] > 0.5 if half else None)

        unpack_strips(recvbuf, roles, undeal, rcnt, there, half, width, part, put)

    second_legs = [
        relay(passing.at[half], recvbuf.at[chip_x, half], chip_y, strip_send_sem.at[2], strip_recv_sem.at[2], half)
        for half in range(HALVES)
    ]
    for first_leg, second_leg in zip(first_legs, second_legs):
        first_leg.wait_recv()
        second_leg.start()
    for half in range(HALVES):
        unpack(chip_y, 1, half)

    for copy in tail_copies:
        copy.wait()
    ends = tails_recv[...]
    needs[0] = jnp.max(ends, axis=0)
    need_copies = axis_sends(needs, need_send_sem, need_recv_sem)
    for copy in need_copies:
        copy.start()
    first_sum = column_in(ends, 0).reshape(members, part, 1)
    second_sum = column_in(ends, 1).reshape(members, part, 1)
    value = (second_sum - advantage * first_sum) * (samples / ntok)[None]
    shape = (members, part, LANES)
    spread = lax.broadcasted_iota(jnp.int32, shape, 1) == lax.broadcasted_iota(jnp.int32, shape, 2)
    loss_ref[...] = jnp.sum(jnp.where(spread, value, 0.0), axis=1)[:, :part]
    adv_ref[...] = jnp.sum(jnp.where(spread, advantage, 0.0), axis=1)[:, :part]
    for copy in need_copies:
        copy.wait()
    fullest = needs[0]
    for off in range(1, n_gx):
        fullest = jnp.maximum(fullest, needs[off])
    over_ref[0, 0] = (jnp.max(fullest[:, fill_lane : fill_lane + 1]) > STRIP_BLOCKS).astype(jnp.int32)
    for copy in first_copies:
        copy.wait_send()
    pltpu.make_async_copy(given, given, give_send_sem.at[0]).wait()
    give_own.wait_send()

    scale_ref[...] = jnp.broadcast_to(scale, scale_ref.shape)

    def unpack_step(i, carry):
        unpack(peer_of(chip, 1 + 2 * i, chips), 2 * i, 0)
        return carry

    lax.fori_loop(0, 2, unpack_step, 0)
    for t in (0, 2):
        landed = recvbuf.at[0, 0]
        pltpu.make_async_copy(landed, landed, strip_recv_sem.at[t, 1]).wait()
    for half in range(HALVES):
        first_legs[half].wait_send()
        for t in range(chips - 1):
            sent = sendbuf.at[0, 0]
            pltpu.make_async_copy(sent, sent, strip_send_sem.at[t, half]).wait()


def store(
    n_gy, done, loss, adv, recvbuf, undeal, rcnt, len_rows, adv_rows, half_rows, scale_ref,
    grad, loss_out, adv_out, last, roles, sem,
):
    chips = n_gy // 2
    members, part, seq = done.shape
    group = members // chips
    width = seq - roles.shape[1]
    chip = lax.axis_index("gy") // 2
    scale = scale_ref[:1, :1]
    lane_width = lax.broadcasted_iota(jnp.int32, (part, width), 1).astype(jnp.float32)

    def chip_rows(there):
        return pl.ds(there * group, group)

    whole = [chip_rows(chip), chip_rows(peer_of(chip, 2, chips))]
    late = [peer_of(chip, 1, chips), peer_of(chip, 3, chips)]
    first = pl.ds(0, width)
    copies = [pltpu.make_async_copy(done.at[rows], grad.at[rows], sem.at[k]) for k, rows in enumerate(whole)]
    copies += [
        pltpu.make_async_copy(done.at[chip_rows(there), :, first], grad.at[chip_rows(there), :, first], sem.at[2 + k])
        for k, there in enumerate(late)
    ]
    copies += [pltpu.make_async_copy(loss, loss_out, sem.at[4]), pltpu.make_async_copy(adv, adv_out, sem.at[5])]
    for copy in copies:
        copy.start()

    def store_late(i):
        rows = chip_rows(peer_of(chip, 1 + 2 * i, chips))
        return pltpu.make_async_copy(last.at[i], grad.at[rows, :, pl.ds(width, seq - width)], sem.at[6 + i])

    def late_step(i, carry):
        there = peer_of(chip, 1 + 2 * i, chips)

        def put(r, c, rows):
            k = there * group + r
            value = (rows - adv_rows[k][:, :1]) * scale
            valid = lane_width < len_rows[k][:, :1] - c * width
            before = done[k, :, c * width : (c + 1) * width]
            value = jnp.where(half_rows[k][:, :1] > 0.5, jnp.where(valid, value, 0.0), before)
            last[i, r, :, (c - 1) * width : c * width] = value

        unpack_strips(recvbuf, roles, undeal, rcnt, there, 1, width, part, put)
        store_late(i).start()
        return carry

    lax.fori_loop(0, 2, late_step, 0)
    copies += [store_late(i) for i in range(2)]
    for copy in copies:
        copy.wait()


def packed_body(n_gx, n_gy, policy_logp, anchor_logp, lengths, rewards, slot_prompt):
    members_dev, slots, seq = policy_logp.shape
    members, part = members_dev * n_gy, slots // n_gy
    f32, bf16 = jnp.float32, jnp.bfloat16
    chips, rows = n_gy // 2, members_dev * part
    pool = 2 * rows
    width = seq // CHUNKS
    chunked = (CHUNKS, members_dev, slots, width)
    strips = (chips, HALVES, 8, STRIP_BLOCKS * LANES)
    per_slot = (members_dev, slots, LANES)
    per_sample = (members, part, LANES)
    tile = (n_gy, 8, LANES)
    hbm_spec = pl.BlockSpec(memory_space=pltpu.HBM)
    vmem_spec = pl.BlockSpec(memory_space=pltpu.VMEM)
    dma = pltpu.SemaphoreType.DMA
    handed = (
        pltpu.VMEM(strips, f32),
        pltpu.VMEM((chips, HALVES, pool, LANES), bf16),
        pltpu.VMEM((chips * pool, LANES), f32),
        pltpu.VMEM(per_sample, f32),
        pltpu.VMEM(per_sample, f32),
        pltpu.VMEM(per_sample, f32),
        pltpu.VMEM((8, LANES), f32),
    )
    done, loss, adv, over, *rest = pl.pallas_call(
        functools.partial(packed_exchange, n_gx, n_gy),
        out_shape=(
            pltpu.VMEM((members, part, seq), f32),
            pltpu.VMEM((members, part), f32),
            pltpu.VMEM((members, part), f32),
            pltpu.SMEM((1, 1), jnp.int32),
        ) + handed,
        in_specs=[hbm_spec] * 5,
        out_specs=(vmem_spec,) * 3 + (pl.BlockSpec(memory_space=pltpu.SMEM),) + (vmem_spec,) * len(handed),
        scratch_shapes=[
            pltpu.VMEM(chunked, f32),
            pltpu.VMEM(chunked, f32),
            pltpu.VMEM((members_dev, slots), jnp.int32),
            pltpu.VMEM((members_dev, slots), jnp.int32),
            pltpu.VMEM((members_dev, slots), jnp.int32),
            pltpu.VMEM((2 * chips * rows, members_dev * slots), bf16),
            pltpu.VMEM((2, chips, rows, seq), f32),
            pltpu.VMEM((chips, rows, seq), f32),
            pltpu.VMEM((n_gy, rows, width), f32),
            pltpu.VMEM(strips, f32),
            pltpu.VMEM(strips[1:], f32),
            pltpu.VMEM((pool, seq - width), f32),
            pltpu.VMEM((chips, pool, pool), bf16),
            pltpu.VMEM((chips * pool, LANES), f32),
            pltpu.VMEM(per_slot, f32),
            pltpu.VMEM(per_slot, f32),
            pltpu.VMEM(per_slot, f32),
            pltpu.VMEM(tile, f32),
            pltpu.VMEM((chips, 8, LANES), f32),
            pltpu.VMEM(tile, f32),
            pltpu.VMEM(tile, f32),
            pltpu.VMEM(tile, f32),
            pltpu.VMEM((n_gx, 8, LANES), f32),
            pltpu.VMEM((n_gx, 8, LANES), f32),
            dma((3,)),
            dma((2, CHUNKS)),
            dma((2,)),
            dma((2,)),
            dma((n_gy - 2,)),
            dma((n_gy - 2,)),
            dma((chips - 1, HALVES)),
            dma((chips - 1, HALVES)),
            dma((HALVES,)),
            dma((HALVES,)),
            dma((n_gy - 1,)),
            dma((n_gy - 1,)),
            dma((n_gy - 1,)),
            dma((n_gy - 1,)),
            dma((n_gx - 1,)),
            dma((n_gx - 1,)),
            dma((n_gx - 1,)),
            dma((n_gx - 1,)),
        ],
        compiler_params=pltpu.CompilerParams(collective_id=0, has_side_effects=True, vmem_limit_bytes=36 * 2**20),
    )(policy_logp, anchor_logp, lengths, rewards, slot_prompt)

    def fits(policy_logp, anchor_logp, lengths, rewards, slot_prompt, done, loss, adv, *rest):
        small = jax.ShapeDtypeStruct((members, part), f32)
        return tuple(pl.pallas_call(
            functools.partial(store, n_gy),
            out_shape=(jax.ShapeDtypeStruct((members, part, seq), f32), small, small),
            in_specs=[vmem_spec] * (3 + len(rest)),
            out_specs=(hbm_spec,) * 3,
            scratch_shapes=[
                pltpu.VMEM((2, 2 * members_dev, part, seq - width), f32),
                pltpu.VMEM((ROLES * 8, seq - width), f32),
                dma((8,)),
            ],
            compiler_params=pltpu.CompilerParams(vmem_limit_bytes=16 * 2**20),
        )(done, loss, adv, *rest))

    def overflows(policy_logp, anchor_logp, lengths, rewards, slot_prompt, done, loss, adv, *rest):
        return tuple(unpacked_body(n_gx, n_gy, policy_logp, anchor_logp, lengths, rewards, slot_prompt))

    return lax.cond(
        over[0, 0] > 0, overflows, fits,
        policy_logp, anchor_logp, lengths, rewards, slot_prompt, done, loss, adv, *rest,
    )


def body(n_gx, n_gy, *args):
    members_dev, slots, seq = args[0].shape
    pool = 2 * members_dev * slots // n_gy
    packs = n_gy == 8 and pool == ROLES * STRIPS and slots == LANES and seq == LANES * 32 and seq == CHUNKS * HEAD_BLOCKS * LANES
    return (packed_body if packs else unpacked_body)(n_gx, n_gy, *args)


def solution(mesh):
    placed = (P("gy", "gx", None), P("gy", "gx", None), P("gy", "gx"), P("gy", "gx"), P("gy", "gx"))
    return jax.shard_map(
        functools.partial(body, mesh.shape["gx"], mesh.shape["gy"]),
        mesh=mesh,
        in_specs=placed,
        out_specs=(P(None, ("gx", "gy"), None), P(None, ("gx", "gy")), P(None, ("gx", "gy"))),
        check_vma=False,
    )
```

```python
import functools

import jax
import jax.numpy as jnp
from jax import lax
from jax.experimental import pallas as pl
from jax.experimental.pallas import tpu as pltpu
from jax.sharding import PartitionSpec as P

kl_weight = 0.1
LANES = 128
CHUNKS = 8
MESH = pl.DeviceIdType.MESH
ROLES = 4
STRIPS = 16
HALVES = STRIPS // 8
SHIFTS = 5
PIECES = 8
DEALS = 1
UNDEALS = 1
HEAD_BLOCKS = 6
STRIP_BLOCKS = 66
FIRST_ORDER = (2, 4, 3, 5, 6, 7)


def partner(index, off, count):
    out, bit = index, 1
    while bit < count:
        if off & bit:
            out = out + bit - 2 * bit * lax.rem(index // bit, 2)
        bit *= 2
    return out


def offsets_by_distance(count):
    far = max(bin(off // 2).count("1") for off in range(1, count))
    near = [off for off in range(1, count) if bin(off // 2).count("1") < far]
    return near, [off for off in range(1, count) if off not in near]


def permuted(onehot, rows):
    high = rows.astype(jnp.bfloat16)
    rest = rows - high.astype(jnp.float32)
    middle = rest.astype(jnp.bfloat16)
    low = (rest - middle.astype(jnp.float32)).astype(jnp.bfloat16)
    dot = functools.partial(jnp.dot, preferred_element_type=jnp.float32)
    return dot(onehot, high) + dot(onehot, middle) + dot(onehot, low)


def folded(x):
    out = x[:, :LANES]
    for start in range(LANES, x.shape[1], LANES):
        out = out + x[:, start : start + LANES]
    return out


def exchange(
    n_gx, n_gy, policy_hbm, anchor_hbm, len_ref, reward_ref, prompt_ref,
    raw_hbm, heads_ref, tails_ref, ntok_ref,
    policy, anchor, sendbuf, onehot, len_col, sum_policy, sum_kl,
    heads_send, heads_recv, tails_send, tails_recv, counts,
    load_sem, send_sem, recv_sem, own_sem,
    head_send_sem, head_recv_sem, tail_send_sem, tail_recv_sem, count_send_sem, count_recv_sem,
):
    gx, gy = lax.axis_index("gx"), lax.axis_index("gy")
    members_dev, slots, seq = policy_hbm.shape
    part = slots // n_gy
    width = seq // CHUNKS

    near, far = offsets_by_distance(n_gy)
    barrier = pltpu.get_barrier_semaphore()
    for off in range(1, n_gy):
        pl.semaphore_signal(barrier, inc=1, device_id=(gx, partner(gy, off, n_gy)), device_id_type=MESH)
    for off in range(1, n_gx):
        pl.semaphore_signal(barrier, inc=1, device_id=(lax.rem(gx + off, n_gx), gy), device_id_type=MESH)

    def loads(c):
        cols = pl.ds(pl.multiple_of(c * width, LANES), width)
        return (
            pltpu.make_async_copy(policy_hbm.at[:, :, cols], policy.at[c], load_sem.at[0, c]),
            pltpu.make_async_copy(anchor_hbm.at[:, :, cols], anchor.at[c], load_sem.at[1, c]),
        )

    for c in range(CHUNKS):
        for copy in loads(c):
            copy.start()

    sublane = lax.broadcasted_iota(jnp.int32, (slots, slots), 0)
    lane = lax.broadcasted_iota(jnp.int32, (slots, slots), 1)
    column = lax.broadcasted_iota(jnp.int32, (slots, LANES), 1)
    local_tokens = jnp.sum(len_ref[...].astype(jnp.float32))
    for m in range(members_dev):
        seq_len = len_ref[m : m + 1, :].astype(jnp.float32)
        reward = reward_ref[m : m + 1, :].astype(jnp.float32) * 0.25
        match = sublane == lax.rem(prompt_ref[m : m + 1, :], slots)
        onehot[m] = jnp.where(match, 1.0, 0.0).astype(jnp.bfloat16)
        len_col[m] = jnp.broadcast_to(
            jnp.sum(jnp.where(sublane == lane, seq_len, 0.0), axis=1, keepdims=True), (slots, LANES)
        )
        sorted_len = jnp.sum(jnp.where(match, seq_len, 0.0), axis=1, keepdims=True)
        sorted_reward = jnp.sum(jnp.where(match, reward, 0.0), axis=1, keepdims=True)
        heads_send[m] = jnp.where(
            column == 0, sorted_len, jnp.where(column == 1, sorted_reward, local_tokens)
        )
    sum_policy[...] = jnp.zeros_like(sum_policy)
    sum_kl[...] = jnp.zeros_like(sum_kl)

    def compute(c):
        for copy in loads(c):
            copy.wait()
        positions = (lax.broadcasted_iota(jnp.int32, (slots, width), 1) + c * width).astype(jnp.float32)
        for m in range(members_dev):
            pol = policy[c, m]
            log_ratio = anchor[c, m] - pol
            ratio = jnp.exp(log_ratio)
            valid = positions < len_col[m][:, :1]
            sum_policy[m] += folded(jnp.where(valid, pol, 0.0))
            sum_kl[m] += folded(jnp.where(valid, kl_weight * (ratio - log_ratio - 1.0), 0.0))
            sendbuf[c, m] = permuted(onehot[m], kl_weight * (1.0 - ratio))

    def rows_of(device):
        return pl.ds(pl.multiple_of(device * part, part), part)

    my_members = pl.ds(gy * members_dev, members_dev)

    def sends(c, offs):
        cols = pl.ds(pl.multiple_of(c * width, LANES), width)
        copies = []
        for off in offs:
            peer = partner(gy, off, n_gy)
            copies.append(
                pltpu.make_async_remote_copy(
                    src_ref=sendbuf.at[c, :, rows_of(peer), :],
                    dst_ref=raw_hbm.at[my_members, :, cols],
                    send_sem=send_sem.at[off - 1],
                    recv_sem=recv_sem.at[off - 1],
                    device_id=(gx, peer),
                    device_id_type=MESH,
                )
            )
        return copies

    def own(c):
        cols = pl.ds(pl.multiple_of(c * width, LANES), width)
        return pltpu.make_async_copy(
            sendbuf.at[c, :, rows_of(gy), :], raw_hbm.at[my_members, :, cols], own_sem.at[c]
        )

    def small_sends(src, dst, send, recv):
        copies = []
        for off in range(1, n_gy):
            peer = partner(gy, off, n_gy)
            copies.append(
                pltpu.make_async_remote_copy(
                    src_ref=src.at[:, rows_of(peer), :],
                    dst_ref=dst.at[my_members],
                    send_sem=send.at[off - 1],
                    recv_sem=recv.at[off - 1],
                    device_id=(gx, peer),
                    device_id_type=MESH,
                )
            )
        copies.append(pltpu.make_async_copy(src.at[:, rows_of(gy), :], dst.at[my_members], send.at[n_gy - 1]))
        return copies

    def count_sends():
        return [
            pltpu.make_async_remote_copy(
                src_ref=counts.at[0],
                dst_ref=counts.at[off],
                send_sem=count_send_sem.at[off - 1],
                recv_sem=count_recv_sem.at[off - 1],
                device_id=(lax.rem(gx + off, n_gx), gy),
                device_id_type=MESH,
            )
            for off in range(1, n_gx)
        ]

    compute(0)
    pl.semaphore_wait(barrier, n_gy - 1 + n_gx - 1)
    head_copies = small_sends(heads_send, heads_recv, head_send_sem, head_recv_sem)
    for copy in head_copies:
        copy.start()

    def step(c, carry):
        for copy in sends(c - 1, near):
            copy.start()
        own(c - 1).start()
        compute(c)
        return carry

    lax.fori_loop(1, CHUNKS, step, 0)
    for copy in sends(CHUNKS - 1, near):
        copy.start()

    def far_step(c, carry):
        for copy in sends(c, far):
            copy.start()
        return carry

    lax.fori_loop(0, CHUNKS, far_step, 0)
    own(CHUNKS - 1).start()

    for m in range(members_dev):
        s1 = jnp.sum(permuted(onehot[m], sum_policy[m]), axis=1, keepdims=True)
        s2 = jnp.sum(permuted(onehot[m], sum_kl[m]), axis=1, keepdims=True)
        tails_send[m] = jnp.where(column == 0, s1, s2)
    for copy in head_copies:
        copy.wait()
    tokens = jnp.zeros((8, LANES), jnp.float32)
    for source in range(n_gy):
        tokens = tokens + heads_recv[source * members_dev, :8, :]
    counts[0] = tokens
    heads_ref[...] = heads_recv[...]
    tail_copies = small_sends(tails_send, tails_recv, tail_send_sem, tail_recv_sem)
    for copy in tail_copies:
        copy.start()
    count_copies = count_sends()
    for copy in count_copies:
        copy.start()
    for copy in count_copies:
        copy.wait()
    ntok_ref[...] = jnp.sum(counts[...], axis=0)
    for copy in tail_copies:
        copy.wait()
    tails_ref[...] = tails_recv[...]
    for c in range(CHUNKS):
        own(c).wait()
    for off in range(1, n_gy):
        source = partner(gy, off, n_gy)
        landed = raw_hbm.at[pl.ds(source * members_dev, members_dev)]
        pltpu.make_async_copy(landed, landed, recv_sem.at[off - 1]).wait()
        pltpu.make_async_copy(landed, landed, send_sem.at[off - 1]).wait()


def finish(samples, raw, heads, tails, ntok, grad, loss, adv, done, done_sem):
    members, part, seq = raw.shape
    tokens = ntok[:1, 2:3]
    total = jnp.sum(heads[...], axis=0)
    advantage = (members * heads[:, :, 1:2] - total[None, :, 1:2]) / (members - 1)
    positions = lax.broadcasted_iota(jnp.int32, (part, seq), 1).astype(jnp.float32)
    scale = samples * seq / tokens

    def store(k):
        return pltpu.make_async_copy(done.at[k], grad.at[k], done_sem.at[k])

    for k in range(members):
        done[k] = jnp.where(positions < heads[k, :, :1], raw[k] - advantage[k], 0.0) * scale
        if k > 0:
            store(k - 1).start()
    shape = (members, part, LANES)
    eye = lax.broadcasted_iota(jnp.int32, shape, 1) == lax.broadcasted_iota(jnp.int32, shape, 2)
    store(members - 1).start()
    value = (tails[:, :, 1:2] - advantage * tails[:, :, :1]) * (samples / tokens)[None]
    loss[...] = jnp.sum(jnp.where(eye, value, 0.0), axis=1)[:, :part]
    adv[...] = jnp.sum(jnp.where(eye, advantage, 0.0), axis=1)[:, :part]
    for k in range(members):
        store(k).wait()


def unpacked_body(n_gx, n_gy, policy_logp, anchor_logp, lengths, rewards, slot_prompt):
    members_dev, slots, seq = policy_logp.shape
    members, part = members_dev * n_gy, slots // n_gy
    f32 = jnp.float32
    chunked = (CHUNKS, members_dev, slots, seq // CHUNKS)
    small = (members, part, LANES)
    hbm_spec = pl.BlockSpec(memory_space=pltpu.HBM)
    vmem_spec = pl.BlockSpec(memory_space=pltpu.VMEM)
    dma = pltpu.SemaphoreType.DMA
    raw, heads, tails, ntok = pl.pallas_call(
        functools.partial(exchange, n_gx, n_gy),
        out_shape=(
            pltpu.VMEM((members, part, seq), f32),
            pltpu.VMEM(small, f32),
            pltpu.VMEM(small, f32),
            pltpu.VMEM((8, LANES), f32),
        ),
        in_specs=[hbm_spec, hbm_spec, vmem_spec, vmem_spec, vmem_spec],
        out_specs=(vmem_spec, vmem_spec, vmem_spec, vmem_spec),
        scratch_shapes=[
            pltpu.VMEM(chunked, f32),
            pltpu.VMEM(chunked, f32),
            pltpu.VMEM(chunked, f32),
            pltpu.VMEM((members_dev, slots, slots), jnp.bfloat16),
            pltpu.VMEM((members_dev, slots, LANES), f32),
            pltpu.VMEM((members_dev, slots, LANES), f32),
            pltpu.VMEM((members_dev, slots, LANES), f32),
            pltpu.VMEM((members_dev, slots, LANES), f32),
            pltpu.VMEM(small, f32),
            pltpu.VMEM((members_dev, slots, LANES), f32),
            pltpu.VMEM(small, f32),
            pltpu.VMEM((n_gx, 8, LANES), f32),
            dma((2, CHUNKS)),
            dma((n_gy - 1,)),
            dma((n_gy - 1,)),
            dma((CHUNKS,)),
            dma((n_gy,)),
            dma((n_gy - 1,)),
            dma((n_gy,)),
            dma((n_gy - 1,)),
            dma((n_gx - 1,)),
            dma((n_gx - 1,)),
        ],
        compiler_params=pltpu.CompilerParams(collective_id=1, has_side_effects=True, vmem_limit_bytes=36 * 2**20),
    )(policy_logp, anchor_logp, lengths, rewards, slot_prompt)
    samples = members * slots * n_gx
    return pl.pallas_call(
        functools.partial(finish, samples),
        out_shape=(
            jax.ShapeDtypeStruct((members, part, seq), f32),
            jax.ShapeDtypeStruct((members, part), f32),
            jax.ShapeDtypeStruct((members, part), f32),
        ),
        in_specs=[vmem_spec] * 4,
        out_specs=(hbm_spec, vmem_spec, vmem_spec),
        scratch_shapes=[pltpu.VMEM((members, part, seq), f32), dma((members,))],
        compiler_params=pltpu.CompilerParams(vmem_limit_bytes=32 * 2**20),
    )(raw, heads, tails, ntok)


def row_of(column):
    n = column.shape[0]
    eye = lax.broadcasted_iota(jnp.int32, (n, n), 0) == lax.broadcasted_iota(jnp.int32, (n, n), 1)
    return jnp.sum(jnp.where(eye, column, 0.0), axis=0, keepdims=True)


def row_sums(place, targets, values):
    out = None
    for target, value in zip(targets, values):
        here = jnp.sum(jnp.where(place == target, value, 0.0), axis=1, keepdims=True)
        out = here if out is None else out + here
    return out


def strip_spot(rank):
    first, second, third = rank < STRIPS, rank < 2 * STRIPS, rank < 3 * STRIPS
    strip = jnp.where(
        first, rank, jnp.where(second, 2 * STRIPS - 1 - rank, jnp.where(third, 3 * STRIPS - 1 - rank, rank - 3 * STRIPS))
    )
    role = jnp.where(first, 0.0, jnp.where(second, 3.0, jnp.where(third, 2.0, 1.0)))
    half = jnp.floor(strip * (1.0 / 8))
    return half * (ROLES * 8) + role * 8 + strip - half * 8


def strip_plan(len_row, len_column, group_row, group_column, index_row, index_column, n_groups, seq):
    rows = ROLES * STRIPS
    key_row = group_row * ((seq + 1) * rows) + len_row * rows + index_row
    key_column = group_column * ((seq + 1) * rows) + len_column * rows + index_column
    above_row = jnp.sum(jnp.where(key_column > key_row, 1.0, 0.0), axis=0, keepdims=True)
    above_column = jnp.sum(jnp.where(key_row > key_column, 1.0, 0.0), axis=1, keepdims=True)
    return (
        strip_spot(above_row - rows * (n_groups - 1 - group_row)),
        strip_spot(above_column - rows * (n_groups - 1 - group_column)),
    )


def tail_blocks(lens):
    return jnp.maximum(jnp.floor((lens + (LANES - 1)) * (1.0 / LANES)) - HEAD_BLOCKS, 0.0)


def shift_bits(count):
    shift = count.astype(jnp.int32)
    return [(lax.shift_right_logical(shift, k) & 1) == 1 for k in range(SHIFTS)]


def shifted_up(blocks, bits, reach):
    for k in range(SHIFTS):
        step, n = 2**k, len(blocks)
        moved = []
        for p in range(min(n + step, reach)):
            if p < step:
                moved.append(blocks[p])
            elif p >= n:
                moved.append(blocks[p - step])
            else:
                moved.append(jnp.where(bits[k], blocks[p - step], blocks[p]))
        blocks = moved
    return blocks


def shifted_down(blocks, bits, count):
    for k in reversed(range(SHIFTS)):
        step = 2**k
        keep = min(len(blocks), count + step - 1)
        blocks = [
            jnp.where(bits[k], blocks[p + step], blocks[p]) if p + step < len(blocks) else blocks[p] for p in range(keep)
        ]
    return blocks


def peer_of(index, off, count):
    out, bit = 0, 1
    while bit < count:
        a, b = lax.rem(index // bit, 2), lax.rem(off // bit, 2)
        out = out + bit * (a + b - 2 * a * b)
        bit *= 2
    return out


def unpack_strips(recvbuf, roles, undeal, rcnt, there, half, part, put):
    pool, seq_tail = undeal.shape[2], roles.shape[1]
    nblocks = seq_tail // LANES

    def count(role):
        at = there * pool + half * ROLES * 8 + role * 8
        return rcnt[pl.ds(pl.multiple_of(at, 8), 8), :]

    def block(p):
        return recvbuf[there, half, :, p * LANES : (p + 1) * LANES]

    for outer, inner, at in ((0, 1, lambda p: p), (3, 2, lambda p: STRIP_BLOCKS - 1 - p)):
        for j in range(nblocks):
            roles[outer * 8 : outer * 8 + 8, j * LANES : (j + 1) * LANES] = block(at(j))
        behind = [block(at(p)) for p in range(2 * nblocks)]
        behind = shifted_down(behind, shift_bits(count(outer)), nblocks)
        for j in range(nblocks):
            roles[inner * 8 : inner * 8 + 8, j * LANES : (j + 1) * LANES] = behind[j]
    order = undeal[there, half][:, : ROLES * 8]
    span = seq_tail // UNDEALS

    def undeal_step(i, carry):
        start = pl.multiple_of(i * span, LANES)
        out = permuted(order, roles[: ROLES * 8, pl.ds(start, span)])
        for r in range(pool // part):
            put(r, start, out[r * part : (r + 1) * part])
        return carry

    lax.fori_loop(0, UNDEALS, undeal_step, 0)


def packed_exchange(
    n_gx, n_gy, policy_hbm, anchor_hbm, len_hbm, reward_hbm, prompt_hbm,
    done, loss_ref, adv_ref, over_ref, recvbuf, undeal, rcnt, len_rows, adv_rows, half_rows, scale_ref,
    policy, anchor, len_ref, reward_ref, prompt_ref, onehot, ordered, got, heads_in, sendbuf, passing, roles,
    deal, cnt, len_col, sum_policy, sum_kl,
    info_send, info_got, info_recv, tails_send, tails_recv, counts, needs,
    small_sem, load_sem, give_send_sem, give_recv_sem, first_send_sem, first_recv_sem, strip_send_sem, strip_recv_sem, first_leg_send_sem, first_leg_recv_sem,
    info_send_sem, info_recv_sem, tail_send_sem, tail_recv_sem, count_send_sem, count_recv_sem, need_send_sem, need_recv_sem,
):
    gx, gy = lax.axis_index("gx"), lax.axis_index("gy")
    core, chip = lax.rem(gy, 2), gy // 2
    mate = chip * 2 + 1 - core
    members_dev, slots, seq = policy_hbm.shape
    members, part = members_dev * n_gy, slots // n_gy
    chips = n_gy // 2
    width = HEAD_BLOCKS * LANES
    piece = seq // PIECES
    nblocks = seq // LANES - HEAD_BLOCKS
    rows = members_dev * part
    pool = 2 * rows
    total_rows = chips * pool
    samples = members * slots * n_gx
    info_lane, fill_lane = 16, 17
    f32 = jnp.float32

    small_loads = [
        pltpu.make_async_copy(src, dst, small_sem.at[k])
        for k, (src, dst) in enumerate(((len_hbm, len_ref), (prompt_hbm, prompt_ref), (reward_hbm, reward_ref)))
    ]
    for copy in small_loads:
        copy.start()

    def loads(c):
        cols = pl.ds(pl.multiple_of(c * piece, LANES), piece)
        return (
            pltpu.make_async_copy(policy_hbm.at[:, :, cols], policy.at[c], load_sem.at[0, c]),
            pltpu.make_async_copy(anchor_hbm.at[:, :, cols], anchor.at[c], load_sem.at[1, c]),
        )

    for copy in loads(0):
        copy.start()
    barrier = pltpu.get_barrier_semaphore()
    for off in range(1, n_gy):
        pl.semaphore_signal(barrier, inc=1, device_id=(gx, partner(gy, off, n_gy)), device_id_type=MESH)
    for off in range(1, n_gx):
        pl.semaphore_signal(barrier, inc=1, device_id=(lax.rem(gx + off, n_gx), gy), device_id_type=MESH)
    for c in range(1, PIECES):
        for copy in loads(c):
            copy.start()
    for copy in small_loads:
        copy.wait()

    lens = [len_ref[m : m + 1, :].astype(f32) for m in range(members_dev)]
    targets = []
    for m in range(members_dev):
        spot = lax.rem(prompt_ref[m : m + 1, :], slots)
        device = spot // part
        other = lax.rem(device + core, 2)
        target = (other * chips + device // 2) * rows + m * part + spot - device * part
        targets.append(target.astype(f32))
    place = lax.broadcasted_iota(jnp.int32, (total_rows, slots), 0).astype(f32)
    for m in range(members_dev):
        onehot[:, m * slots : (m + 1) * slots] = jnp.where(place == targets[m], 1.0, 0.0).astype(jnp.bfloat16)

    def put_in_order(c):
        for copy in loads(c):
            copy.wait()
        values = kl_weight * (1.0 - jnp.exp(anchor[c] - policy[c]))
        out = permuted(onehot[...], values.reshape(members_dev * slots, piece))
        cols = pl.ds(pl.multiple_of(c * piece, LANES), piece)
        ordered[:, :, :, cols] = out.reshape(2, chips, rows, piece)

    def give(c, there):
        cols = pl.ds(pl.multiple_of(c * piece, LANES), piece)
        return pltpu.make_async_remote_copy(
            src_ref=ordered.at[1, there, :, cols],
            dst_ref=got.at[there, :, cols],
            send_sem=give_send_sem.at[0],
            recv_sem=give_recv_sem.at[0],
            device_id=(gx, mate),
            device_id_type=MESH,
        )

    give_own = pltpu.make_async_remote_copy(
        src_ref=ordered.at[1, chip],
        dst_ref=got.at[chip],
        send_sem=give_send_sem.at[1],
        recv_sem=give_recv_sem.at[1],
        device_id=(gx, mate),
        device_id_type=MESH,
    )
    given = got.at[pl.ds(0, chips - 1), :, pl.ds(piece, seq - piece)]

    def first_send(off, lo, hi):
        peer = partner(gy, off, n_gy)
        cols = pl.ds(lo, hi - lo)
        return pltpu.make_async_remote_copy(
            src_ref=ordered.at[off % 2, peer // 2, :, cols],
            dst_ref=heads_in.at[gy, :, cols],
            send_sem=first_send_sem.at[off - 2],
            recv_sem=first_recv_sem.at[off - 2],
            device_id=(gx, peer),
            device_id_type=MESH,
        )

    tile_lane = lax.broadcasted_iota(jnp.int32, (n_gy, 8, LANES), 2)
    groups = rows // 8
    local_tokens = sum(jnp.sum(length) for length in lens)

    def tiles(columns, base):
        out = base
        for f, column in enumerate(columns):
            split = column.reshape(n_gy, groups, 8, 1)
            for g in range(groups):
                out = jnp.where(tile_lane == g * 4 + f, split[:, g], out)
        return out

    def column_in(tile, f):
        parts = [tile[:, :, g * 4 + f : g * 4 + f + 1][:, None] for g in range(groups)]
        return jnp.concatenate(parts, axis=1)

    def tile_sends(src, dst, send, recv, offs):
        copies = []
        for off in offs:
            peer = partner(gy, off, n_gy)
            copies.append(
                pltpu.make_async_remote_copy(
                    src_ref=src.at[off % 2 * chips + peer // 2],
                    dst_ref=dst.at[gy],
                    send_sem=send.at[off - 1],
                    recv_sem=recv.at[off - 1],
                    device_id=(gx, peer),
                    device_id_type=MESH,
                )
            )
        return copies

    mate_info = pltpu.make_async_remote_copy(
        src_ref=info_send.at[pl.ds(chips, chips)],
        dst_ref=info_got,
        send_sem=info_send_sem.at[0],
        recv_sem=info_recv_sem.at[0],
        device_id=(gx, mate),
        device_id_type=MESH,
    )
    info_copies = [mate_info] + tile_sends(info_send, info_recv, info_send_sem, info_recv_sem, range(2, n_gy))

    def order_step(c, carry):
        put_in_order(c)

        @pl.when(c == 0)
        def _():
            pl.semaphore_wait(barrier, n_gy - 1 + n_gx - 1)
            for off in FIRST_ORDER:
                first_send(off, 0, piece).start()
            lens_out = row_sums(place, targets, lens)
            rewards = [reward_ref[m : m + 1, :].astype(f32) * 0.25 for m in range(members_dev)]
            rewards_out = row_sums(place, targets, rewards)
            info_send[...] = tiles((lens_out, rewards_out), jnp.broadcast_to(local_tokens, (n_gy, 8, LANES)))
            for copy in info_copies:
                copy.start()

        @pl.when(c == 1)
        def _():
            for off in FIRST_ORDER:
                first_send(off, piece, width).start()

        @pl.when(c >= 1)
        def _():
            for t in range(1, chips):
                give(c, peer_of(chip, t, chips)).start()

        return carry

    lax.fori_loop(0, PIECES, order_step, 0)
    give_own.start()
    own_len = column_in(info_send[:chips], 0).reshape(chips * rows, 1)

    mate_info.wait()
    pair_lens = jnp.concatenate(
        [own_len[: chips * rows].reshape(chips, 1, rows, 1), column_in(info_got[...], 0).reshape(chips, 1, rows, 1)], axis=1
    ).reshape(total_rows, 1)
    row = lax.broadcasted_iota(jnp.int32, (1, total_rows), 1)
    column = lax.broadcasted_iota(jnp.int32, (total_rows, 1), 0)

    def pair_index(i):
        inside = lax.rem(i, pool)
        return (lax.rem(inside // rows + core, 2) * rows + lax.rem(inside, rows)).astype(f32)

    pair_row = row_of(pair_lens)
    spot_row, _ = strip_plan(
        pair_row, pair_lens, (row // pool).astype(f32), (column // pool).astype(f32), pair_index(row), pair_index(column),
        chips, seq,
    )
    wide = lax.broadcasted_iota(jnp.int32, (total_rows, total_rows), 0).astype(f32)

    def strip_counts(spots, lens_row):
        return row_sums(wide, [spots + (row // pool).astype(f32) * pool], [tail_blocks(lens_row)])

    pair_counts = strip_counts(spot_row, pair_row)
    cnt[...] = jnp.broadcast_to(pair_counts, cnt.shape)
    fill = jnp.sum(pair_counts.reshape(chips, HALVES, ROLES, 8, 1), axis=2)
    sent_chip = lax.broadcasted_iota(jnp.int32, fill.shape, 0) != chip
    local_fill = jnp.max(jnp.where(sent_chip, fill, 0.0))
    square = lax.broadcasted_iota(jnp.int32, (pool, pool), 0).astype(f32)
    for s in range(chips):
        deal[s] = jnp.where(square == spot_row[:, s * pool : (s + 1) * pool], 1.0, 0.0).astype(jnp.bfloat16)
    pltpu.make_async_copy(given, given, give_recv_sem.at[0]).wait()

    chip_x, chip_y = peer_of(chip, 1, chips), peer_of(chip, 2, chips)

    def relay(src, dst, there, send, recv, half):
        return pltpu.make_async_remote_copy(
            src_ref=src,
            dst_ref=dst,
            send_sem=send.at[half],
            recv_sem=recv.at[half],
            device_id=(gx, there * 2 + core),
            device_id_type=MESH,
        )

    def near_sends(there, t):
        return [
            relay(sendbuf.at[there, half], recvbuf.at[chip, half], there, strip_send_sem.at[t], strip_recv_sem.at[t], half)
            for half in range(HALVES)
        ]

    reach = 2 * nblocks

    def pack(there):
        span = (seq - width) // DEALS

        def deal_step(i, carry):
            cols = pl.ds(pl.multiple_of(width + i * span, LANES), span)
            both = jnp.concatenate([ordered[0, there, :, cols], got[there, :, cols]], axis=0)
            roles[:, pl.ds(pl.multiple_of(i * span, LANES), span)] = permuted(deal[there], both)
            return carry

        lax.fori_loop(0, DEALS, deal_step, 0)

        def half_step(half, carry):
            def count(role):
                at = there * pool + half * ROLES * 8 + role * 8
                return cnt[pl.ds(pl.multiple_of(at, 8), 8), :]

            def blocks(role):
                at = pl.ds(pl.multiple_of(half * ROLES * 8 + role * 8, 8), 8)
                return [roles[at, j * LANES : (j + 1) * LANES] for j in range(nblocks)]

            def side(outer, inner):
                n = count(outer)
                behind = shifted_up(blocks(inner), shift_bits(n), reach)
                near_end = blocks(outer)
                return [jnp.where(n > p, near_end[p], behind[p]) for p in range(nblocks)] + behind[nblocks:]

            left, right = side(0, 1), side(3, 2)
            left_n = count(0) + count(1)
            for p in range(STRIP_BLOCKS):
                q = STRIP_BLOCKS - 1 - p
                if q >= reach:
                    value = left[p]
                elif p >= reach:
                    value = right[q]
                else:
                    value = jnp.where(left_n > p, left[p], right[q])
                sendbuf[there, half, :, p * LANES : (p + 1) * LANES] = value
            return carry

        lax.fori_loop(0, HALVES, half_step, 0)

    far = peer_of(chip, chips - 1, chips)
    first_legs = [relay(sendbuf.at[far, half], passing.at[half], chip_x, first_leg_send_sem, first_leg_recv_sem, half) for half in range(HALVES)]

    def pack_step(t, carry):
        pack(peer_of(chip, chips - 1 - t, chips))

        @pl.when(t == 0)
        def _():
            for copy in first_legs:
                copy.start()

        @pl.when(t == 1)
        def _():
            for copy in near_sends(chip_y, 1):
                copy.start()

        return carry

    lax.fori_loop(0, chips - 1, pack_step, 0)

    info_recv[gy] = info_send[chip]
    for copy in info_copies[1:]:
        copy.wait()
    info_recv[mate] = info_got[chip]
    arrived = info_recv[...]
    counts[0] = jnp.sum(arrived, axis=0)

    def axis_sends(buf, send, recv):
        return [
            pltpu.make_async_remote_copy(
                src_ref=buf.at[0],
                dst_ref=buf.at[off],
                send_sem=send.at[off - 1],
                recv_sem=recv.at[off - 1],
                device_id=(lax.rem(gx + off, n_gx), gy),
                device_id_type=MESH,
            )
            for off in range(1, n_gx)
        ]

    count_copies = axis_sends(counts, count_send_sem, count_recv_sem)
    for copy in count_copies:
        copy.start()

    eye = lax.broadcasted_iota(jnp.int32, (slots, slots), 0) == lax.broadcasted_iota(jnp.int32, (slots, slots), 1)
    for m in range(members_dev):
        len_col[m] = jnp.broadcast_to(jnp.sum(jnp.where(eye, lens[m], 0.0), axis=1, keepdims=True), (slots, LANES))
    sum_policy[...] = jnp.zeros_like(sum_policy)
    sum_kl[...] = jnp.zeros_like(sum_kl)

    def sum_step(c, carry):
        positions = (lax.broadcasted_iota(jnp.int32, (slots, piece), 1) + c * piece).astype(f32)
        for m in range(members_dev):
            pol = policy[c, m]
            log_ratio = anchor[c, m] - pol
            ratio = jnp.exp(log_ratio)
            valid = positions < len_col[m][:, :1]
            sum_policy[m] += folded(jnp.where(valid, pol, 0.0))
            sum_kl[m] += folded(jnp.where(valid, kl_weight * (ratio - log_ratio - 1.0), 0.0))
        return carry

    lax.fori_loop(0, PIECES, sum_step, 0)
    sums = []
    for buf in (sum_policy, sum_kl):
        per_member = [row_of(jnp.sum(buf[m], axis=1, keepdims=True)) for m in range(members_dev)]
        sums.append(row_sums(place, targets, per_member))
    tails_send[...] = tiles(sums, jnp.broadcast_to(local_fill, (n_gy, 8, LANES)))
    tail_copies = tile_sends(tails_send, tails_recv, tail_send_sem, tail_recv_sem, range(1, n_gy))
    for copy in tail_copies:
        copy.start()
    tails_recv[gy] = tails_send[chip]

    for copy in near_sends(chip_x, 0):
        copy.start()


    for copy in count_copies:
        copy.wait()
    tokens = counts[0]
    for off in range(1, n_gx):
        tokens = tokens + counts[off]
    ntok = tokens[:1, info_lane : info_lane + 1]
    scale = samples * seq / ntok
    got_len = column_in(arrived, 0).reshape(total_rows, 1)
    got_row = row_of(got_len)
    reward = column_in(arrived, 1).reshape(members, part, 1)
    advantage = (members * reward - jnp.sum(reward, axis=0)[None]) / (members - 1)
    adv_rows[...] = jnp.broadcast_to(advantage, adv_rows.shape)
    len_rows[...] = jnp.broadcast_to(got_len.reshape(members, part, 1), len_rows.shape)
    got_spot_row, got_spot = strip_plan(
        got_row, got_len, (row // pool).astype(f32), (column // pool).astype(f32),
        lax.rem(row, pool).astype(f32), lax.rem(column, pool).astype(f32), chips, seq,
    )
    rcnt[...] = jnp.broadcast_to(strip_counts(got_spot_row, got_row), rcnt.shape)
    lane = lax.broadcasted_iota(jnp.int32, (total_rows, LANES), 1).astype(f32)
    for half in range(HALVES):
        pick = got_spot - half * ROLES * 8 == lane
        pick = jnp.where(pick & (lane < ROLES * 8), 1.0, 0.0).astype(jnp.bfloat16)
        undeal[:, half] = pick.reshape(chips, pool, LANES)
    half_rows[...] = jnp.broadcast_to(jnp.where(got_spot < ROLES * 8, 0.0, 1.0).reshape(members, part, 1), half_rows.shape)
    def finish_rows(k, start, value, only=None):
        span = value.shape[1]
        cols = pl.ds(pl.multiple_of(start, LANES), span)
        positions = (lax.broadcasted_iota(jnp.int32, (part, span), 1) + start).astype(f32)
        value = (value - adv_rows[k][:, :1]) * scale
        value = jnp.where(positions < len_rows[k][:, :1], value, 0.0)
        if only is not None:
            value = jnp.where(only, value, done[k, :, cols])
        done[k, :, cols] = value

    def own_step(which, source):
        def column_step(c, carry):
            start = pl.multiple_of(c * piece, LANES)
            for m in range(members_dev):
                finish_rows(source * members_dev + m, start, which(m * part, pl.ds(start, piece)))
            return carry

        lax.fori_loop(0, PIECES, column_step, 0)

    own_step(lambda r, cols: ordered[0, chip, r : r + part, cols], gy)
    give_own.wait_recv()
    own_step(lambda r, cols: got[chip, r : r + part, cols], mate)

    def first_wait(off):
        landed = heads_in.at[0]
        pltpu.make_async_copy(landed, landed, first_recv_sem.at[off - 2]).wait()

    def first_step(off, carry):
        first_wait(off)
        source = peer_of(gy, off, n_gy)
        for m in range(members_dev):
            finish_rows(source * members_dev + m, 0, heads_in[source, m * part : (m + 1) * part, :])
        return carry

    lax.fori_loop(2, n_gy, first_step, 0)

    def unpack(there, t, half):
        landed = recvbuf.at[0, 0]
        pltpu.make_async_copy(landed, landed, strip_recv_sem.at[t, half]).wait()

        def put(r, start, rows):
            k = there * 2 * members_dev + r
            finish_rows(k, width + start, rows, half_rows[k][:, :1] > 0.5 if half else None)

        unpack_strips(recvbuf, roles, undeal, rcnt, there, half, part, put)

    second_legs = [
        relay(passing.at[half], recvbuf.at[chip_x, half], chip_y, strip_send_sem.at[2], strip_recv_sem.at[2], half)
        for half in range(HALVES)
    ]
    for first_leg, second_leg in zip(first_legs, second_legs):
        first_leg.wait_recv()
        second_leg.start()
    for half in range(HALVES):
        unpack(chip_y, 1, half)

    for copy in tail_copies:
        copy.wait()
    ends = tails_recv[...]
    needs[0] = jnp.max(ends, axis=0)
    need_copies = axis_sends(needs, need_send_sem, need_recv_sem)
    for copy in need_copies:
        copy.start()
    first_sum = column_in(ends, 0).reshape(members, part, 1)
    second_sum = column_in(ends, 1).reshape(members, part, 1)
    value = (second_sum - advantage * first_sum) * (samples / ntok)[None]
    shape = (members, part, LANES)
    spread = lax.broadcasted_iota(jnp.int32, shape, 1) == lax.broadcasted_iota(jnp.int32, shape, 2)
    loss_ref[...] = jnp.sum(jnp.where(spread, value, 0.0), axis=1)[:, :part]
    adv_ref[...] = jnp.sum(jnp.where(spread, advantage, 0.0), axis=1)[:, :part]
    for copy in need_copies:
        copy.wait()
    fullest = needs[0]
    for off in range(1, n_gx):
        fullest = jnp.maximum(fullest, needs[off])
    over_ref[0, 0] = (jnp.max(fullest[:, fill_lane : fill_lane + 1]) > STRIP_BLOCKS).astype(jnp.int32)
    for off in FIRST_ORDER:
        landed = heads_in.at[0]
        pltpu.make_async_copy(landed, landed, first_send_sem.at[off - 2]).wait()
    pltpu.make_async_copy(given, given, give_send_sem.at[0]).wait()
    give_own.wait_send()

    scale_ref[...] = jnp.broadcast_to(scale, scale_ref.shape)

    def unpack_step(i, carry):
        unpack(peer_of(chip, 1 + 2 * i, chips), 2 * i, 0)
        return carry

    lax.fori_loop(0, 2, unpack_step, 0)
    for t in (0, 2):
        landed = recvbuf.at[0, 0]
        pltpu.make_async_copy(landed, landed, strip_recv_sem.at[t, 1]).wait()
    for half in range(HALVES):
        first_legs[half].wait_send()
        for t in range(chips - 1):
            sent = sendbuf.at[0, 0]
            pltpu.make_async_copy(sent, sent, strip_send_sem.at[t, half]).wait()


def store(
    n_gy, done, loss, adv, recvbuf, undeal, rcnt, len_rows, adv_rows, half_rows, scale_ref,
    grad, loss_out, adv_out, last, roles, sem,
):
    chips = n_gy // 2
    members, part, seq = done.shape
    group = members // chips
    width = seq - roles.shape[1]
    chip = lax.axis_index("gy") // 2
    scale = scale_ref[:1, :1]

    def chip_rows(there):
        return pl.ds(there * group, group)

    whole = [chip_rows(chip), chip_rows(peer_of(chip, 2, chips))]
    late = [peer_of(chip, 1, chips), peer_of(chip, 3, chips)]
    first = pl.ds(0, width)
    copies = [pltpu.make_async_copy(done.at[rows], grad.at[rows], sem.at[k]) for k, rows in enumerate(whole)]
    copies += [
        pltpu.make_async_copy(done.at[chip_rows(there), :, first], grad.at[chip_rows(there), :, first], sem.at[2 + k])
        for k, there in enumerate(late)
    ]
    copies += [pltpu.make_async_copy(loss, loss_out, sem.at[4]), pltpu.make_async_copy(adv, adv_out, sem.at[5])]
    for copy in copies:
        copy.start()

    def store_late(i):
        rows = chip_rows(peer_of(chip, 1 + 2 * i, chips))
        return pltpu.make_async_copy(last.at[i], grad.at[rows, :, pl.ds(width, seq - width)], sem.at[6 + i])

    def late_step(i, carry):
        there = peer_of(chip, 1 + 2 * i, chips)

        def put(r, start, rows):
            k, span = there * group + r, rows.shape[1]
            positions = (lax.broadcasted_iota(jnp.int32, (part, span), 1) + (width + start)).astype(jnp.float32)
            value = (rows - adv_rows[k][:, :1]) * scale
            before = done[k, :, pl.ds(pl.multiple_of(width + start, LANES), span)]
            value = jnp.where(half_rows[k][:, :1] > 0.5, jnp.where(positions < len_rows[k][:, :1], value, 0.0), before)
            last[i, r, :, pl.ds(start, span)] = value

        unpack_strips(recvbuf, roles, undeal, rcnt, there, 1, part, put)
        store_late(i).start()
        return carry

    lax.fori_loop(0, 2, late_step, 0)
    copies += [store_late(i) for i in range(2)]
    for copy in copies:
        copy.wait()


def packed_body(n_gx, n_gy, policy_logp, anchor_logp, lengths, rewards, slot_prompt):
    members_dev, slots, seq = policy_logp.shape
    members, part = members_dev * n_gy, slots // n_gy
    f32, bf16 = jnp.float32, jnp.bfloat16
    chips, rows = n_gy // 2, members_dev * part
    pool = 2 * rows
    width = HEAD_BLOCKS * LANES
    chunked = (PIECES, members_dev, slots, seq // PIECES)
    strips = (chips, HALVES, 8, STRIP_BLOCKS * LANES)
    per_slot = (members_dev, slots, LANES)
    per_sample = (members, part, LANES)
    tile = (n_gy, 8, LANES)
    hbm_spec = pl.BlockSpec(memory_space=pltpu.HBM)
    vmem_spec = pl.BlockSpec(memory_space=pltpu.VMEM)
    dma = pltpu.SemaphoreType.DMA
    handed = (
        pltpu.VMEM(strips, f32),
        pltpu.VMEM((chips, HALVES, pool, LANES), bf16),
        pltpu.VMEM((chips * pool, LANES), f32),
        pltpu.VMEM(per_sample, f32),
        pltpu.VMEM(per_sample, f32),
        pltpu.VMEM(per_sample, f32),
        pltpu.VMEM((8, LANES), f32),
    )
    done, loss, adv, over, *rest = pl.pallas_call(
        functools.partial(packed_exchange, n_gx, n_gy),
        out_shape=(
            pltpu.VMEM((members, part, seq), f32),
            pltpu.VMEM((members, part), f32),
            pltpu.VMEM((members, part), f32),
            pltpu.SMEM((1, 1), jnp.int32),
        ) + handed,
        in_specs=[hbm_spec] * 5,
        out_specs=(vmem_spec,) * 3 + (pl.BlockSpec(memory_space=pltpu.SMEM),) + (vmem_spec,) * len(handed),
        scratch_shapes=[
            pltpu.VMEM(chunked, f32),
            pltpu.VMEM(chunked, f32),
            pltpu.VMEM((members_dev, slots), jnp.int32),
            pltpu.VMEM((members_dev, slots), jnp.int32),
            pltpu.VMEM((members_dev, slots), jnp.int32),
            pltpu.VMEM((2 * chips * rows, members_dev * slots), bf16),
            pltpu.VMEM((2, chips, rows, seq), f32),
            pltpu.VMEM((chips, rows, seq), f32),
            pltpu.VMEM((n_gy, rows, width), f32),
            pltpu.VMEM(strips, f32),
            pltpu.VMEM(strips[1:], f32),
            pltpu.VMEM((pool, seq - width), f32),
            pltpu.VMEM((chips, pool, pool), bf16),
            pltpu.VMEM((chips * pool, LANES), f32),
            pltpu.VMEM(per_slot, f32),
            pltpu.VMEM(per_slot, f32),
            pltpu.VMEM(per_slot, f32),
            pltpu.VMEM(tile, f32),
            pltpu.VMEM((chips, 8, LANES), f32),
            pltpu.VMEM(tile, f32),
            pltpu.VMEM(tile, f32),
            pltpu.VMEM(tile, f32),
            pltpu.VMEM((n_gx, 8, LANES), f32),
            pltpu.VMEM((n_gx, 8, LANES), f32),
            dma((3,)),
            dma((2, PIECES)),
            dma((2,)),
            dma((2,)),
            dma((n_gy - 2,)),
            dma((n_gy - 2,)),
            dma((chips - 1, HALVES)),
            dma((chips - 1, HALVES)),
            dma((HALVES,)),
            dma((HALVES,)),
            dma((n_gy - 1,)),
            dma((n_gy - 1,)),
            dma((n_gy - 1,)),
            dma((n_gy - 1,)),
            dma((n_gx - 1,)),
            dma((n_gx - 1,)),
            dma((n_gx - 1,)),
            dma((n_gx - 1,)),
        ],
        compiler_params=pltpu.CompilerParams(collective_id=0, has_side_effects=True, vmem_limit_bytes=36 * 2**20),
    )(policy_logp, anchor_logp, lengths, rewards, slot_prompt)

    def fits(policy_logp, anchor_logp, lengths, rewards, slot_prompt, done, loss, adv, *rest):
        small = jax.ShapeDtypeStruct((members, part), f32)
        return tuple(pl.pallas_call(
            functools.partial(store, n_gy),
            out_shape=(jax.ShapeDtypeStruct((members, part, seq), f32), small, small),
            in_specs=[vmem_spec] * (3 + len(rest)),
            out_specs=(hbm_spec,) * 3,
            scratch_shapes=[
                pltpu.VMEM((2, 2 * members_dev, part, seq - width), f32),
                pltpu.VMEM((ROLES * 8, seq - width), f32),
                dma((8,)),
            ],
            compiler_params=pltpu.CompilerParams(vmem_limit_bytes=16 * 2**20),
        )(done, loss, adv, *rest))

    def overflows(policy_logp, anchor_logp, lengths, rewards, slot_prompt, done, loss, adv, *rest):
        return tuple(unpacked_body(n_gx, n_gy, policy_logp, anchor_logp, lengths, rewards, slot_prompt))

    return lax.cond(
        over[0, 0] > 0, overflows, fits,
        policy_logp, anchor_logp, lengths, rewards, slot_prompt, done, loss, adv, *rest,
    )


def body(n_gx, n_gy, *args):
    members_dev, slots, seq = args[0].shape
    pool = 2 * members_dev * slots // n_gy
    packs = n_gy == 8 and pool == ROLES * STRIPS and slots == LANES and seq == LANES * 32 and seq % (PIECES * LANES) == 0
    return (packed_body if packs else unpacked_body)(n_gx, n_gy, *args)


def solution(mesh):
    placed = (P("gy", "gx", None), P("gy", "gx", None), P("gy", "gx"), P("gy", "gx"), P("gy", "gx"))
    return jax.shard_map(
        functools.partial(body, mesh.shape["gx"], mesh.shape["gy"]),
        mesh=mesh,
        in_specs=placed,
        out_specs=(P(None, ("gx", "gy"), None), P(None, ("gx", "gy")), P(None, ("gx", "gy"))),
        check_vma=False,
    )
```

```python
import functools

import jax
import jax.numpy as jnp
from jax import lax
from jax.experimental import pallas as pl
from jax.experimental.pallas import tpu as pltpu
from jax.sharding import PartitionSpec as P

kl_weight = 0.1
LANES = 128
CHUNKS = 8
MESH = pl.DeviceIdType.MESH
ROLES = 4
STRIPS = 16
HALVES = STRIPS // 8
SHIFTS = 5
PIECES = 8
DEALS = 1
UNDEALS = 1
HEAD_BLOCKS = 6
STRIP_BLOCKS = 66
FIRST_ORDER = (2, 4, 3, 5, 6, 7)


def partner(index, off, count):
    out, bit = index, 1
    while bit < count:
        if off & bit:
            out = out + bit - 2 * bit * lax.rem(index // bit, 2)
        bit *= 2
    return out


def offsets_by_distance(count):
    far = max(bin(off // 2).count("1") for off in range(1, count))
    near = [off for off in range(1, count) if bin(off // 2).count("1") < far]
    return near, [off for off in range(1, count) if off not in near]


def permuted(onehot, rows):
    high = rows.astype(jnp.bfloat16)
    rest = rows - high.astype(jnp.float32)
    middle = rest.astype(jnp.bfloat16)
    low = (rest - middle.astype(jnp.float32)).astype(jnp.bfloat16)
    dot = functools.partial(jnp.dot, preferred_element_type=jnp.float32)
    return dot(onehot, high) + dot(onehot, middle) + dot(onehot, low)


def folded(x):
    out = x[:, :LANES]
    for start in range(LANES, x.shape[1], LANES):
        out = out + x[:, start : start + LANES]
    return out


def exchange(
    n_gx, n_gy, policy_hbm, anchor_hbm, len_ref, reward_ref, prompt_ref,
    raw_hbm, heads_ref, tails_ref, ntok_ref,
    policy, anchor, sendbuf, onehot, len_col, sum_policy, sum_kl,
    heads_send, heads_recv, tails_send, tails_recv, counts,
    load_sem, send_sem, recv_sem, own_sem,
    head_send_sem, head_recv_sem, tail_send_sem, tail_recv_sem, count_send_sem, count_recv_sem,
):
    gx, gy = lax.axis_index("gx"), lax.axis_index("gy")
    members_dev, slots, seq = policy_hbm.shape
    part = slots // n_gy
    width = seq // CHUNKS

    near, far = offsets_by_distance(n_gy)
    barrier = pltpu.get_barrier_semaphore()
    for off in range(1, n_gy):
        pl.semaphore_signal(barrier, inc=1, device_id=(gx, partner(gy, off, n_gy)), device_id_type=MESH)
    for off in range(1, n_gx):
        pl.semaphore_signal(barrier, inc=1, device_id=(lax.rem(gx + off, n_gx), gy), device_id_type=MESH)

    def loads(c):
        cols = pl.ds(pl.multiple_of(c * width, LANES), width)
        return (
            pltpu.make_async_copy(policy_hbm.at[:, :, cols], policy.at[c], load_sem.at[0, c]),
            pltpu.make_async_copy(anchor_hbm.at[:, :, cols], anchor.at[c], load_sem.at[1, c]),
        )

    for c in range(CHUNKS):
        for copy in loads(c):
            copy.start()

    sublane = lax.broadcasted_iota(jnp.int32, (slots, slots), 0)
    lane = lax.broadcasted_iota(jnp.int32, (slots, slots), 1)
    column = lax.broadcasted_iota(jnp.int32, (slots, LANES), 1)
    local_tokens = jnp.sum(len_ref[...].astype(jnp.float32))
    for m in range(members_dev):
        seq_len = len_ref[m : m + 1, :].astype(jnp.float32)
        reward = reward_ref[m : m + 1, :].astype(jnp.float32) * 0.25
        match = sublane == lax.rem(prompt_ref[m : m + 1, :], slots)
        onehot[m] = jnp.where(match, 1.0, 0.0).astype(jnp.bfloat16)
        len_col[m] = jnp.broadcast_to(
            jnp.sum(jnp.where(sublane == lane, seq_len, 0.0), axis=1, keepdims=True), (slots, LANES)
        )
        sorted_len = jnp.sum(jnp.where(match, seq_len, 0.0), axis=1, keepdims=True)
        sorted_reward = jnp.sum(jnp.where(match, reward, 0.0), axis=1, keepdims=True)
        heads_send[m] = jnp.where(
            column == 0, sorted_len, jnp.where(column == 1, sorted_reward, local_tokens)
        )
    sum_policy[...] = jnp.zeros_like(sum_policy)
    sum_kl[...] = jnp.zeros_like(sum_kl)

    def compute(c):
        for copy in loads(c):
            copy.wait()
        positions = (lax.broadcasted_iota(jnp.int32, (slots, width), 1) + c * width).astype(jnp.float32)
        for m in range(members_dev):
            pol = policy[c, m]
            log_ratio = anchor[c, m] - pol
            ratio = jnp.exp(log_ratio)
            valid = positions < len_col[m][:, :1]
            sum_policy[m] += folded(jnp.where(valid, pol, 0.0))
            sum_kl[m] += folded(jnp.where(valid, kl_weight * (ratio - log_ratio - 1.0), 0.0))
            sendbuf[c, m] = permuted(onehot[m], kl_weight * (1.0 - ratio))

    def rows_of(device):
        return pl.ds(pl.multiple_of(device * part, part), part)

    my_members = pl.ds(gy * members_dev, members_dev)

    def sends(c, offs):
        cols = pl.ds(pl.multiple_of(c * width, LANES), width)
        copies = []
        for off in offs:
            peer = partner(gy, off, n_gy)
            copies.append(
                pltpu.make_async_remote_copy(
                    src_ref=sendbuf.at[c, :, rows_of(peer), :],
                    dst_ref=raw_hbm.at[my_members, :, cols],
                    send_sem=send_sem.at[off - 1],
                    recv_sem=recv_sem.at[off - 1],
                    device_id=(gx, peer),
                    device_id_type=MESH,
                )
            )
        return copies

    def own(c):
        cols = pl.ds(pl.multiple_of(c * width, LANES), width)
        return pltpu.make_async_copy(
            sendbuf.at[c, :, rows_of(gy), :], raw_hbm.at[my_members, :, cols], own_sem.at[c]
        )

    def small_sends(src, dst, send, recv):
        copies = []
        for off in range(1, n_gy):
            peer = partner(gy, off, n_gy)
            copies.append(
                pltpu.make_async_remote_copy(
                    src_ref=src.at[:, rows_of(peer), :],
                    dst_ref=dst.at[my_members],
                    send_sem=send.at[off - 1],
                    recv_sem=recv.at[off - 1],
                    device_id=(gx, peer),
                    device_id_type=MESH,
                )
            )
        copies.append(pltpu.make_async_copy(src.at[:, rows_of(gy), :], dst.at[my_members], send.at[n_gy - 1]))
        return copies

    def count_sends():
        return [
            pltpu.make_async_remote_copy(
                src_ref=counts.at[0],
                dst_ref=counts.at[off],
                send_sem=count_send_sem.at[off - 1],
                recv_sem=count_recv_sem.at[off - 1],
                device_id=(lax.rem(gx + off, n_gx), gy),
                device_id_type=MESH,
            )
            for off in range(1, n_gx)
        ]

    compute(0)
    pl.semaphore_wait(barrier, n_gy - 1 + n_gx - 1)
    head_copies = small_sends(heads_send, heads_recv, head_send_sem, head_recv_sem)
    for copy in head_copies:
        copy.start()

    def step(c, carry):
        for copy in sends(c - 1, near):
            copy.start()
        own(c - 1).start()
        compute(c)
        return carry

    lax.fori_loop(1, CHUNKS, step, 0)
    for copy in sends(CHUNKS - 1, near):
        copy.start()

    def far_step(c, carry):
        for copy in sends(c, far):
            copy.start()
        return carry

    lax.fori_loop(0, CHUNKS, far_step, 0)
    own(CHUNKS - 1).start()

    for m in range(members_dev):
        s1 = jnp.sum(permuted(onehot[m], sum_policy[m]), axis=1, keepdims=True)
        s2 = jnp.sum(permuted(onehot[m], sum_kl[m]), axis=1, keepdims=True)
        tails_send[m] = jnp.where(column == 0, s1, s2)
    for copy in head_copies:
        copy.wait()
    tokens = jnp.zeros((8, LANES), jnp.float32)
    for source in range(n_gy):
        tokens = tokens + heads_recv[source * members_dev, :8, :]
    counts[0] = tokens
    heads_ref[...] = heads_recv[...]
    tail_copies = small_sends(tails_send, tails_recv, tail_send_sem, tail_recv_sem)
    for copy in tail_copies:
        copy.start()
    count_copies = count_sends()
    for copy in count_copies:
        copy.start()
    for copy in count_copies:
        copy.wait()
    ntok_ref[...] = jnp.sum(counts[...], axis=0)
    for copy in tail_copies:
        copy.wait()
    tails_ref[...] = tails_recv[...]
    for c in range(CHUNKS):
        own(c).wait()
    for off in range(1, n_gy):
        source = partner(gy, off, n_gy)
        landed = raw_hbm.at[pl.ds(source * members_dev, members_dev)]
        pltpu.make_async_copy(landed, landed, recv_sem.at[off - 1]).wait()
        pltpu.make_async_copy(landed, landed, send_sem.at[off - 1]).wait()


def finish(samples, raw, heads, tails, ntok, grad, loss, adv, done, done_sem):
    members, part, seq = raw.shape
    tokens = ntok[:1, 2:3]
    total = jnp.sum(heads[...], axis=0)
    advantage = (members * heads[:, :, 1:2] - total[None, :, 1:2]) / (members - 1)
    positions = lax.broadcasted_iota(jnp.int32, (part, seq), 1).astype(jnp.float32)
    scale = samples * seq / tokens

    def store(k):
        return pltpu.make_async_copy(done.at[k], grad.at[k], done_sem.at[k])

    for k in range(members):
        done[k] = jnp.where(positions < heads[k, :, :1], raw[k] - advantage[k], 0.0) * scale
        if k > 0:
            store(k - 1).start()
    shape = (members, part, LANES)
    eye = lax.broadcasted_iota(jnp.int32, shape, 1) == lax.broadcasted_iota(jnp.int32, shape, 2)
    store(members - 1).start()
    value = (tails[:, :, 1:2] - advantage * tails[:, :, :1]) * (samples / tokens)[None]
    loss[...] = jnp.sum(jnp.where(eye, value, 0.0), axis=1)[:, :part]
    adv[...] = jnp.sum(jnp.where(eye, advantage, 0.0), axis=1)[:, :part]
    for k in range(members):
        store(k).wait()


def unpacked_body(n_gx, n_gy, policy_logp, anchor_logp, lengths, rewards, slot_prompt):
    members_dev, slots, seq = policy_logp.shape
    members, part = members_dev * n_gy, slots // n_gy
    f32 = jnp.float32
    chunked = (CHUNKS, members_dev, slots, seq // CHUNKS)
    small = (members, part, LANES)
    hbm_spec = pl.BlockSpec(memory_space=pltpu.HBM)
    vmem_spec = pl.BlockSpec(memory_space=pltpu.VMEM)
    dma = pltpu.SemaphoreType.DMA
    raw, heads, tails, ntok = pl.pallas_call(
        functools.partial(exchange, n_gx, n_gy),
        out_shape=(
            pltpu.VMEM((members, part, seq), f32),
            pltpu.VMEM(small, f32),
            pltpu.VMEM(small, f32),
            pltpu.VMEM((8, LANES), f32),
        ),
        in_specs=[hbm_spec, hbm_spec, vmem_spec, vmem_spec, vmem_spec],
        out_specs=(vmem_spec, vmem_spec, vmem_spec, vmem_spec),
        scratch_shapes=[
            pltpu.VMEM(chunked, f32),
            pltpu.VMEM(chunked, f32),
            pltpu.VMEM(chunked, f32),
            pltpu.VMEM((members_dev, slots, slots), jnp.bfloat16),
            pltpu.VMEM((members_dev, slots, LANES), f32),
            pltpu.VMEM((members_dev, slots, LANES), f32),
            pltpu.VMEM((members_dev, slots, LANES), f32),
            pltpu.VMEM((members_dev, slots, LANES), f32),
            pltpu.VMEM(small, f32),
            pltpu.VMEM((members_dev, slots, LANES), f32),
            pltpu.VMEM(small, f32),
            pltpu.VMEM((n_gx, 8, LANES), f32),
            dma((2, CHUNKS)),
            dma((n_gy - 1,)),
            dma((n_gy - 1,)),
            dma((CHUNKS,)),
            dma((n_gy,)),
            dma((n_gy - 1,)),
            dma((n_gy,)),
            dma((n_gy - 1,)),
            dma((n_gx - 1,)),
            dma((n_gx - 1,)),
        ],
        compiler_params=pltpu.CompilerParams(collective_id=1, has_side_effects=True, vmem_limit_bytes=36 * 2**20),
    )(policy_logp, anchor_logp, lengths, rewards, slot_prompt)
    samples = members * slots * n_gx
    return pl.pallas_call(
        functools.partial(finish, samples),
        out_shape=(
            jax.ShapeDtypeStruct((members, part, seq), f32),
            jax.ShapeDtypeStruct((members, part), f32),
            jax.ShapeDtypeStruct((members, part), f32),
        ),
        in_specs=[vmem_spec] * 4,
        out_specs=(hbm_spec, vmem_spec, vmem_spec),
        scratch_shapes=[pltpu.VMEM((members, part, seq), f32), dma((members,))],
        compiler_params=pltpu.CompilerParams(vmem_limit_bytes=32 * 2**20),
    )(raw, heads, tails, ntok)


def row_of(column):
    n = column.shape[0]
    eye = lax.broadcasted_iota(jnp.int32, (n, n), 0) == lax.broadcasted_iota(jnp.int32, (n, n), 1)
    return jnp.sum(jnp.where(eye, column, 0.0), axis=0, keepdims=True)


def row_sums(place, targets, values):
    out = None
    for target, value in zip(targets, values):
        here = jnp.sum(jnp.where(place == target, value, 0.0), axis=1, keepdims=True)
        out = here if out is None else out + here
    return out


def strip_spot(rank):
    first, second, third = rank < STRIPS, rank < 2 * STRIPS, rank < 3 * STRIPS
    strip = jnp.where(
        first, rank, jnp.where(second, 2 * STRIPS - 1 - rank, jnp.where(third, 3 * STRIPS - 1 - rank, rank - 3 * STRIPS))
    )
    role = jnp.where(first, 0.0, jnp.where(second, 3.0, jnp.where(third, 2.0, 1.0)))
    half = jnp.floor(strip * (1.0 / 8))
    return half * (ROLES * 8) + role * 8 + strip - half * 8


def strip_plan(len_row, len_column, group_row, group_column, index_row, index_column, n_groups, seq):
    rows = ROLES * STRIPS
    key_row = group_row * ((seq + 1) * rows) + len_row * rows + index_row
    key_column = group_column * ((seq + 1) * rows) + len_column * rows + index_column
    above_row = jnp.sum(jnp.where(key_column > key_row, 1.0, 0.0), axis=0, keepdims=True)
    above_column = jnp.sum(jnp.where(key_row > key_column, 1.0, 0.0), axis=1, keepdims=True)
    return (
        strip_spot(above_row - rows * (n_groups - 1 - group_row)),
        strip_spot(above_column - rows * (n_groups - 1 - group_column)),
    )


def tail_blocks(lens):
    return jnp.maximum(jnp.floor((lens + (LANES - 1)) * (1.0 / LANES)) - HEAD_BLOCKS, 0.0)


def shift_bits(count):
    shift = count.astype(jnp.int32)
    return [(lax.shift_right_logical(shift, k) & 1) == 1 for k in range(SHIFTS)]


def shifted_up(blocks, bits, reach):
    for k in range(SHIFTS):
        step, n = 2**k, len(blocks)
        moved = []
        for p in range(min(n + step, reach)):
            if p < step:
                moved.append(blocks[p])
            elif p >= n:
                moved.append(blocks[p - step])
            else:
                moved.append(jnp.where(bits[k], blocks[p - step], blocks[p]))
        blocks = moved
    return blocks


def shifted_down(blocks, bits, count):
    for k in reversed(range(SHIFTS)):
        step = 2**k
        keep = min(len(blocks), count + step - 1)
        blocks = [
            jnp.where(bits[k], blocks[p + step], blocks[p]) if p + step < len(blocks) else blocks[p] for p in range(keep)
        ]
    return blocks


def peer_of(index, off, count):
    out, bit = 0, 1
    while bit < count:
        a, b = lax.rem(index // bit, 2), lax.rem(off // bit, 2)
        out = out + bit * (a + b - 2 * a * b)
        bit *= 2
    return out


def unpack_strips(recvbuf, roles, undeal, rcnt, there, half, part, put):
    pool, seq_tail = undeal.shape[2], roles.shape[1]
    nblocks = seq_tail // LANES

    def count(role):
        at = there * pool + half * ROLES * 8 + role * 8
        return rcnt[pl.ds(pl.multiple_of(at, 8), 8), :]

    def block(p):
        return recvbuf[there, half, :, p * LANES : (p + 1) * LANES]

    for outer, inner, at in ((0, 1, lambda p: p), (3, 2, lambda p: STRIP_BLOCKS - 1 - p)):
        for j in range(nblocks):
            roles[outer * 8 : outer * 8 + 8, j * LANES : (j + 1) * LANES] = block(at(j))
        behind = [block(at(p)) for p in range(2 * nblocks)]
        behind = shifted_down(behind, shift_bits(count(outer)), nblocks)
        for j in range(nblocks):
            roles[inner * 8 : inner * 8 + 8, j * LANES : (j + 1) * LANES] = behind[j]
    order = undeal[there, half][:, : ROLES * 8]
    span = seq_tail // UNDEALS

    def undeal_step(i, carry):
        start = pl.multiple_of(i * span, LANES)
        out = permuted(order, roles[: ROLES * 8, pl.ds(start, span)])
        for r in range(pool // part):
            put(r, start, out[r * part : (r + 1) * part])
        return carry

    lax.fori_loop(0, UNDEALS, undeal_step, 0)


def packed_exchange(
    n_gx, n_gy, policy_hbm, anchor_hbm, len_hbm, reward_hbm, prompt_hbm,
    done, loss_ref, adv_ref, over_ref, recvbuf, undeal, rcnt, len_rows, adv_rows, half_rows, scale_ref,
    policy, anchor, len_ref, reward_ref, prompt_ref, onehot, ordered, got, heads_in, sendbuf, passing, roles,
    deal, cnt, len_col, sum_policy, sum_kl,
    info_send, info_got, info_recv, tails_send, tails_recv, counts,
    small_sem, load_sem, give_send_sem, give_recv_sem, first_send_sem, first_recv_sem, strip_send_sem, strip_recv_sem, first_leg_send_sem, first_leg_recv_sem,
    info_send_sem, info_recv_sem, tail_send_sem, tail_recv_sem, count_send_sem, count_recv_sem,
):
    gx, gy = lax.axis_index("gx"), lax.axis_index("gy")
    core, chip = lax.rem(gy, 2), gy // 2
    mate = chip * 2 + 1 - core
    members_dev, slots, seq = policy_hbm.shape
    members, part = members_dev * n_gy, slots // n_gy
    chips = n_gy // 2
    width = HEAD_BLOCKS * LANES
    piece = seq // PIECES
    nblocks = seq // LANES - HEAD_BLOCKS
    rows = members_dev * part
    pool = 2 * rows
    total_rows = chips * pool
    samples = members * slots * n_gx
    info_lane, fill_lane = 16, 17
    rounds = n_gx.bit_length() - 1
    f32 = jnp.float32

    small_loads = [
        pltpu.make_async_copy(src, dst, small_sem.at[k])
        for k, (src, dst) in enumerate(((len_hbm, len_ref), (prompt_hbm, prompt_ref), (reward_hbm, reward_ref)))
    ]
    for copy in small_loads:
        copy.start()

    def loads(c):
        cols = pl.ds(pl.multiple_of(c * piece, LANES), piece)
        return (
            pltpu.make_async_copy(policy_hbm.at[:, :, cols], policy.at[c], load_sem.at[0, c]),
            pltpu.make_async_copy(anchor_hbm.at[:, :, cols], anchor.at[c], load_sem.at[1, c]),
        )

    for copy in loads(0):
        copy.start()
    barrier = pltpu.get_barrier_semaphore()
    for off in range(1, n_gy):
        pl.semaphore_signal(barrier, inc=1, device_id=(gx, partner(gy, off, n_gy)), device_id_type=MESH)
    for k in range(rounds):
        pl.semaphore_signal(barrier, inc=1, device_id=(partner(gx, 2**k, n_gx), gy), device_id_type=MESH)
    for c in range(1, PIECES):
        for copy in loads(c):
            copy.start()
    for copy in small_loads:
        copy.wait()

    lens = [len_ref[m : m + 1, :].astype(f32) for m in range(members_dev)]
    targets = []
    for m in range(members_dev):
        spot = lax.rem(prompt_ref[m : m + 1, :], slots)
        device = spot // part
        other = lax.rem(device + core, 2)
        target = (other * chips + device // 2) * rows + m * part + spot - device * part
        targets.append(target.astype(f32))
    place = lax.broadcasted_iota(jnp.int32, (total_rows, slots), 0).astype(f32)
    for m in range(members_dev):
        onehot[:, m * slots : (m + 1) * slots] = jnp.where(place == targets[m], 1.0, 0.0).astype(jnp.bfloat16)

    def put_in_order(c):
        for copy in loads(c):
            copy.wait()
        values = kl_weight * (1.0 - jnp.exp(anchor[c] - policy[c]))
        out = permuted(onehot[...], values.reshape(members_dev * slots, piece))
        cols = pl.ds(pl.multiple_of(c * piece, LANES), piece)
        ordered[:, :, :, cols] = out.reshape(2, chips, rows, piece)

    def give(c, there):
        cols = pl.ds(pl.multiple_of(c * piece, LANES), piece)
        return pltpu.make_async_remote_copy(
            src_ref=ordered.at[1, there, :, cols],
            dst_ref=got.at[there, :, cols],
            send_sem=give_send_sem.at[0],
            recv_sem=give_recv_sem.at[0],
            device_id=(gx, mate),
            device_id_type=MESH,
        )

    give_own = pltpu.make_async_remote_copy(
        src_ref=ordered.at[1, chip],
        dst_ref=got.at[chip],
        send_sem=give_send_sem.at[1],
        recv_sem=give_recv_sem.at[1],
        device_id=(gx, mate),
        device_id_type=MESH,
    )
    given = got.at[pl.ds(0, chips - 1), :, pl.ds(piece, seq - piece)]

    def first_send(off, lo, hi):
        peer = partner(gy, off, n_gy)
        cols = pl.ds(lo, hi - lo)
        return pltpu.make_async_remote_copy(
            src_ref=ordered.at[off % 2, peer // 2, :, cols],
            dst_ref=heads_in.at[gy, :, cols],
            send_sem=first_send_sem.at[off - 2],
            recv_sem=first_recv_sem.at[off - 2],
            device_id=(gx, peer),
            device_id_type=MESH,
        )

    tile_lane = lax.broadcasted_iota(jnp.int32, (n_gy, 8, LANES), 2)
    groups = rows // 8
    local_tokens = sum(jnp.sum(length) for length in lens)

    def tiles(columns, base):
        out = base
        for f, column in enumerate(columns):
            split = column.reshape(n_gy, groups, 8, 1)
            for g in range(groups):
                out = jnp.where(tile_lane == g * 4 + f, split[:, g], out)
        return out

    def column_in(tile, f):
        parts = [tile[:, :, g * 4 + f : g * 4 + f + 1][:, None] for g in range(groups)]
        return jnp.concatenate(parts, axis=1)

    def tile_sends(src, dst, send, recv, offs):
        copies = []
        for off in offs:
            peer = partner(gy, off, n_gy)
            copies.append(
                pltpu.make_async_remote_copy(
                    src_ref=src.at[off % 2 * chips + peer // 2],
                    dst_ref=dst.at[gy],
                    send_sem=send.at[off - 1],
                    recv_sem=recv.at[off - 1],
                    device_id=(gx, peer),
                    device_id_type=MESH,
                )
            )
        return copies

    mate_info = pltpu.make_async_remote_copy(
        src_ref=info_send.at[pl.ds(chips, chips)],
        dst_ref=info_got,
        send_sem=info_send_sem.at[0],
        recv_sem=info_recv_sem.at[0],
        device_id=(gx, mate),
        device_id_type=MESH,
    )
    info_copies = [mate_info] + tile_sends(info_send, info_recv, info_send_sem, info_recv_sem, range(2, n_gy))

    def order_step(c, carry):
        put_in_order(c)

        @pl.when(c == 0)
        def _():
            pl.semaphore_wait(barrier, n_gy - 1 + rounds)
            for off in FIRST_ORDER:
                first_send(off, 0, piece).start()
            lens_out = row_sums(place, targets, lens)
            rewards = [reward_ref[m : m + 1, :].astype(f32) * 0.25 for m in range(members_dev)]
            rewards_out = row_sums(place, targets, rewards)
            info_send[...] = tiles((lens_out, rewards_out), jnp.broadcast_to(local_tokens, (n_gy, 8, LANES)))
            for copy in info_copies:
                copy.start()

        @pl.when(c == 1)
        def _():
            for off in FIRST_ORDER:
                first_send(off, piece, width).start()

        @pl.when(c >= 1)
        def _():
            for t in range(1, chips):
                give(c, peer_of(chip, t, chips)).start()

        return carry

    lax.fori_loop(0, PIECES, order_step, 0)
    give_own.start()
    own_len = column_in(info_send[:chips], 0).reshape(chips * rows, 1)

    mate_info.wait()
    pair_lens = jnp.concatenate(
        [own_len[: chips * rows].reshape(chips, 1, rows, 1), column_in(info_got[...], 0).reshape(chips, 1, rows, 1)], axis=1
    ).reshape(total_rows, 1)
    row = lax.broadcasted_iota(jnp.int32, (1, total_rows), 1)
    column = lax.broadcasted_iota(jnp.int32, (total_rows, 1), 0)

    def pair_index(i):
        inside = lax.rem(i, pool)
        return (lax.rem(inside // rows + core, 2) * rows + lax.rem(inside, rows)).astype(f32)

    pair_row = row_of(pair_lens)
    spot_row, _ = strip_plan(
        pair_row, pair_lens, (row // pool).astype(f32), (column // pool).astype(f32), pair_index(row), pair_index(column),
        chips, seq,
    )
    wide = lax.broadcasted_iota(jnp.int32, (total_rows, total_rows), 0).astype(f32)

    def strip_counts(spots, lens_row):
        return row_sums(wide, [spots + (row // pool).astype(f32) * pool], [tail_blocks(lens_row)])

    pair_counts = strip_counts(spot_row, pair_row)
    cnt[...] = jnp.broadcast_to(pair_counts, cnt.shape)
    fill = jnp.sum(pair_counts.reshape(chips, HALVES, ROLES, 8, 1), axis=2)
    sent_chip = lax.broadcasted_iota(jnp.int32, fill.shape, 0) != chip
    local_fill = jnp.max(jnp.where(sent_chip, fill, 0.0))
    square = lax.broadcasted_iota(jnp.int32, (pool, pool), 0).astype(f32)
    for s in range(chips):
        deal[s] = jnp.where(square == spot_row[:, s * pool : (s + 1) * pool], 1.0, 0.0).astype(jnp.bfloat16)
    pltpu.make_async_copy(given, given, give_recv_sem.at[0]).wait()

    chip_x, chip_y = peer_of(chip, 1, chips), peer_of(chip, 2, chips)

    def relay(src, dst, there, send, recv, half):
        return pltpu.make_async_remote_copy(
            src_ref=src,
            dst_ref=dst,
            send_sem=send.at[half],
            recv_sem=recv.at[half],
            device_id=(gx, there * 2 + core),
            device_id_type=MESH,
        )

    def near_sends(there, t):
        return [
            relay(sendbuf.at[there, half], recvbuf.at[chip, half], there, strip_send_sem.at[t], strip_recv_sem.at[t], half)
            for half in range(HALVES)
        ]

    reach = 2 * nblocks

    def pack(there):
        span = (seq - width) // DEALS

        def deal_step(i, carry):
            cols = pl.ds(pl.multiple_of(width + i * span, LANES), span)
            both = jnp.concatenate([ordered[0, there, :, cols], got[there, :, cols]], axis=0)
            roles[:, pl.ds(pl.multiple_of(i * span, LANES), span)] = permuted(deal[there], both)
            return carry

        lax.fori_loop(0, DEALS, deal_step, 0)

        def half_step(half, carry):
            def count(role):
                at = there * pool + half * ROLES * 8 + role * 8
                return cnt[pl.ds(pl.multiple_of(at, 8), 8), :]

            def blocks(role):
                at = pl.ds(pl.multiple_of(half * ROLES * 8 + role * 8, 8), 8)
                return [roles[at, j * LANES : (j + 1) * LANES] for j in range(nblocks)]

            def side(outer, inner):
                n = count(outer)
                behind = shifted_up(blocks(inner), shift_bits(n), reach)
                near_end = blocks(outer)
                return [jnp.where(n > p, near_end[p], behind[p]) for p in range(nblocks)] + behind[nblocks:]

            left, right = side(0, 1), side(3, 2)
            left_n = count(0) + count(1)
            for p in range(STRIP_BLOCKS):
                q = STRIP_BLOCKS - 1 - p
                if q >= reach:
                    value = left[p]
                elif p >= reach:
                    value = right[q]
                else:
                    value = jnp.where(left_n > p, left[p], right[q])
                sendbuf[there, half, :, p * LANES : (p + 1) * LANES] = value
            return carry

        lax.fori_loop(0, HALVES, half_step, 0)

    far = peer_of(chip, chips - 1, chips)
    first_legs = [relay(sendbuf.at[far, half], passing.at[half], chip_x, first_leg_send_sem, first_leg_recv_sem, half) for half in range(HALVES)]

    def pack_step(t, carry):
        pack(peer_of(chip, chips - 1 - t, chips))

        @pl.when(t == 0)
        def _():
            for copy in first_legs:
                copy.start()

        @pl.when(t == 1)
        def _():
            for copy in near_sends(chip_y, 1):
                copy.start()

        return carry

    lax.fori_loop(0, chips - 1, pack_step, 0)

    info_recv[gy] = info_send[chip]
    for copy in info_copies[1:]:
        copy.wait()
    info_recv[mate] = info_got[chip]
    arrived = info_recv[...]
    fill_here = lax.broadcasted_iota(jnp.int32, (8, LANES), 1) == fill_lane
    counts[0] = jnp.where(fill_here, local_fill, jnp.sum(arrived, axis=0))

    def count_send(k):
        return pltpu.make_async_remote_copy(
            src_ref=counts.at[2 * k],
            dst_ref=counts.at[2 * k + 1],
            send_sem=count_send_sem.at[k],
            recv_sem=count_recv_sem.at[k],
            device_id=(partner(gx, 2**k, n_gx), gy),
            device_id_type=MESH,
        )

    def count_join(k):
        count_send(k).wait()
        one, other = counts[2 * k], counts[2 * k + 1]
        counts[2 * k + 2] = jnp.where(fill_here, jnp.maximum(one, other), one + other)

    count_send(0).start()

    eye = lax.broadcasted_iota(jnp.int32, (slots, slots), 0) == lax.broadcasted_iota(jnp.int32, (slots, slots), 1)
    for m in range(members_dev):
        len_col[m] = jnp.broadcast_to(jnp.sum(jnp.where(eye, lens[m], 0.0), axis=1, keepdims=True), (slots, LANES))
    sum_policy[...] = jnp.zeros_like(sum_policy)
    sum_kl[...] = jnp.zeros_like(sum_kl)

    def sum_step(c, carry):
        positions = (lax.broadcasted_iota(jnp.int32, (slots, piece), 1) + c * piece).astype(f32)
        for m in range(members_dev):
            pol = policy[c, m]
            log_ratio = anchor[c, m] - pol
            ratio = jnp.exp(log_ratio)
            valid = positions < len_col[m][:, :1]
            sum_policy[m] += folded(jnp.where(valid, pol, 0.0))
            sum_kl[m] += folded(jnp.where(valid, kl_weight * (ratio - log_ratio - 1.0), 0.0))
        return carry

    lax.fori_loop(0, PIECES, sum_step, 0)
    sums = []
    for buf in (sum_policy, sum_kl):
        per_member = [row_of(jnp.sum(buf[m], axis=1, keepdims=True)) for m in range(members_dev)]
        sums.append(row_sums(place, targets, per_member))
    for k in range(1, rounds):
        count_join(k - 1)
        count_send(k).start()
    count_join(rounds - 1)
    tails_send[...] = tiles(sums, jnp.broadcast_to(counts[2 * rounds][None], (n_gy, 8, LANES)))
    tail_copies = tile_sends(tails_send, tails_recv, tail_send_sem, tail_recv_sem, range(1, n_gy))
    for copy in tail_copies:
        copy.start()
    tails_recv[gy] = tails_send[chip]

    for copy in near_sends(chip_x, 0):
        copy.start()


    ntok = counts[2 * rounds][:1, info_lane : info_lane + 1]
    scale = samples * seq / ntok
    got_len = column_in(arrived, 0).reshape(total_rows, 1)
    got_row = row_of(got_len)
    reward = column_in(arrived, 1).reshape(members, part, 1)
    advantage = (members * reward - jnp.sum(reward, axis=0)[None]) / (members - 1)
    adv_rows[...] = jnp.broadcast_to(advantage, adv_rows.shape)
    len_rows[...] = jnp.broadcast_to(got_len.reshape(members, part, 1), len_rows.shape)
    got_spot_row, got_spot = strip_plan(
        got_row, got_len, (row // pool).astype(f32), (column // pool).astype(f32),
        lax.rem(row, pool).astype(f32), lax.rem(column, pool).astype(f32), chips, seq,
    )
    rcnt[...] = jnp.broadcast_to(strip_counts(got_spot_row, got_row), rcnt.shape)
    lane = lax.broadcasted_iota(jnp.int32, (total_rows, LANES), 1).astype(f32)
    for half in range(HALVES):
        pick = got_spot - half * ROLES * 8 == lane
        pick = jnp.where(pick & (lane < ROLES * 8), 1.0, 0.0).astype(jnp.bfloat16)
        undeal[:, half] = pick.reshape(chips, pool, LANES)
    half_rows[...] = jnp.broadcast_to(jnp.where(got_spot < ROLES * 8, 0.0, 1.0).reshape(members, part, 1), half_rows.shape)
    def finish_rows(k, start, value, only=None):
        span = value.shape[1]
        cols = pl.ds(pl.multiple_of(start, LANES), span)
        positions = (lax.broadcasted_iota(jnp.int32, (part, span), 1) + start).astype(f32)
        value = (value - adv_rows[k][:, :1]) * scale
        value = jnp.where(positions < len_rows[k][:, :1], value, 0.0)
        if only is not None:
            value = jnp.where(only, value, done[k, :, cols])
        done[k, :, cols] = value

    def own_step(which, source):
        def column_step(c, carry):
            start = pl.multiple_of(c * piece, LANES)
            for m in range(members_dev):
                finish_rows(source * members_dev + m, start, which(m * part, pl.ds(start, piece)))
            return carry

        lax.fori_loop(0, PIECES, column_step, 0)

    own_step(lambda r, cols: ordered[0, chip, r : r + part, cols], gy)
    give_own.wait_recv()
    own_step(lambda r, cols: got[chip, r : r + part, cols], mate)

    def first_wait(off):
        landed = heads_in.at[0]
        pltpu.make_async_copy(landed, landed, first_recv_sem.at[off - 2]).wait()

    def first_step(off, carry):
        first_wait(off)
        source = peer_of(gy, off, n_gy)
        for m in range(members_dev):
            finish_rows(source * members_dev + m, 0, heads_in[source, m * part : (m + 1) * part, :])
        return carry

    lax.fori_loop(2, n_gy, first_step, 0)

    def unpack(there, t, half):
        landed = recvbuf.at[0, 0]
        pltpu.make_async_copy(landed, landed, strip_recv_sem.at[t, half]).wait()

        def put(r, start, rows):
            k = there * 2 * members_dev + r
            finish_rows(k, width + start, rows, half_rows[k][:, :1] > 0.5 if half else None)

        unpack_strips(recvbuf, roles, undeal, rcnt, there, half, part, put)

    second_legs = [
        relay(passing.at[half], recvbuf.at[chip_x, half], chip_y, strip_send_sem.at[2], strip_recv_sem.at[2], half)
        for half in range(HALVES)
    ]
    for first_leg, second_leg in zip(first_legs, second_legs):
        first_leg.wait_recv()
        second_leg.start()
    for half in range(HALVES):
        unpack(chip_y, 1, half)

    for copy in tail_copies:
        copy.wait()
    ends = tails_recv[...]
    first_sum = column_in(ends, 0).reshape(members, part, 1)
    second_sum = column_in(ends, 1).reshape(members, part, 1)
    value = (second_sum - advantage * first_sum) * (samples / ntok)[None]
    shape = (members, part, LANES)
    spread = lax.broadcasted_iota(jnp.int32, shape, 1) == lax.broadcasted_iota(jnp.int32, shape, 2)
    loss_ref[...] = jnp.sum(jnp.where(spread, value, 0.0), axis=1)[:, :part]
    adv_ref[...] = jnp.sum(jnp.where(spread, advantage, 0.0), axis=1)[:, :part]
    over_ref[0, 0] = (jnp.max(ends[:, :, fill_lane : fill_lane + 1]) > STRIP_BLOCKS).astype(jnp.int32)
    for off in FIRST_ORDER:
        landed = heads_in.at[0]
        pltpu.make_async_copy(landed, landed, first_send_sem.at[off - 2]).wait()
    pltpu.make_async_copy(given, given, give_send_sem.at[0]).wait()
    give_own.wait_send()

    scale_ref[...] = jnp.broadcast_to(scale, scale_ref.shape)

    def unpack_step(i, carry):
        unpack(peer_of(chip, 1 + 2 * i, chips), 2 * i, 0)
        return carry

    lax.fori_loop(0, 2, unpack_step, 0)
    for t in (0, 2):
        landed = recvbuf.at[0, 0]
        pltpu.make_async_copy(landed, landed, strip_recv_sem.at[t, 1]).wait()
    for half in range(HALVES):
        first_legs[half].wait_send()
        for t in range(chips - 1):
            sent = sendbuf.at[0, 0]
            pltpu.make_async_copy(sent, sent, strip_send_sem.at[t, half]).wait()


def store(
    n_gy, done, loss, adv, recvbuf, undeal, rcnt, len_rows, adv_rows, half_rows, scale_ref,
    grad, loss_out, adv_out, last, roles, sem,
):
    chips = n_gy // 2
    members, part, seq = done.shape
    group = members // chips
    width = seq - roles.shape[1]
    chip = lax.axis_index("gy") // 2
    scale = scale_ref[:1, :1]

    def chip_rows(there):
        return pl.ds(there * group, group)

    whole = [chip_rows(chip), chip_rows(peer_of(chip, 2, chips))]
    late = [peer_of(chip, 1, chips), peer_of(chip, 3, chips)]
    first = pl.ds(0, width)
    copies = [pltpu.make_async_copy(done.at[rows], grad.at[rows], sem.at[k]) for k, rows in enumerate(whole)]
    copies += [
        pltpu.make_async_copy(done.at[chip_rows(there), :, first], grad.at[chip_rows(there), :, first], sem.at[2 + k])
        for k, there in enumerate(late)
    ]
    copies += [pltpu.make_async_copy(loss, loss_out, sem.at[4]), pltpu.make_async_copy(adv, adv_out, sem.at[5])]
    for copy in copies:
        copy.start()

    def store_late(i):
        rows = chip_rows(peer_of(chip, 1 + 2 * i, chips))
        return pltpu.make_async_copy(last.at[i], grad.at[rows, :, pl.ds(width, seq - width)], sem.at[6 + i])

    def late_step(i, carry):
        there = peer_of(chip, 1 + 2 * i, chips)

        def put(r, start, rows):
            k, span = there * group + r, rows.shape[1]
            positions = (lax.broadcasted_iota(jnp.int32, (part, span), 1) + (width + start)).astype(jnp.float32)
            value = (rows - adv_rows[k][:, :1]) * scale
            before = done[k, :, pl.ds(pl.multiple_of(width + start, LANES), span)]
            value = jnp.where(half_rows[k][:, :1] > 0.5, jnp.where(positions < len_rows[k][:, :1], value, 0.0), before)
            last[i, r, :, pl.ds(start, span)] = value

        unpack_strips(recvbuf, roles, undeal, rcnt, there, 1, part, put)
        store_late(i).start()
        return carry

    lax.fori_loop(0, 2, late_step, 0)
    copies += [store_late(i) for i in range(2)]
    for copy in copies:
        copy.wait()


def packed_body(n_gx, n_gy, policy_logp, anchor_logp, lengths, rewards, slot_prompt):
    members_dev, slots, seq = policy_logp.shape
    members, part = members_dev * n_gy, slots // n_gy
    f32, bf16 = jnp.float32, jnp.bfloat16
    chips, rows = n_gy // 2, members_dev * part
    pool = 2 * rows
    width = HEAD_BLOCKS * LANES
    chunked = (PIECES, members_dev, slots, seq // PIECES)
    strips = (chips, HALVES, 8, STRIP_BLOCKS * LANES)
    per_slot = (members_dev, slots, LANES)
    per_sample = (members, part, LANES)
    tile = (n_gy, 8, LANES)
    hbm_spec = pl.BlockSpec(memory_space=pltpu.HBM)
    vmem_spec = pl.BlockSpec(memory_space=pltpu.VMEM)
    dma = pltpu.SemaphoreType.DMA
    handed = (
        pltpu.VMEM(strips, f32),
        pltpu.VMEM((chips, HALVES, pool, LANES), bf16),
        pltpu.VMEM((chips * pool, LANES), f32),
        pltpu.VMEM(per_sample, f32),
        pltpu.VMEM(per_sample, f32),
        pltpu.VMEM(per_sample, f32),
        pltpu.VMEM((8, LANES), f32),
    )
    done, loss, adv, over, *rest = pl.pallas_call(
        functools.partial(packed_exchange, n_gx, n_gy),
        out_shape=(
            pltpu.VMEM((members, part, seq), f32),
            pltpu.VMEM((members, part), f32),
            pltpu.VMEM((members, part), f32),
            pltpu.SMEM((1, 1), jnp.int32),
        ) + handed,
        in_specs=[hbm_spec] * 5,
        out_specs=(vmem_spec,) * 3 + (pl.BlockSpec(memory_space=pltpu.SMEM),) + (vmem_spec,) * len(handed),
        scratch_shapes=[
            pltpu.VMEM(chunked, f32),
            pltpu.VMEM(chunked, f32),
            pltpu.VMEM((members_dev, slots), jnp.int32),
            pltpu.VMEM((members_dev, slots), jnp.int32),
            pltpu.VMEM((members_dev, slots), jnp.int32),
            pltpu.VMEM((2 * chips * rows, members_dev * slots), bf16),
            pltpu.VMEM((2, chips, rows, seq), f32),
            pltpu.VMEM((chips, rows, seq), f32),
            pltpu.VMEM((n_gy, rows, width), f32),
            pltpu.VMEM(strips, f32),
            pltpu.VMEM(strips[1:], f32),
            pltpu.VMEM((pool, seq - width), f32),
            pltpu.VMEM((chips, pool, pool), bf16),
            pltpu.VMEM((chips * pool, LANES), f32),
            pltpu.VMEM(per_slot, f32),
            pltpu.VMEM(per_slot, f32),
            pltpu.VMEM(per_slot, f32),
            pltpu.VMEM(tile, f32),
            pltpu.VMEM((chips, 8, LANES), f32),
            pltpu.VMEM(tile, f32),
            pltpu.VMEM(tile, f32),
            pltpu.VMEM(tile, f32),
            pltpu.VMEM((2 * n_gx, 8, LANES), f32),
            dma((3,)),
            dma((2, PIECES)),
            dma((2,)),
            dma((2,)),
            dma((n_gy - 2,)),
            dma((n_gy - 2,)),
            dma((chips - 1, HALVES)),
            dma((chips - 1, HALVES)),
            dma((HALVES,)),
            dma((HALVES,)),
            dma((n_gy - 1,)),
            dma((n_gy - 1,)),
            dma((n_gy - 1,)),
            dma((n_gy - 1,)),
            dma((n_gx,)),
            dma((n_gx,)),
        ],
        compiler_params=pltpu.CompilerParams(collective_id=0, has_side_effects=True, vmem_limit_bytes=36 * 2**20),
    )(policy_logp, anchor_logp, lengths, rewards, slot_prompt)

    def fits(policy_logp, anchor_logp, lengths, rewards, slot_prompt, done, loss, adv, *rest):
        small = jax.ShapeDtypeStruct((members, part), f32)
        return tuple(pl.pallas_call(
            functools.partial(store, n_gy),
            out_shape=(jax.ShapeDtypeStruct((members, part, seq), f32), small, small),
            in_specs=[vmem_spec] * (3 + len(rest)),
            out_specs=(hbm_spec,) * 3,
            scratch_shapes=[
                pltpu.VMEM((2, 2 * members_dev, part, seq - width), f32),
                pltpu.VMEM((ROLES * 8, seq - width), f32),
                dma((8,)),
            ],
            compiler_params=pltpu.CompilerParams(vmem_limit_bytes=16 * 2**20),
        )(done, loss, adv, *rest))

    def overflows(policy_logp, anchor_logp, lengths, rewards, slot_prompt, done, loss, adv, *rest):
        return tuple(unpacked_body(n_gx, n_gy, policy_logp, anchor_logp, lengths, rewards, slot_prompt))

    return lax.cond(
        over[0, 0] > 0, overflows, fits,
        policy_logp, anchor_logp, lengths, rewards, slot_prompt, done, loss, adv, *rest,
    )


def body(n_gx, n_gy, *args):
    members_dev, slots, seq = args[0].shape
    pool = 2 * members_dev * slots // n_gy
    packs = n_gy == 8 and n_gx in (2, 4, 8) and pool == ROLES * STRIPS and slots == LANES and seq == LANES * 32 and seq % (PIECES * LANES) == 0
    return (packed_body if packs else unpacked_body)(n_gx, n_gy, *args)


def solution(mesh):
    placed = (P("gy", "gx", None), P("gy", "gx", None), P("gy", "gx"), P("gy", "gx"), P("gy", "gx"))
    return jax.shard_map(
        functools.partial(body, mesh.shape["gx"], mesh.shape["gy"]),
        mesh=mesh,
        in_specs=placed,
        out_specs=(P(None, ("gx", "gy"), None), P(None, ("gx", "gy")), P(None, ("gx", "gy"))),
        check_vma=False,
    )
```

```python
import functools

import jax
import jax.numpy as jnp
from jax import lax
from jax.experimental import pallas as pl
from jax.experimental.pallas import tpu as pltpu
from jax.sharding import PartitionSpec as P

kl_weight = 0.1
LANES = 128
CHUNKS = 8
MESH = pl.DeviceIdType.MESH
ROLES = 4
STRIPS = 16
HALVES = STRIPS // 8
SHIFTS = 5
PIECES = 8
DEALS = 1
UNDEALS = 1
HEAD_BLOCKS = 6
STRIP_BLOCKS = 66
FIRST_ORDER = (2, 4, 3, 5, 6, 7)


def partner(index, off, count):
    out, bit = index, 1
    while bit < count:
        if off & bit:
            out = out + bit - 2 * bit * lax.rem(index // bit, 2)
        bit *= 2
    return out


def offsets_by_distance(count):
    far = max(bin(off // 2).count("1") for off in range(1, count))
    near = [off for off in range(1, count) if bin(off // 2).count("1") < far]
    return near, [off for off in range(1, count) if off not in near]


def permuted(onehot, rows):
    high = rows.astype(jnp.bfloat16)
    rest = rows - high.astype(jnp.float32)
    middle = rest.astype(jnp.bfloat16)
    low = (rest - middle.astype(jnp.float32)).astype(jnp.bfloat16)
    dot = functools.partial(jnp.dot, preferred_element_type=jnp.float32)
    return dot(onehot, high) + dot(onehot, middle) + dot(onehot, low)


def folded(x):
    out = x[:, :LANES]
    for start in range(LANES, x.shape[1], LANES):
        out = out + x[:, start : start + LANES]
    return out


def exchange(
    n_gx, n_gy, policy_hbm, anchor_hbm, len_ref, reward_ref, prompt_ref,
    raw_hbm, heads_ref, tails_ref, ntok_ref,
    policy, anchor, sendbuf, onehot, len_col, sum_policy, sum_kl,
    heads_send, heads_recv, tails_send, tails_recv, counts,
    load_sem, send_sem, recv_sem, own_sem,
    head_send_sem, head_recv_sem, tail_send_sem, tail_recv_sem, count_send_sem, count_recv_sem,
):
    gx, gy = lax.axis_index("gx"), lax.axis_index("gy")
    members_dev, slots, seq = policy_hbm.shape
    part = slots // n_gy
    width = seq // CHUNKS

    near, far = offsets_by_distance(n_gy)
    barrier = pltpu.get_barrier_semaphore()
    for off in range(1, n_gy):
        pl.semaphore_signal(barrier, inc=1, device_id=(gx, partner(gy, off, n_gy)), device_id_type=MESH)
    for off in range(1, n_gx):
        pl.semaphore_signal(barrier, inc=1, device_id=(lax.rem(gx + off, n_gx), gy), device_id_type=MESH)

    def loads(c):
        cols = pl.ds(pl.multiple_of(c * width, LANES), width)
        return (
            pltpu.make_async_copy(policy_hbm.at[:, :, cols], policy.at[c], load_sem.at[0, c]),
            pltpu.make_async_copy(anchor_hbm.at[:, :, cols], anchor.at[c], load_sem.at[1, c]),
        )

    for c in range(CHUNKS):
        for copy in loads(c):
            copy.start()

    sublane = lax.broadcasted_iota(jnp.int32, (slots, slots), 0)
    lane = lax.broadcasted_iota(jnp.int32, (slots, slots), 1)
    column = lax.broadcasted_iota(jnp.int32, (slots, LANES), 1)
    local_tokens = jnp.sum(len_ref[...].astype(jnp.float32))
    for m in range(members_dev):
        seq_len = len_ref[m : m + 1, :].astype(jnp.float32)
        reward = reward_ref[m : m + 1, :].astype(jnp.float32) * 0.25
        match = sublane == lax.rem(prompt_ref[m : m + 1, :], slots)
        onehot[m] = jnp.where(match, 1.0, 0.0).astype(jnp.bfloat16)
        len_col[m] = jnp.broadcast_to(
            jnp.sum(jnp.where(sublane == lane, seq_len, 0.0), axis=1, keepdims=True), (slots, LANES)
        )
        sorted_len = jnp.sum(jnp.where(match, seq_len, 0.0), axis=1, keepdims=True)
        sorted_reward = jnp.sum(jnp.where(match, reward, 0.0), axis=1, keepdims=True)
        heads_send[m] = jnp.where(
            column == 0, sorted_len, jnp.where(column == 1, sorted_reward, local_tokens)
        )
    sum_policy[...] = jnp.zeros_like(sum_policy)
    sum_kl[...] = jnp.zeros_like(sum_kl)

    def compute(c):
        for copy in loads(c):
            copy.wait()
        positions = (lax.broadcasted_iota(jnp.int32, (slots, width), 1) + c * width).astype(jnp.float32)
        for m in range(members_dev):
            pol = policy[c, m]
            log_ratio = anchor[c, m] - pol
            ratio = jnp.exp(log_ratio)
            valid = positions < len_col[m][:, :1]
            sum_policy[m] += folded(jnp.where(valid, pol, 0.0))
            sum_kl[m] += folded(jnp.where(valid, kl_weight * (ratio - log_ratio - 1.0), 0.0))
            sendbuf[c, m] = permuted(onehot[m], kl_weight * (1.0 - ratio))

    def rows_of(device):
        return pl.ds(pl.multiple_of(device * part, part), part)

    my_members = pl.ds(gy * members_dev, members_dev)

    def sends(c, offs):
        cols = pl.ds(pl.multiple_of(c * width, LANES), width)
        copies = []
        for off in offs:
            peer = partner(gy, off, n_gy)
            copies.append(
                pltpu.make_async_remote_copy(
                    src_ref=sendbuf.at[c, :, rows_of(peer), :],
                    dst_ref=raw_hbm.at[my_members, :, cols],
                    send_sem=send_sem.at[off - 1],
                    recv_sem=recv_sem.at[off - 1],
                    device_id=(gx, peer),
                    device_id_type=MESH,
                )
            )
        return copies

    def own(c):
        cols = pl.ds(pl.multiple_of(c * width, LANES), width)
        return pltpu.make_async_copy(
            sendbuf.at[c, :, rows_of(gy), :], raw_hbm.at[my_members, :, cols], own_sem.at[c]
        )

    def small_sends(src, dst, send, recv):
        copies = []
        for off in range(1, n_gy):
            peer = partner(gy, off, n_gy)
            copies.append(
                pltpu.make_async_remote_copy(
                    src_ref=src.at[:, rows_of(peer), :],
                    dst_ref=dst.at[my_members],
                    send_sem=send.at[off - 1],
                    recv_sem=recv.at[off - 1],
                    device_id=(gx, peer),
                    device_id_type=MESH,
                )
            )
        copies.append(pltpu.make_async_copy(src.at[:, rows_of(gy), :], dst.at[my_members], send.at[n_gy - 1]))
        return copies

    def count_sends():
        return [
            pltpu.make_async_remote_copy(
                src_ref=counts.at[0],
                dst_ref=counts.at[off],
                send_sem=count_send_sem.at[off - 1],
                recv_sem=count_recv_sem.at[off - 1],
                device_id=(lax.rem(gx + off, n_gx), gy),
                device_id_type=MESH,
            )
            for off in range(1, n_gx)
        ]

    compute(0)
    pl.semaphore_wait(barrier, n_gy - 1 + n_gx - 1)
    head_copies = small_sends(heads_send, heads_recv, head_send_sem, head_recv_sem)
    for copy in head_copies:
        copy.start()

    def step(c, carry):
        for copy in sends(c - 1, near):
            copy.start()
        own(c - 1).start()
        compute(c)
        return carry

    lax.fori_loop(1, CHUNKS, step, 0)
    for copy in sends(CHUNKS - 1, near):
        copy.start()

    def far_step(c, carry):
        for copy in sends(c, far):
            copy.start()
        return carry

    lax.fori_loop(0, CHUNKS, far_step, 0)
    own(CHUNKS - 1).start()

    for m in range(members_dev):
        s1 = jnp.sum(permuted(onehot[m], sum_policy[m]), axis=1, keepdims=True)
        s2 = jnp.sum(permuted(onehot[m], sum_kl[m]), axis=1, keepdims=True)
        tails_send[m] = jnp.where(column == 0, s1, s2)
    for copy in head_copies:
        copy.wait()
    tokens = jnp.zeros((8, LANES), jnp.float32)
    for source in range(n_gy):
        tokens = tokens + heads_recv[source * members_dev, :8, :]
    counts[0] = tokens
    heads_ref[...] = heads_recv[...]
    tail_copies = small_sends(tails_send, tails_recv, tail_send_sem, tail_recv_sem)
    for copy in tail_copies:
        copy.start()
    count_copies = count_sends()
    for copy in count_copies:
        copy.start()
    for copy in count_copies:
        copy.wait()
    ntok_ref[...] = jnp.sum(counts[...], axis=0)
    for copy in tail_copies:
        copy.wait()
    tails_ref[...] = tails_recv[...]
    for c in range(CHUNKS):
        own(c).wait()
    for off in range(1, n_gy):
        source = partner(gy, off, n_gy)
        landed = raw_hbm.at[pl.ds(source * members_dev, members_dev)]
        pltpu.make_async_copy(landed, landed, recv_sem.at[off - 1]).wait()
        pltpu.make_async_copy(landed, landed, send_sem.at[off - 1]).wait()


def finish(samples, raw, heads, tails, ntok, grad, loss, adv, done, done_sem):
    members, part, seq = raw.shape
    tokens = ntok[:1, 2:3]
    total = jnp.sum(heads[...], axis=0)
    advantage = (members * heads[:, :, 1:2] - total[None, :, 1:2]) / (members - 1)
    positions = lax.broadcasted_iota(jnp.int32, (part, seq), 1).astype(jnp.float32)
    scale = samples * seq / tokens

    def store(k):
        return pltpu.make_async_copy(done.at[k], grad.at[k], done_sem.at[k])

    for k in range(members):
        done[k] = jnp.where(positions < heads[k, :, :1], raw[k] - advantage[k], 0.0) * scale
        if k > 0:
            store(k - 1).start()
    shape = (members, part, LANES)
    eye = lax.broadcasted_iota(jnp.int32, shape, 1) == lax.broadcasted_iota(jnp.int32, shape, 2)
    store(members - 1).start()
    value = (tails[:, :, 1:2] - advantage * tails[:, :, :1]) * (samples / tokens)[None]
    loss[...] = jnp.sum(jnp.where(eye, value, 0.0), axis=1)[:, :part]
    adv[...] = jnp.sum(jnp.where(eye, advantage, 0.0), axis=1)[:, :part]
    for k in range(members):
        store(k).wait()


def unpacked_body(n_gx, n_gy, policy_logp, anchor_logp, lengths, rewards, slot_prompt):
    members_dev, slots, seq = policy_logp.shape
    members, part = members_dev * n_gy, slots // n_gy
    f32 = jnp.float32
    chunked = (CHUNKS, members_dev, slots, seq // CHUNKS)
    small = (members, part, LANES)
    hbm_spec = pl.BlockSpec(memory_space=pltpu.HBM)
    vmem_spec = pl.BlockSpec(memory_space=pltpu.VMEM)
    dma = pltpu.SemaphoreType.DMA
    raw, heads, tails, ntok = pl.pallas_call(
        functools.partial(exchange, n_gx, n_gy),
        out_shape=(
            pltpu.VMEM((members, part, seq), f32),
            pltpu.VMEM(small, f32),
            pltpu.VMEM(small, f32),
            pltpu.VMEM((8, LANES), f32),
        ),
        in_specs=[hbm_spec, hbm_spec, vmem_spec, vmem_spec, vmem_spec],
        out_specs=(vmem_spec, vmem_spec, vmem_spec, vmem_spec),
        scratch_shapes=[
            pltpu.VMEM(chunked, f32),
            pltpu.VMEM(chunked, f32),
            pltpu.VMEM(chunked, f32),
            pltpu.VMEM((members_dev, slots, slots), jnp.bfloat16),
            pltpu.VMEM((members_dev, slots, LANES), f32),
            pltpu.VMEM((members_dev, slots, LANES), f32),
            pltpu.VMEM((members_dev, slots, LANES), f32),
            pltpu.VMEM((members_dev, slots, LANES), f32),
            pltpu.VMEM(small, f32),
            pltpu.VMEM((members_dev, slots, LANES), f32),
            pltpu.VMEM(small, f32),
            pltpu.VMEM((n_gx, 8, LANES), f32),
            dma((2, CHUNKS)),
            dma((n_gy - 1,)),
            dma((n_gy - 1,)),
            dma((CHUNKS,)),
            dma((n_gy,)),
            dma((n_gy - 1,)),
            dma((n_gy,)),
            dma((n_gy - 1,)),
            dma((n_gx - 1,)),
            dma((n_gx - 1,)),
        ],
        compiler_params=pltpu.CompilerParams(collective_id=1, has_side_effects=True, vmem_limit_bytes=36 * 2**20),
    )(policy_logp, anchor_logp, lengths, rewards, slot_prompt)
    samples = members * slots * n_gx
    return pl.pallas_call(
        functools.partial(finish, samples),
        out_shape=(
            jax.ShapeDtypeStruct((members, part, seq), f32),
            jax.ShapeDtypeStruct((members, part), f32),
            jax.ShapeDtypeStruct((members, part), f32),
        ),
        in_specs=[vmem_spec] * 4,
        out_specs=(hbm_spec, vmem_spec, vmem_spec),
        scratch_shapes=[pltpu.VMEM((members, part, seq), f32), dma((members,))],
        compiler_params=pltpu.CompilerParams(vmem_limit_bytes=32 * 2**20),
    )(raw, heads, tails, ntok)


def row_of(column):
    n = column.shape[0]
    eye = lax.broadcasted_iota(jnp.int32, (n, n), 0) == lax.broadcasted_iota(jnp.int32, (n, n), 1)
    return jnp.sum(jnp.where(eye, column, 0.0), axis=0, keepdims=True)


def row_sums(place, targets, values):
    out = None
    for target, value in zip(targets, values):
        here = jnp.sum(jnp.where(place == target, value, 0.0), axis=1, keepdims=True)
        out = here if out is None else out + here
    return out


def strip_spot(rank):
    first, second, third = rank < STRIPS, rank < 2 * STRIPS, rank < 3 * STRIPS
    strip = jnp.where(
        first, rank, jnp.where(second, 2 * STRIPS - 1 - rank, jnp.where(third, 3 * STRIPS - 1 - rank, rank - 3 * STRIPS))
    )
    role = jnp.where(first, 0.0, jnp.where(second, 3.0, jnp.where(third, 2.0, 1.0)))
    half = jnp.floor(strip * (1.0 / 8))
    return half * (ROLES * 8) + role * 8 + strip - half * 8


def strip_plan(len_row, len_column, group_row, group_column, index_row, index_column, n_groups, seq):
    rows = ROLES * STRIPS
    key_row = group_row * ((seq + 1) * rows) + len_row * rows + index_row
    key_column = group_column * ((seq + 1) * rows) + len_column * rows + index_column
    above_row = jnp.sum(jnp.where(key_column > key_row, 1.0, 0.0), axis=0, keepdims=True)
    above_column = jnp.sum(jnp.where(key_row > key_column, 1.0, 0.0), axis=1, keepdims=True)
    return (
        strip_spot(above_row - rows * (n_groups - 1 - group_row)),
        strip_spot(above_column - rows * (n_groups - 1 - group_column)),
    )


def tail_blocks(lens):
    return jnp.maximum(jnp.floor((lens + (LANES - 1)) * (1.0 / LANES)) - HEAD_BLOCKS, 0.0)


def shift_bits(count):
    shift = count.astype(jnp.int32)
    return [(lax.shift_right_logical(shift, k) & 1) == 1 for k in range(SHIFTS)]


def shifted_up(blocks, bits, reach):
    for k in range(SHIFTS):
        step, n = 2**k, len(blocks)
        moved = []
        for p in range(min(n + step, reach)):
            if p < step:
                moved.append(blocks[p])
            elif p >= n:
                moved.append(blocks[p - step])
            else:
                moved.append(jnp.where(bits[k], blocks[p - step], blocks[p]))
        blocks = moved
    return blocks


def shifted_down(blocks, bits, count):
    for k in reversed(range(SHIFTS)):
        step = 2**k
        keep = min(len(blocks), count + step - 1)
        blocks = [
            jnp.where(bits[k], blocks[p + step], blocks[p]) if p + step < len(blocks) else blocks[p] for p in range(keep)
        ]
    return blocks


def peer_of(index, off, count):
    out, bit = 0, 1
    while bit < count:
        a, b = lax.rem(index // bit, 2), lax.rem(off // bit, 2)
        out = out + bit * (a + b - 2 * a * b)
        bit *= 2
    return out


def unpack_strips(recvbuf, roles, undeal, rcnt, there, half, part, put):
    pool, seq_tail = undeal.shape[2], roles.shape[1]
    nblocks = seq_tail // LANES

    def count(role):
        at = there * pool + half * ROLES * 8 + role * 8
        return rcnt[pl.ds(pl.multiple_of(at, 8), 8), :]

    def block(p):
        return recvbuf[there, half, :, p * LANES : (p + 1) * LANES]

    for outer, inner, at in ((0, 1, lambda p: p), (3, 2, lambda p: STRIP_BLOCKS - 1 - p)):
        for j in range(nblocks):
            roles[outer * 8 : outer * 8 + 8, j * LANES : (j + 1) * LANES] = block(at(j))
        behind = [block(at(p)) for p in range(2 * nblocks)]
        behind = shifted_down(behind, shift_bits(count(outer)), nblocks)
        for j in range(nblocks):
            roles[inner * 8 : inner * 8 + 8, j * LANES : (j + 1) * LANES] = behind[j]
    order = undeal[there, half][:, : ROLES * 8]
    span = seq_tail // UNDEALS

    def undeal_step(i, carry):
        start = pl.multiple_of(i * span, LANES)
        out = permuted(order, roles[: ROLES * 8, pl.ds(start, span)])
        for r in range(pool // part):
            put(r, start, out[r * part : (r + 1) * part])
        return carry

    lax.fori_loop(0, UNDEALS, undeal_step, 0)


def packed_exchange(
    n_gx, n_gy, policy_hbm, anchor_hbm, len_hbm, reward_hbm, prompt_hbm,
    done, loss_ref, adv_ref, over_ref, recvbuf, undeal, rcnt, len_rows, adv_rows, half_rows, scale_ref,
    policy, anchor, len_ref, reward_ref, prompt_ref, onehot, ordered, got, heads_in, sendbuf, passing, roles,
    deal, cnt, len_col, sum_policy, sum_kl,
    info_send, info_got, info_recv, tails_send, tails_recv, counts,
    small_sem, load_sem, give_send_sem, give_recv_sem, first_send_sem, first_recv_sem, strip_send_sem, strip_recv_sem, first_leg_send_sem, first_leg_recv_sem,
    info_send_sem, info_recv_sem, tail_send_sem, tail_recv_sem, count_send_sem, count_recv_sem,
):
    gx, gy = lax.axis_index("gx"), lax.axis_index("gy")
    core, chip = lax.rem(gy, 2), gy // 2
    mate = chip * 2 + 1 - core
    members_dev, slots, seq = policy_hbm.shape
    members, part = members_dev * n_gy, slots // n_gy
    chips = n_gy // 2
    width = HEAD_BLOCKS * LANES
    piece = seq // PIECES
    nblocks = seq // LANES - HEAD_BLOCKS
    rows = members_dev * part
    pool = 2 * rows
    total_rows = chips * pool
    samples = members * slots * n_gx
    info_lane, fill_lane = 16, 17
    inner = (gx == 1) | (gx == 2)
    f32 = jnp.float32

    small_loads = [
        pltpu.make_async_copy(src, dst, small_sem.at[k])
        for k, (src, dst) in enumerate(((len_hbm, len_ref), (prompt_hbm, prompt_ref), (reward_hbm, reward_ref)))
    ]
    for copy in small_loads:
        copy.start()

    def loads(c):
        cols = pl.ds(pl.multiple_of(c * piece, LANES), piece)
        return (
            pltpu.make_async_copy(policy_hbm.at[:, :, cols], policy.at[c], load_sem.at[0, c]),
            pltpu.make_async_copy(anchor_hbm.at[:, :, cols], anchor.at[c], load_sem.at[1, c]),
        )

    for copy in loads(0):
        copy.start()
    barrier = pltpu.get_barrier_semaphore()
    for off in range(1, n_gy):
        pl.semaphore_signal(barrier, inc=1, device_id=(gx, partner(gy, off, n_gy)), device_id_type=MESH)
    pl.semaphore_signal(barrier, inc=1, device_id=(partner(gx, 1, n_gx), gy), device_id_type=MESH)

    @pl.when(inner)
    def _():
        pl.semaphore_signal(barrier, inc=1, device_id=(n_gx - 1 - gx, gy), device_id_type=MESH)

    for c in range(1, PIECES):
        for copy in loads(c):
            copy.start()
    for copy in small_loads:
        copy.wait()

    lens = [len_ref[m : m + 1, :].astype(f32) for m in range(members_dev)]
    targets = []
    for m in range(members_dev):
        spot = lax.rem(prompt_ref[m : m + 1, :], slots)
        device = spot // part
        other = lax.rem(device + core, 2)
        target = (other * chips + device // 2) * rows + m * part + spot - device * part
        targets.append(target.astype(f32))
    place = lax.broadcasted_iota(jnp.int32, (total_rows, slots), 0).astype(f32)
    for m in range(members_dev):
        onehot[:, m * slots : (m + 1) * slots] = jnp.where(place == targets[m], 1.0, 0.0).astype(jnp.bfloat16)

    def put_in_order(c):
        for copy in loads(c):
            copy.wait()
        values = kl_weight * (1.0 - jnp.exp(anchor[c] - policy[c]))
        out = permuted(onehot[...], values.reshape(members_dev * slots, piece))
        cols = pl.ds(pl.multiple_of(c * piece, LANES), piece)
        ordered[:, :, :, cols] = out.reshape(2, chips, rows, piece)

    def give(c, there):
        cols = pl.ds(pl.multiple_of(c * piece, LANES), piece)
        return pltpu.make_async_remote_copy(
            src_ref=ordered.at[1, there, :, cols],
            dst_ref=got.at[there, :, cols],
            send_sem=give_send_sem.at[0],
            recv_sem=give_recv_sem.at[0],
            device_id=(gx, mate),
            device_id_type=MESH,
        )

    give_own = pltpu.make_async_remote_copy(
        src_ref=ordered.at[1, chip],
        dst_ref=got.at[chip],
        send_sem=give_send_sem.at[1],
        recv_sem=give_recv_sem.at[1],
        device_id=(gx, mate),
        device_id_type=MESH,
    )
    given = got.at[pl.ds(0, chips - 1), :, pl.ds(piece, seq - piece)]

    def first_send(off, lo, hi):
        peer = partner(gy, off, n_gy)
        cols = pl.ds(lo, hi - lo)
        return pltpu.make_async_remote_copy(
            src_ref=ordered.at[off % 2, peer // 2, :, cols],
            dst_ref=heads_in.at[gy, :, cols],
            send_sem=first_send_sem.at[off - 2],
            recv_sem=first_recv_sem.at[off - 2],
            device_id=(gx, peer),
            device_id_type=MESH,
        )

    tile_lane = lax.broadcasted_iota(jnp.int32, (n_gy, 8, LANES), 2)
    groups = rows // 8
    local_tokens = sum(jnp.sum(length) for length in lens)

    def tiles(columns, base):
        out = base
        for f, column in enumerate(columns):
            split = column.reshape(n_gy, groups, 8, 1)
            for g in range(groups):
                out = jnp.where(tile_lane == g * 4 + f, split[:, g], out)
        return out

    def column_in(tile, f):
        parts = [tile[:, :, g * 4 + f : g * 4 + f + 1][:, None] for g in range(groups)]
        return jnp.concatenate(parts, axis=1)

    def tile_sends(src, dst, send, recv, offs):
        copies = []
        for off in offs:
            peer = partner(gy, off, n_gy)
            copies.append(
                pltpu.make_async_remote_copy(
                    src_ref=src.at[off % 2 * chips + peer // 2],
                    dst_ref=dst.at[gy],
                    send_sem=send.at[off - 1],
                    recv_sem=recv.at[off - 1],
                    device_id=(gx, peer),
                    device_id_type=MESH,
                )
            )
        return copies

    mate_info = pltpu.make_async_remote_copy(
        src_ref=info_send.at[pl.ds(chips, chips)],
        dst_ref=info_got,
        send_sem=info_send_sem.at[0],
        recv_sem=info_recv_sem.at[0],
        device_id=(gx, mate),
        device_id_type=MESH,
    )
    info_copies = [mate_info] + tile_sends(info_send, info_recv, info_send_sem, info_recv_sem, range(2, n_gy))

    def order_step(c, carry):
        put_in_order(c)

        @pl.when(c == 0)
        def _():
            pl.semaphore_wait(barrier, n_gy + lax.rem((gx + 1) // 2, 2))
            for off in FIRST_ORDER:
                first_send(off, 0, piece).start()
            lens_out = row_sums(place, targets, lens)
            rewards = [reward_ref[m : m + 1, :].astype(f32) * 0.25 for m in range(members_dev)]
            rewards_out = row_sums(place, targets, rewards)
            info_send[...] = tiles((lens_out, rewards_out), jnp.broadcast_to(local_tokens, (n_gy, 8, LANES)))
            for copy in info_copies:
                copy.start()

        @pl.when(c == 1)
        def _():
            for off in FIRST_ORDER:
                first_send(off, piece, width).start()

        @pl.when(c >= 1)
        def _():
            for t in range(1, chips):
                give(c, peer_of(chip, t, chips)).start()

        return carry

    lax.fori_loop(0, PIECES, order_step, 0)
    give_own.start()
    own_len = column_in(info_send[:chips], 0).reshape(chips * rows, 1)

    mate_info.wait()
    pair_lens = jnp.concatenate(
        [own_len[: chips * rows].reshape(chips, 1, rows, 1), column_in(info_got[...], 0).reshape(chips, 1, rows, 1)], axis=1
    ).reshape(total_rows, 1)
    row = lax.broadcasted_iota(jnp.int32, (1, total_rows), 1)
    column = lax.broadcasted_iota(jnp.int32, (total_rows, 1), 0)

    def pair_index(i):
        inside = lax.rem(i, pool)
        return (lax.rem(inside // rows + core, 2) * rows + lax.rem(inside, rows)).astype(f32)

    pair_row = row_of(pair_lens)
    spot_row, _ = strip_plan(
        pair_row, pair_lens, (row // pool).astype(f32), (column // pool).astype(f32), pair_index(row), pair_index(column),
        chips, seq,
    )
    wide = lax.broadcasted_iota(jnp.int32, (total_rows, total_rows), 0).astype(f32)

    def strip_counts(spots, lens_row):
        return row_sums(wide, [spots + (row // pool).astype(f32) * pool], [tail_blocks(lens_row)])

    pair_counts = strip_counts(spot_row, pair_row)
    cnt[...] = jnp.broadcast_to(pair_counts, cnt.shape)
    fill = jnp.sum(pair_counts.reshape(chips, HALVES, ROLES, 8, 1), axis=2)
    sent_chip = lax.broadcasted_iota(jnp.int32, fill.shape, 0) != chip
    local_fill = jnp.max(jnp.where(sent_chip, fill, 0.0))
    square = lax.broadcasted_iota(jnp.int32, (pool, pool), 0).astype(f32)
    for s in range(chips):
        deal[s] = jnp.where(square == spot_row[:, s * pool : (s + 1) * pool], 1.0, 0.0).astype(jnp.bfloat16)
    pltpu.make_async_copy(given, given, give_recv_sem.at[0]).wait()

    chip_x, chip_y = peer_of(chip, 1, chips), peer_of(chip, 2, chips)

    def relay(src, dst, there, send, recv, half):
        return pltpu.make_async_remote_copy(
            src_ref=src,
            dst_ref=dst,
            send_sem=send.at[half],
            recv_sem=recv.at[half],
            device_id=(gx, there * 2 + core),
            device_id_type=MESH,
        )

    def near_sends(there, t):
        return [
            relay(sendbuf.at[there, half], recvbuf.at[chip, half], there, strip_send_sem.at[t], strip_recv_sem.at[t], half)
            for half in range(HALVES)
        ]

    reach = 2 * nblocks

    def pack(there):
        span = (seq - width) // DEALS

        def deal_step(i, carry):
            cols = pl.ds(pl.multiple_of(width + i * span, LANES), span)
            both = jnp.concatenate([ordered[0, there, :, cols], got[there, :, cols]], axis=0)
            roles[:, pl.ds(pl.multiple_of(i * span, LANES), span)] = permuted(deal[there], both)
            return carry

        lax.fori_loop(0, DEALS, deal_step, 0)

        def half_step(half, carry):
            def count(role):
                at = there * pool + half * ROLES * 8 + role * 8
                return cnt[pl.ds(pl.multiple_of(at, 8), 8), :]

            def blocks(role):
                at = pl.ds(pl.multiple_of(half * ROLES * 8 + role * 8, 8), 8)
                return [roles[at, j * LANES : (j + 1) * LANES] for j in range(nblocks)]

            def side(outer, inner):
                n = count(outer)
                behind = shifted_up(blocks(inner), shift_bits(n), reach)
                near_end = blocks(outer)
                return [jnp.where(n > p, near_end[p], behind[p]) for p in range(nblocks)] + behind[nblocks:]

            left, right = side(0, 1), side(3, 2)
            left_n = count(0) + count(1)
            for p in range(STRIP_BLOCKS):
                q = STRIP_BLOCKS - 1 - p
                if q >= reach:
                    value = left[p]
                elif p >= reach:
                    value = right[q]
                else:
                    value = jnp.where(left_n > p, left[p], right[q])
                sendbuf[there, half, :, p * LANES : (p + 1) * LANES] = value
            return carry

        lax.fori_loop(0, HALVES, half_step, 0)

    far = peer_of(chip, chips - 1, chips)
    first_legs = [relay(sendbuf.at[far, half], passing.at[half], chip_x, first_leg_send_sem, first_leg_recv_sem, half) for half in range(HALVES)]

    def pack_step(t, carry):
        pack(peer_of(chip, chips - 1 - t, chips))

        @pl.when(t == 0)
        def _():
            for copy in first_legs:
                copy.start()

        @pl.when(t == 1)
        def _():
            for copy in near_sends(chip_y, 1):
                copy.start()

        return carry

    lax.fori_loop(0, chips - 1, pack_step, 0)

    info_recv[gy] = info_send[chip]
    for copy in info_copies[1:]:
        copy.wait()
    info_recv[mate] = info_got[chip]
    arrived = info_recv[...]
    fill_here = lax.broadcasted_iota(jnp.int32, (8, LANES), 1) == fill_lane
    counts[0] = jnp.where(fill_here, local_fill, jnp.sum(arrived, axis=0))

    def count_send(k, to):
        return pltpu.make_async_remote_copy(
            src_ref=counts.at[2 * k],
            dst_ref=counts.at[2 * k + 1],
            send_sem=count_send_sem.at[k],
            recv_sem=count_recv_sem.at[k],
            device_id=(to, gy),
            device_id_type=MESH,
        )

    pair, across = partner(gx, 1, n_gx), n_gx - 1 - gx

    def count_join(k):
        one, other = counts[2 * k], counts[2 * k + 1]
        return jnp.where(fill_here, jnp.maximum(one, other), one + other)

    count_send(0, pair).start()

    eye = lax.broadcasted_iota(jnp.int32, (slots, slots), 0) == lax.broadcasted_iota(jnp.int32, (slots, slots), 1)
    for m in range(members_dev):
        len_col[m] = jnp.broadcast_to(jnp.sum(jnp.where(eye, lens[m], 0.0), axis=1, keepdims=True), (slots, LANES))
    sum_policy[...] = jnp.zeros_like(sum_policy)
    sum_kl[...] = jnp.zeros_like(sum_kl)

    def sum_step(c, carry):
        positions = (lax.broadcasted_iota(jnp.int32, (slots, piece), 1) + c * piece).astype(f32)
        for m in range(members_dev):
            pol = policy[c, m]
            log_ratio = anchor[c, m] - pol
            ratio = jnp.exp(log_ratio)
            valid = positions < len_col[m][:, :1]
            sum_policy[m] += folded(jnp.where(valid, pol, 0.0))
            sum_kl[m] += folded(jnp.where(valid, kl_weight * (ratio - log_ratio - 1.0), 0.0))
        return carry

    lax.fori_loop(0, PIECES, sum_step, 0)
    sums = []
    for buf in (sum_policy, sum_kl):
        per_member = [row_of(jnp.sum(buf[m], axis=1, keepdims=True)) for m in range(members_dev)]
        sums.append(row_sums(place, targets, per_member))
    count_send(0, pair).wait()
    counts[2] = count_join(0)

    @pl.when(inner)
    def _():
        count_send(1, across).start()
        count_send(1, across).wait()
        counts[4] = count_join(1)
        count_send(2, pair).start()
        count_send(2, pair).wait_send()
        counts[6] = counts[4]

    @pl.when(jnp.logical_not(inner))
    def _():
        count_send(2, pair).wait_recv()
        counts[6] = counts[5]

    tails_send[...] = tiles(sums, jnp.broadcast_to(counts[6][None], (n_gy, 8, LANES)))
    tail_copies = tile_sends(tails_send, tails_recv, tail_send_sem, tail_recv_sem, range(1, n_gy))
    for copy in tail_copies:
        copy.start()
    tails_recv[gy] = tails_send[chip]

    for copy in near_sends(chip_x, 0):
        copy.start()


    ntok = counts[6][:1, info_lane : info_lane + 1]
    scale = samples * seq / ntok
    got_len = column_in(arrived, 0).reshape(total_rows, 1)
    got_row = row_of(got_len)
    reward = column_in(arrived, 1).reshape(members, part, 1)
    advantage = (members * reward - jnp.sum(reward, axis=0)[None]) / (members - 1)
    adv_rows[...] = jnp.broadcast_to(advantage, adv_rows.shape)
    len_rows[...] = jnp.broadcast_to(got_len.reshape(members, part, 1), len_rows.shape)
    got_spot_row, got_spot = strip_plan(
        got_row, got_len, (row // pool).astype(f32), (column // pool).astype(f32),
        lax.rem(row, pool).astype(f32), lax.rem(column, pool).astype(f32), chips, seq,
    )
    rcnt[...] = jnp.broadcast_to(strip_counts(got_spot_row, got_row), rcnt.shape)
    lane = lax.broadcasted_iota(jnp.int32, (total_rows, LANES), 1).astype(f32)
    for half in range(HALVES):
        pick = got_spot - half * ROLES * 8 == lane
        pick = jnp.where(pick & (lane < ROLES * 8), 1.0, 0.0).astype(jnp.bfloat16)
        undeal[:, half] = pick.reshape(chips, pool, LANES)
    half_rows[...] = jnp.broadcast_to(jnp.where(got_spot < ROLES * 8, 0.0, 1.0).reshape(members, part, 1), half_rows.shape)
    def finish_rows(k, start, value, only=None):
        span = value.shape[1]
        cols = pl.ds(pl.multiple_of(start, LANES), span)
        positions = (lax.broadcasted_iota(jnp.int32, (part, span), 1) + start).astype(f32)
        value = (value - adv_rows[k][:, :1]) * scale
        value = jnp.where(positions < len_rows[k][:, :1], value, 0.0)
        if only is not None:
            value = jnp.where(only, value, done[k, :, cols])
        done[k, :, cols] = value

    def own_step(which, source):
        def column_step(c, carry):
            start = pl.multiple_of(c * piece, LANES)
            for m in range(members_dev):
                finish_rows(source * members_dev + m, start, which(m * part, pl.ds(start, piece)))
            return carry

        lax.fori_loop(0, PIECES, column_step, 0)

    own_step(lambda r, cols: ordered[0, chip, r : r + part, cols], gy)
    give_own.wait_recv()
    own_step(lambda r, cols: got[chip, r : r + part, cols], mate)

    def first_wait(off):
        landed = heads_in.at[0]
        pltpu.make_async_copy(landed, landed, first_recv_sem.at[off - 2]).wait()

    def first_step(off, carry):
        first_wait(off)
        source = peer_of(gy, off, n_gy)
        for m in range(members_dev):
            finish_rows(source * members_dev + m, 0, heads_in[source, m * part : (m + 1) * part, :])
        return carry

    lax.fori_loop(2, n_gy, first_step, 0)

    def unpack(there, t, half):
        landed = recvbuf.at[0, 0]
        pltpu.make_async_copy(landed, landed, strip_recv_sem.at[t, half]).wait()

        def put(r, start, rows):
            k = there * 2 * members_dev + r
            finish_rows(k, width + start, rows, half_rows[k][:, :1] > 0.5 if half else None)

        unpack_strips(recvbuf, roles, undeal, rcnt, there, half, part, put)

    second_legs = [
        relay(passing.at[half], recvbuf.at[chip_x, half], chip_y, strip_send_sem.at[2], strip_recv_sem.at[2], half)
        for half in range(HALVES)
    ]
    for first_leg, second_leg in zip(first_legs, second_legs):
        first_leg.wait_recv()
        second_leg.start()
    for half in range(HALVES):
        unpack(chip_y, 1, half)

    for copy in tail_copies:
        copy.wait()
    ends = tails_recv[...]
    first_sum = column_in(ends, 0).reshape(members, part, 1)
    second_sum = column_in(ends, 1).reshape(members, part, 1)
    value = (second_sum - advantage * first_sum) * (samples / ntok)[None]
    shape = (members, part, LANES)
    spread = lax.broadcasted_iota(jnp.int32, shape, 1) == lax.broadcasted_iota(jnp.int32, shape, 2)
    loss_ref[...] = jnp.sum(jnp.where(spread, value, 0.0), axis=1)[:, :part]
    adv_ref[...] = jnp.sum(jnp.where(spread, advantage, 0.0), axis=1)[:, :part]
    over_ref[0, 0] = (jnp.max(ends[:, :, fill_lane : fill_lane + 1]) > STRIP_BLOCKS).astype(jnp.int32)
    for off in FIRST_ORDER:
        landed = heads_in.at[0]
        pltpu.make_async_copy(landed, landed, first_send_sem.at[off - 2]).wait()
    pltpu.make_async_copy(given, given, give_send_sem.at[0]).wait()
    give_own.wait_send()

    scale_ref[...] = jnp.broadcast_to(scale, scale_ref.shape)

    def unpack_step(i, carry):
        unpack(peer_of(chip, 1 + 2 * i, chips), 2 * i, 0)
        return carry

    lax.fori_loop(0, 2, unpack_step, 0)
    for t in (0, 2):
        landed = recvbuf.at[0, 0]
        pltpu.make_async_copy(landed, landed, strip_recv_sem.at[t, 1]).wait()
    for half in range(HALVES):
        first_legs[half].wait_send()
        for t in range(chips - 1):
            sent = sendbuf.at[0, 0]
            pltpu.make_async_copy(sent, sent, strip_send_sem.at[t, half]).wait()


def store(
    n_gy, done, loss, adv, recvbuf, undeal, rcnt, len_rows, adv_rows, half_rows, scale_ref,
    grad, loss_out, adv_out, last, roles, sem,
):
    chips = n_gy // 2
    members, part, seq = done.shape
    group = members // chips
    width = seq - roles.shape[1]
    chip = lax.axis_index("gy") // 2
    scale = scale_ref[:1, :1]

    def chip_rows(there):
        return pl.ds(there * group, group)

    whole = [chip_rows(chip), chip_rows(peer_of(chip, 2, chips))]
    late = [peer_of(chip, 1, chips), peer_of(chip, 3, chips)]
    first = pl.ds(0, width)
    copies = [pltpu.make_async_copy(done.at[rows], grad.at[rows], sem.at[k]) for k, rows in enumerate(whole)]
    copies += [
        pltpu.make_async_copy(done.at[chip_rows(there), :, first], grad.at[chip_rows(there), :, first], sem.at[2 + k])
        for k, there in enumerate(late)
    ]
    copies += [pltpu.make_async_copy(loss, loss_out, sem.at[4]), pltpu.make_async_copy(adv, adv_out, sem.at[5])]
    for copy in copies:
        copy.start()

    def store_late(i):
        rows = chip_rows(peer_of(chip, 1 + 2 * i, chips))
        return pltpu.make_async_copy(last.at[i], grad.at[rows, :, pl.ds(width, seq - width)], sem.at[6 + i])

    def late_step(i, carry):
        there = peer_of(chip, 1 + 2 * i, chips)

        def put(r, start, rows):
            k, span = there * group + r, rows.shape[1]
            positions = (lax.broadcasted_iota(jnp.int32, (part, span), 1) + (width + start)).astype(jnp.float32)
            value = (rows - adv_rows[k][:, :1]) * scale
            before = done[k, :, pl.ds(pl.multiple_of(width + start, LANES), span)]
            value = jnp.where(half_rows[k][:, :1] > 0.5, jnp.where(positions < len_rows[k][:, :1], value, 0.0), before)
            last[i, r, :, pl.ds(start, span)] = value

        unpack_strips(recvbuf, roles, undeal, rcnt, there, 1, part, put)
        store_late(i).start()
        return carry

    lax.fori_loop(0, 2, late_step, 0)
    copies += [store_late(i) for i in range(2)]
    for copy in copies:
        copy.wait()


def packed_body(n_gx, n_gy, policy_logp, anchor_logp, lengths, rewards, slot_prompt):
    members_dev, slots, seq = policy_logp.shape
    members, part = members_dev * n_gy, slots // n_gy
    f32, bf16 = jnp.float32, jnp.bfloat16
    chips, rows = n_gy // 2, members_dev * part
    pool = 2 * rows
    width = HEAD_BLOCKS * LANES
    chunked = (PIECES, members_dev, slots, seq // PIECES)
    strips = (chips, HALVES, 8, STRIP_BLOCKS * LANES)
    per_slot = (members_dev, slots, LANES)
    per_sample = (members, part, LANES)
    tile = (n_gy, 8, LANES)
    hbm_spec = pl.BlockSpec(memory_space=pltpu.HBM)
    vmem_spec = pl.BlockSpec(memory_space=pltpu.VMEM)
    dma = pltpu.SemaphoreType.DMA
    handed = (
        pltpu.VMEM(strips, f32),
        pltpu.VMEM((chips, HALVES, pool, LANES), bf16),
        pltpu.VMEM((chips * pool, LANES), f32),
        pltpu.VMEM(per_sample, f32),
        pltpu.VMEM(per_sample, f32),
        pltpu.VMEM(per_sample, f32),
        pltpu.VMEM((8, LANES), f32),
    )
    done, loss, adv, over, *rest = pl.pallas_call(
        functools.partial(packed_exchange, n_gx, n_gy),
        out_shape=(
            pltpu.VMEM((members, part, seq), f32),
            pltpu.VMEM((members, part), f32),
            pltpu.VMEM((members, part), f32),
            pltpu.SMEM((1, 1), jnp.int32),
        ) + handed,
        in_specs=[hbm_spec] * 5,
        out_specs=(vmem_spec,) * 3 + (pl.BlockSpec(memory_space=pltpu.SMEM),) + (vmem_spec,) * len(handed),
        scratch_shapes=[
            pltpu.VMEM(chunked, f32),
            pltpu.VMEM(chunked, f32),
            pltpu.VMEM((members_dev, slots), jnp.int32),
            pltpu.VMEM((members_dev, slots), jnp.int32),
            pltpu.VMEM((members_dev, slots), jnp.int32),
            pltpu.VMEM((2 * chips * rows, members_dev * slots), bf16),
            pltpu.VMEM((2, chips, rows, seq), f32),
            pltpu.VMEM((chips, rows, seq), f32),
            pltpu.VMEM((n_gy, rows, width), f32),
            pltpu.VMEM(strips, f32),
            pltpu.VMEM(strips[1:], f32),
            pltpu.VMEM((pool, seq - width), f32),
            pltpu.VMEM((chips, pool, pool), bf16),
            pltpu.VMEM((chips * pool, LANES), f32),
            pltpu.VMEM(per_slot, f32),
            pltpu.VMEM(per_slot, f32),
            pltpu.VMEM(per_slot, f32),
            pltpu.VMEM(tile, f32),
            pltpu.VMEM((chips, 8, LANES), f32),
            pltpu.VMEM(tile, f32),
            pltpu.VMEM(tile, f32),
            pltpu.VMEM(tile, f32),
            pltpu.VMEM((2 * n_gx, 8, LANES), f32),
            dma((3,)),
            dma((2, PIECES)),
            dma((2,)),
            dma((2,)),
            dma((n_gy - 2,)),
            dma((n_gy - 2,)),
            dma((chips - 1, HALVES)),
            dma((chips - 1, HALVES)),
            dma((HALVES,)),
            dma((HALVES,)),
            dma((n_gy - 1,)),
            dma((n_gy - 1,)),
            dma((n_gy - 1,)),
            dma((n_gy - 1,)),
            dma((n_gx,)),
            dma((n_gx,)),
        ],
        compiler_params=pltpu.CompilerParams(collective_id=0, has_side_effects=True, vmem_limit_bytes=36 * 2**20),
    )(policy_logp, anchor_logp, lengths, rewards, slot_prompt)

    def fits(policy_logp, anchor_logp, lengths, rewards, slot_prompt, done, loss, adv, *rest):
        small = jax.ShapeDtypeStruct((members, part), f32)
        return tuple(pl.pallas_call(
            functools.partial(store, n_gy),
            out_shape=(jax.ShapeDtypeStruct((members, part, seq), f32), small, small),
            in_specs=[vmem_spec] * (3 + len(rest)),
            out_specs=(hbm_spec,) * 3,
            scratch_shapes=[
                pltpu.VMEM((2, 2 * members_dev, part, seq - width), f32),
                pltpu.VMEM((ROLES * 8, seq - width), f32),
                dma((8,)),
            ],
            compiler_params=pltpu.CompilerParams(vmem_limit_bytes=16 * 2**20),
        )(done, loss, adv, *rest))

    def overflows(policy_logp, anchor_logp, lengths, rewards, slot_prompt, done, loss, adv, *rest):
        return tuple(unpacked_body(n_gx, n_gy, policy_logp, anchor_logp, lengths, rewards, slot_prompt))

    return lax.cond(
        over[0, 0] > 0, overflows, fits,
        policy_logp, anchor_logp, lengths, rewards, slot_prompt, done, loss, adv, *rest,
    )


def body(n_gx, n_gy, *args):
    members_dev, slots, seq = args[0].shape
    pool = 2 * members_dev * slots // n_gy
    packs = n_gy == 8 and n_gx == 4 and pool == ROLES * STRIPS and slots == LANES and seq == LANES * 32 and seq % (PIECES * LANES) == 0
    return (packed_body if packs else unpacked_body)(n_gx, n_gy, *args)


def solution(mesh):
    placed = (P("gy", "gx", None), P("gy", "gx", None), P("gy", "gx"), P("gy", "gx"), P("gy", "gx"))
    return jax.shard_map(
        functools.partial(body, mesh.shape["gx"], mesh.shape["gy"]),
        mesh=mesh,
        in_specs=placed,
        out_specs=(P(None, ("gx", "gy"), None), P(None, ("gx", "gy")), P(None, ("gx", "gy"))),
        check_vma=False,
    )
```
